64 devices in a mesh: dp: 4 (over x, y), sp: 16 (over z, core).
Axes of the slice: x: 2, y: 2, z: 8, core: 2. Of those that a mesh axis runs over, the one named last changes fastest.
The devices are a block of a 4x4x8 slice.
Arguments:
- dec_hidden: bfloat16 [8192, 1024], P(('dp', 'sp')), parts along dimension 0
- enc_memory: bfloat16 [65536, 1024], P(('dp', 'sp')), parts along dimension 0
- mem_len: int32 [4], P('dp'), parts along dimension 0
- norm_self: bfloat16 [2, 1024], replicated
- norm_cross: bfloat16 [2, 1024], replicated
- norm_mlp: bfloat16 [2, 1024], replicated
- self_q: bfloat16 [2, 1024, 1024], replicated
- self_k: bfloat16 [2, 1024, 1024], replicated
- self_v: bfloat16 [2, 1024, 1024], replicated
- self_o: bfloat16 [2, 16, 64, 1024], replicated
- cross_q: bfloat16 [2, 1024, 1024], replicated
- cross_k: bfloat16 [2, 1024, 1024], replicated
- cross_v: bfloat16 [2, 1024, 1024], replicated
- cross_o: bfloat16 [2, 16, 64, 1024], replicated
- mlp_gate: bfloat16 [2, 1024, 2816], replicated
- mlp_up: bfloat16 [2, 1024, 2816], replicated
- mlp_down: bfloat16 [2, 2816, 1024], replicated
Outputs:
- output: bfloat16 [8192, 1024], P(('dp', 'sp')), parts along dimension 0
There are 4 independent parts. The reference program is written for one: setup_inputs(seed, part) draws one part's arguments, and reference() takes and returns one part's arrays. A program takes and returns all parts, laid end to end along the dimension named above; an argument that names none is the same for every part.
All inputs are finite; a program needn't handle non-finite values.
Results may differ from the reference program's by a relative error of at most 0.0150947.
Values are sent between devices in bfloat16 or wider.
A program may use at most 768 MiB of HBM per device.

```python
import jax
import jax.numpy as jnp
from jax import lax

D = 1024
HEADS = 16
KV_HEADS = 16
HEAD = 64
FF = 2816
LAYERS = 2
TQ = 2048
TM = 16384
WAVES = 4
EPS = 1e-6
NEG_BIG = -1e30
SOFT_SCALE = HEAD ** -0.5
DKV = KV_HEADS * HEAD


def smooth_field(wave_key, n_rows, n_cols):
    directions = jax.random.normal(wave_key, (WAVES, n_cols), jnp.float32)
    positions = jnp.arange(n_rows, dtype=jnp.float32) / n_rows
    freq_list = jnp.arange(1, WAVES + 1, dtype=jnp.float32)
    wave_rows = jnp.cos(jnp.pi * positions[:, None] * freq_list[None, :])
    return jnp.dot(wave_rows, directions)


def setup_inputs(seed: int = 0, part: int = 0) -> dict:
    part_key = jax.random.fold_in(jax.random.key(seed), part)
    part_keys = jax.random.split(part_key, 5)
    shared = jax.random.split(jax.random.key(seed + 1), 16)

    def weight(key_index, shape_tail, fan_in):
        raw_draw = jax.random.normal(shared[key_index], (LAYERS,) + shape_tail, jnp.float32)
        return (raw_draw * fan_in ** -0.5).astype(jnp.bfloat16)

    def gain(key_index):
        return jax.random.uniform(shared[key_index], (LAYERS, D), jnp.float32, 0.5, 1.5).astype(jnp.bfloat16)

    dec_hidden = jax.random.normal(part_keys[0], (TQ, D), jnp.float32) + smooth_field(part_keys[1], TQ, D)
    enc_memory = jax.random.normal(part_keys[2], (TM, D), jnp.float32) + smooth_field(part_keys[3], TM, D)
    mem_len = jax.random.randint(part_keys[4], (1,), TM // 4, 3 * TM // 4 + 1, dtype=jnp.int32)
    return {
        'dec_hidden': dec_hidden.astype(jnp.bfloat16),
        'enc_memory': enc_memory.astype(jnp.bfloat16),
        'mem_len': mem_len,
        'norm_self': gain(0),
        'norm_cross': gain(1),
        'norm_mlp': gain(2),
        'self_q': weight(3, (D, D), D),
        'self_k': weight(4, (D, D), D),
        'self_v': weight(5, (D, D), D),
        'self_o': weight(6, (HEADS, HEAD, D), D),
        'cross_q': weight(7, (D, D), D),
        'cross_k': weight(8, (D, DKV), D),
        'cross_v': weight(9, (D, DKV), D),
        'cross_o': weight(10, (HEADS, HEAD, D), D),
        'mlp_gate': weight(11, (D, FF), D),
        'mlp_up': weight(12, (D, FF), D),
        'mlp_down': weight(13, (FF, D), FF),
    }


def rms_norm(hidden, gain_vec):
    hidden32 = hidden.astype(jnp.float32)
    inv_rms = lax.rsqrt(jnp.mean(hidden32 * hidden32, axis=-1, keepdims=True) + EPS)
    return (hidden32 * inv_rms * gain_vec.astype(jnp.float32)).astype(jnp.bfloat16)


def project(acts, weight_mat):
    return jnp.dot(acts, weight_mat, preferred_element_type=jnp.float32).astype(jnp.bfloat16)


def add_residual(hidden, update):
    return (hidden.astype(jnp.float32) + update).astype(jnp.bfloat16)


def head_attend(query_h, key_h, value_h, allowed):
    scores = jnp.dot(query_h, key_h.T, preferred_element_type=jnp.float32) * SOFT_SCALE
    scores = jnp.where(allowed, scores, NEG_BIG)
    weights = jnp.exp(scores - jnp.max(scores, axis=-1, keepdims=True))
    numerator = jnp.dot(weights.astype(jnp.bfloat16), value_h, preferred_element_type=jnp.float32)
    return numerator / jnp.sum(weights, axis=-1, keepdims=True)


def multi_head(queries, keys_all, values_all, allowed):
    q_rows = queries.shape[0]
    k_rows = keys_all.shape[0]
    kv_count = keys_all.shape[1] // HEAD
    q_heads = queries.reshape(q_rows, HEADS, HEAD).transpose(1, 0, 2)
    k_heads = jnp.repeat(keys_all.reshape(k_rows, kv_count, HEAD).transpose(1, 0, 2), HEADS // kv_count, axis=0)
    v_heads = jnp.repeat(values_all.reshape(k_rows, kv_count, HEAD).transpose(1, 0, 2), HEADS // kv_count, axis=0)
    per_head = lax.map(lambda head_trio: head_attend(head_trio[0], head_trio[1], head_trio[2], allowed), (q_heads, k_heads, v_heads))
    return per_head.transpose(1, 0, 2).astype(jnp.bfloat16)


def reference(dec_hidden, enc_memory, mem_len, norm_self, norm_cross, norm_mlp, self_q, self_k, self_v, self_o, cross_q, cross_k, cross_v, cross_o, mlp_gate, mlp_up, mlp_down):
    causal = jnp.arange(TQ)[:, None] >= jnp.arange(TQ)[None, :]
    mem_valid = (jnp.arange(TM) < mem_len[0])[None, :]
    stacked = {
        'norm_self': norm_self, 'norm_cross': norm_cross, 'norm_mlp': norm_mlp,
        'self_q': self_q, 'self_k': self_k, 'self_v': self_v, 'self_o': self_o,
        'cross_q': cross_q, 'cross_k': cross_k, 'cross_v': cross_v, 'cross_o': cross_o,
        'mlp_gate': mlp_gate, 'mlp_up': mlp_up, 'mlp_down': mlp_down,
    }

    def layer_step(hidden, params):
        normed = rms_norm(hidden, params['norm_self'])
        attended = multi_head(project(normed, params['self_q']), project(normed, params['self_k']), project(normed, params['self_v']), causal)
        update = jnp.einsum('thd,hdo->to', attended.astype(jnp.float32), params['self_o'].astype(jnp.float32))
        hidden = add_residual(hidden, update)
        normed = rms_norm(hidden, params['norm_cross'])
        attended = multi_head(project(normed, params['cross_q']), project(enc_memory, params['cross_k']), project(enc_memory, params['cross_v']), mem_valid)
        update = jnp.einsum('thd,hdo->to', attended.astype(jnp.float32), params['cross_o'].astype(jnp.float32))
        hidden = add_residual(hidden, update)
        normed = rms_norm(hidden, params['norm_mlp'])
        gate_pre = jnp.dot(normed, params['mlp_gate'], preferred_element_type=jnp.float32)
        up_proj = jnp.dot(normed, params['mlp_up'], preferred_element_type=jnp.float32)
        hidden_act = (jax.nn.silu(gate_pre) * up_proj).astype(jnp.bfloat16)
        update = jnp.dot(hidden_act, params['mlp_down'], preferred_element_type=jnp.float32)
        return add_residual(hidden, update), None

    final_hidden, _ = lax.scan(layer_step, dec_hidden, stacked)
    return final_hidden
```

```python
import functools
import math

import jax
import jax.numpy as jnp
from jax import lax
from jax.experimental import pallas as pl
from jax.experimental.pallas import tpu as pltpu
from jax.sharding import PartitionSpec as P

MESH = pl.DeviceIdType.MESH
EPS = 1e-6
NEG = -1e30
T = 256
F32 = jnp.float32
BF16 = jnp.bfloat16
NT = (((1,), (1,)), ((), ()))


def dot(a, b):
    return jnp.dot(a, b, preferred_element_type=F32)


def dot_nt(a, b):
    return lax.dot_general(a, b, NT, preferred_element_type=F32)


def fold_max(x):
    return jnp.max(x.reshape(x.shape[0] // 8, 8, x.shape[1]), axis=0)


def fold_sum(x):
    return jnp.sum(x.reshape(x.shape[0] // 8, 8, x.shape[1]), axis=0)


def head_lanes(q2, e):
    lane = lax.broadcasted_iota(jnp.int32, q2.shape, 1)
    keep = lane < 64 if e == 0 else lane >= 64
    return jnp.where(keep, q2.astype(F32), 0.0).astype(BF16)


def ones_lane(rows):
    lane = lax.broadcasted_iota(jnp.int32, (rows, 128), 1)
    return jnp.where(lane == 0, 1.0, 0.0).astype(BF16)


def qk(S, slot, keys, rhs, blocks, masked=None):
    top = None
    for b in range(blocks):
        s = dot_nt(keys(b), rhs)
        if masked is not None:
            s = masked(b, s)
        S[slot, b * T:(b + 1) * T, :] = s
        t = fold_max(s)
        top = t if top is None else jnp.maximum(top, t)
    return top


def pv(S, slot, values, top, blocks, c):
    m = jnp.max(top, axis=0, keepdims=True)
    part = jnp.zeros((8, T), F32)
    num = jnp.zeros((64, T), F32)
    for b in range(blocks):
        p = jnp.exp2((S[slot, b * T:(b + 1) * T, :] - m) * c)
        part = part + fold_sum(p)
        num = num + dot(values(b), p.astype(BF16))
    return num, jnp.sum(part, axis=0, keepdims=True), m


def rms_norm(h, g):
    h = h.astype(F32)
    inv = lax.rsqrt(jnp.mean(h * h, axis=-1, keepdims=True) + EPS)
    return (h * inv * g).astype(BF16)


def kernel(n_dev, head_dim, n_layers,
           mem_len, hid_in, mem_in, g_self, g_cross, g_mlp,
           self_q, self_k, self_v, self_o, cross_q, cross_k, cross_v, cross_o, mlp_g, mlp_u, mlp_d,
           out,
           hid, x_all, mem, ks, vs, kc, vc, bias, qs, q_all, S, top_s,
           wq, wk, wv, wo, cq, ck, cv, co, wg, wu, wd,
           part, part_ml, o_send, ml_send, o_recv, ml_recv,
           a_half, att, xc, act,
           xtx, xrx, ptx, prx, qtx, qrx, otx, orx, mtx, mrx, dtx, drx, wsem, gsem, usem, isem):
    Z = n_dev // 2
    rows, D = hid.shape
    half = rows // 2
    NP = qs.shape[0]
    KBS = ks.shape[0]
    KBC = kc.shape[0]
    NF = wg.shape[0]
    Dc = D // 2
    mem_rows = mem_in.shape[0]
    c_exp = math.log2(math.e) * head_dim ** -0.5

    me = lax.axis_index("sp")
    z = me // 2
    c = me % 2
    partner = z * 2 + (1 - c)

    def ring(k):
        return lax.rem(z + k + 2 * Z, Z)

    def nbr(d):
        return ring(1 - 2 * d) * 2 + c

    def rcopy(src, dst, ssem, rsem, dev):
        return pltpu.make_async_remote_copy(src_ref=src, dst_ref=dst, send_sem=ssem, recv_sem=rsem,
                                            device_id={"sp": dev}, device_id_type=MESH)

    my_rows = pl.multiple_of(c * rows, rows)
    my_cols = pl.multiple_of(c * Dc, Dc)

    barrier = pltpu.get_barrier_semaphore()
    for dev in (nbr(0), nbr(1), partner):
        pl.semaphore_signal(barrier, inc=1, device_id={"sp": dev}, device_id_type=MESH)

    def wcopies(l):
        cols = pl.ds(my_cols, Dc)
        w = [
            (self_k.at[l, :, cols], wk), (self_q.at[l, :, cols], wq), (self_v.at[l, :, cols], wv),
            (cross_k.at[l, :, cols], ck), (cross_v.at[l, :, cols], cv),
            (self_o.at[l], wo), (cross_q.at[l, :, cols], cq), (cross_o.at[l], co), (mlp_d.at[l], wd),
        ]
        return [pltpu.make_async_copy(s, d, wsem.at[i]) for i, (s, d) in enumerate(w)]

    WK, WQ, WV, CK, CV, WO, CQ, CO, WD = range(9)

    def gate_copy(l, f):
        return pltpu.make_async_copy(mlp_g.at[l, :, pl.ds(f * T, T)], wg.at[f], gsem.at[f])

    def up_copy(l, f):
        return pltpu.make_async_copy(mlp_u.at[l, :, pl.ds(f * T, T)], wu.at[f], usem.at[f])

    hid_copy = pltpu.make_async_copy(hid_in, hid, isem.at[0])
    mem_copy = pltpu.make_async_copy(mem_in, mem.at[c], isem.at[1])
    mem_swap = rcopy(mem_in, mem.at[c], dtx.at[3], drx.at[3], partner)
    hid_copy.start()
    first = wcopies(0)
    for i in (WK, WQ, WV):
        first[i].start()
    mem_copy.start()
    for i in (CK, CV, WO, CQ, CO):
        first[i].start()
    for f in range(NF):
        gate_copy(0, f).start()
        up_copy(0, f).start()
    first[WD].start()

    pl.semaphore_wait(barrier, 3)
    mem_swap.start()

    length = mem_len[0]
    for b in range(KBC):
        key = z * (2 * mem_rows) + b * T + lax.broadcasted_iota(jnp.int32, (T, 128), 0)
        lane = lax.broadcasted_iota(jnp.int32, (T, 128), 1)
        bias[b] = jnp.where(jnp.logical_and(lane == 0, key >= length), NEG, 0.0).astype(BF16)

    hid_copy.wait()

    def gain(ref, l):
        g = jnp.zeros((1, D), F32)
        for i in range(n_layers):
            g = jnp.where(l == i, ref[i:i + 1, :].astype(F32), g)
        return g

    def kv_block(x, wk_ref, wv_ref, kdst, vdst, b):
        k = dot(x, wk_ref[...]).astype(BF16)
        for p in range(NP):
            kdst[b, p] = k[:, p * 128:(p + 1) * 128]
        v = dot(x, wv_ref[...])
        for p in range(NP):
            vdst[b, p] = jnp.transpose(v[:, p * 128:(p + 1) * 128]).astype(BF16)

    def swap_heads(k):
        swap = rcopy(a_half.at[k, 1 - c], att.at[k, c], dtx.at[k], drx.at[k], partner)
        swap.start()
        att[k, c] = a_half[k, c]
        swap.wait()

    def project_out(k, w_ref):
        a = jnp.concatenate(
            [jnp.transpose(att[k, i].astype(F32)).astype(BF16) for i in range(2)], axis=1)
        hid[...] = (hid[...].astype(F32) + dot(a, w_ref[...])).astype(BF16)

    def layer_body(l, carry):
        more = l + 1 < n_layers
        cur = wcopies(l)
        nxt = wcopies(jnp.minimum(l + 1, n_layers - 1))

        def prefetch(*ids):
            @pl.when(more)
            def _():
                for i in ids:
                    nxt[i].start()

        x_all[z, pl.ds(my_rows, rows), :] = rms_norm(hid[...], gain(g_self, l))

        def xslot(o, h):
            return x_all.at[o, pl.ds(pl.multiple_of(c * rows + h * half, half), half), :]

        for h in range(2):
            src = xslot(z, h)
            for d in range(2):
                rcopy(src, src, xtx.at[d, 0, h], xrx.at[d, 1, h], nbr(d)).start()
            rcopy(src, src, ptx.at[z, h], prx.at[z, h], partner).start()

        def pslot(o, h):
            return x_all.at[o, pl.ds(pl.multiple_of((1 - c) * rows + h * half, half), half), :]

        def gather_level(s, _):
            for h in range(2):
                for d in range(2):
                    sign = 1 - 2 * d
                    o = ring(-sign * s)
                    src = xslot(o, h)

                    @pl.when(jnp.logical_and(s >= 1, jnp.logical_or(s <= 3, h == d)))
                    def _():
                        rcopy(src, src, xtx.at[d, s, h], xrx.at[d, s, h], nbr(d)).wait_recv()

                        @pl.when(jnp.logical_or(s < 3, jnp.logical_and(s == 3, h == d)))
                        def _():
                            rcopy(src, src, xtx.at[d, s, h], xrx.at[d, s + 1, h], nbr(d)).start()
                        rcopy(src, src, ptx.at[o, h], prx.at[o, h], partner).start()

            @pl.when(s == 0)
            def _():
                for i in (WK, WV, WQ, CK, CV):
                    cur[i].wait()

                @pl.when(l == 0)
                def _():
                    mem_copy.wait()
                    mem_swap.wait()

            def block(j, _):
                o = ring(s * (1 - 2 * j))
                for h in range(2):
                    dst = pslot(o, h)
                    rcopy(dst, dst, ptx.at[o, h], prx.at[o, h], partner).wait_recv()
                kv_block(x_all[o], wk, wv, ks, vs, o)

                @pl.when(o < KBC)
                def _():
                    per = mem_rows // T
                    rowsl = pl.ds(pl.multiple_of(lax.rem(o, per) * T, T), T)
                    kv_block(mem[o // per, rowsl, :], ck, cv, kc, vc, o)
                return 0

            lax.fori_loop(0, jnp.where(jnp.logical_or(s == 0, s == Z // 2), 1, 2), block, 0)

            @pl.when(s == 0)
            def _():
                q = dot(x_all[z], wq[...]).astype(BF16)
                for p in range(NP):
                    qs[p] = q[:, p * 128:(p + 1) * 128]
            return 0

        lax.fori_loop(0, Z // 2 + 1, gather_level, 0)
        prefetch(WK, WQ, WV, CK, CV)

        delta = (lax.broadcasted_iota(jnp.int32, (T, T), 0) - lax.broadcasted_iota(jnp.int32, (T, T), 1))

        def causal(b, s):
            return jnp.where(delta <= (z - b) * T, s, NEG)

        def self_qk(slot, p, e):
            return qk(S, slot, lambda b: ks[b, p], head_lanes(qs[p], e), KBS, causal)

        top_s[...] = self_qk(0, 0, 0)

        def self_pair(p, _):
            t1 = self_qk(1, p, 1)
            o0, l0, m0 = pv(S, 0, lambda b: vs[b, p, 0:64, :], top_s[...], KBS, c_exp)
            top_s[...] = self_qk(0, lax.rem(p + 1, NP), 0)
            o1, l1, m1 = pv(S, 1, lambda b: vs[b, p, 64:128, :], t1, KBS, c_exp)
            a0 = (o0 / l0).astype(BF16)
            a1 = (o1 / l1).astype(BF16)
            at = pl.multiple_of(p * 128, 128)
            for j in range(2):
                a_half[0, j, pl.ds(at, 64), :] = a0[:, j * 128:(j + 1) * 128]
                a_half[0, j, pl.ds(at + 64, 64), :] = a1[:, j * 128:(j + 1) * 128]
            return 0

        lax.fori_loop(0, NP, self_pair, 0)

        swap_heads(0)
        cur[WO].wait()
        project_out(0, wo)
        prefetch(WO)

        for h in range(2):
            for d in range(2):
                for s in range(4):
                    if s < 3 or h == d:
                        src = xslot(z, h)
                        rcopy(src, src, xtx.at[d, s, h], xrx.at[d, s, h], nbr(d)).wait_send()
            for o in range(Z):
                src = xslot(o, h)
                rcopy(src, src, ptx.at[o, h], prx.at[o, h], partner).wait_send()

        xc[c] = rms_norm(hid[...], gain(g_cross, l))
        swap = rcopy(xc.at[c], xc.at[c], dtx.at[2], drx.at[2], partner)
        swap.start()
        cur[CQ].wait()
        swap.wait()
        for i in range(2):
            q = dot(xc[i], cq[...]).astype(BF16)
            for p in range(NP):
                q_all[z, p, i * rows:(i + 1) * rows, :] = q[:, p * 128:(p + 1) * 128]
        prefetch(CQ)

        def q_own(p):
            for d in range(2):
                src = q_all.at[z, p]
                rcopy(src, src, qtx.at[d, 0, p], qrx.at[d, 1, p], nbr(d)).start()

        def q_event(d, s, p):
            sign = 1 - 2 * d
            src = q_all.at[ring(-sign * s), p]
            rcopy(src, src, qtx.at[d, s, p], qrx.at[d, s, p], nbr(d)).wait_recv()

            @pl.when(jnp.logical_or(s < 3, jnp.logical_and(s == 3, lax.rem(p, 2) == d)))
            def _():
                rcopy(src, src, qtx.at[d, s, p], qrx.at[d, s + 1, p], nbr(d)).start()

        one = ones_lane(T)

        def cross_qk(slot, o, p, e):
            rhs = jnp.concatenate([head_lanes(q_all[o, p], e), one], axis=1)
            return qk(S, slot, lambda b: jnp.concatenate([kc[b, p], bias[b]], axis=1), rhs, KBC)

        def cross_group(o, p, o_next, p_next, to):
            t1 = cross_qk(1, o, p, 1)
            o0, l0, m0 = pv(S, 0, lambda b: vc[b, p, 0:64, :], top_s[...], KBC, c_exp)
            top_s[...] = cross_qk(0, o_next, p_next, 0)
            o1, l1, m1 = pv(S, 1, lambda b: vc[b, p, 64:128, :], t1, KBC, c_exp)
            part[to, 0:64, :] = o0
            part[to, 64:128, :] = o1
            part_ml[to] = jnp.concatenate([m0, m1, l0, l1, m0, m1, l0, l1], axis=0)

        def order(i):
            u = i + 2
            s = u // 4
            v = lax.rem(u, 4)
            edge = jnp.logical_or(s == 0, s == 4)
            p = jnp.where(edge, lax.rem(v, 2), v // 2)
            d = jnp.where(edge, p, lax.rem(v, 2))
            return s, d, p

        def origin(s, d):
            return ring(jnp.where(d == 0, -s, s))

        def merge(slot, d, s, p):
            rcopy(o_send.at[d, s, p], o_recv.at[d, s, p], otx.at[d, s, p], orx.at[d, s, p], nbr(d)).wait_recv()
            rcopy(ml_send.at[d, s, p], ml_recv.at[d, s, p], mtx.at[d, s, p], mrx.at[d, s, p], nbr(d)).wait_recv()
            a, b = part_ml[slot], ml_recv[d, s, p]
            m = jnp.maximum(a[0:2], b[0:2])
            ea = jnp.exp2((a[0:2] - m) * c_exp)
            eb = jnp.exp2((b[0:2] - m) * c_exp)
            l = a[2:4] * ea + b[2:4] * eb
            for e in range(2):
                r = slice(e * 64, (e + 1) * 64)
                part[slot, r, :] = (part[slot, r, :] * ea[e:e + 1] + o_recv[d, s, p, r, :].astype(F32) * eb[e:e + 1])
            part_ml[slot] = jnp.concatenate([m, l, m, l], axis=0)

        def reduce_step(slot, s, d_arr, p):
            d = jnp.where(s == 4, lax.rem(p, 2), 1 - d_arr)
            has_in = jnp.logical_and(s >= 1, jnp.logical_or(s < 3, jnp.logical_and(s == 3, lax.rem(p, 2) == d)))

            @pl.when(has_in)
            def _():
                merge(slot, d, s, p)

            @pl.when(s >= 1)
            def _():
                o_send[d, s - 1, p] = part[slot].astype(BF16)
                ml_send[d, s - 1, p] = part_ml[slot]
                rcopy(o_send.at[d, s - 1, p], o_recv.at[d, s - 1, p], otx.at[d, s - 1, p], orx.at[d, s - 1, p], nbr(d)).start()
                rcopy(ml_send.at[d, s - 1, p], ml_recv.at[d, s - 1, p], mtx.at[d, s - 1, p], mrx.at[d, s - 1, p], nbr(d)).start()

            @pl.when(s == 0)
            def _():
                for dd in range(2):
                    merge(slot, dd, 0, p)
                l = part_ml[slot]
                at = pl.multiple_of(p * 128, 128)
                for e in range(2):
                    a = (part[slot, e * 64:(e + 1) * 64, :] / l[2 + e:3 + e]).astype(BF16)
                    for j in range(2):
                        a_half[1, j, pl.ds(at + e * 64, 64), :] = a[:, j * 128:(j + 1) * 128]

        for p in range(NP // 2):
            q_own(p)
        top_s[...] = cross_qk(0, z, 0, 0)

        def near(i, _):
            s, d, p = order(i)
            sn, dn, pn = order(i + 1)
            last = i == 15
            @pl.when(jnp.logical_and(sn >= 1, jnp.logical_not(last)))
            def _():
                q_event(dn, sn, pn)

            @pl.when(i == 0)
            def _():
                for p in range(NP // 2, NP):
                    q_own(p)

            @pl.when(jnp.logical_and(jnp.logical_and(sn >= 2, sn <= 3), jnp.logical_not(last)))
            def _():
                q_event(dn, sn - 1, pn + 2)

            @pl.when(jnp.logical_and(sn == 4, jnp.logical_not(last)))
            def _():
                for dd in range(2):
                    q_event(dd, sn - 1, pn + 2)

            @pl.when(last)
            def _():
                q_event(1, 4, 3)
            o_next = jnp.where(last, ring(4), origin(sn, dn))
            p_next = jnp.where(last, 3, pn)
            cross_group(origin(s, d), p, o_next, p_next, i)
            return 0

        lax.fori_loop(0, 16, near, 0)

        def far(k, _):
            i = 15 - k
            s, d, p = order(i)
            last = k == 15
            sn, dn, pn = order(jnp.maximum(i - 1, 0))

            @pl.when(k == 0)
            def _():
                q_event(0, 4, 2)
            cross_group(origin(s, d), p + 2, origin(sn, dn), pn + 2, 16)

            def both(j, _):
                reduce_step(jnp.where(j == 0, i, 16), s, d, p + 2 * j)
                return 0

            lax.fori_loop(0, 2, both, 0)
            return 0

        lax.fori_loop(0, 16, far, 0)

        swap_heads(1)
        cur[CO].wait()
        project_out(1, co)
        prefetch(CO)

        for p in range(NP):
            for d in range(2):
                for s in range(4):
                    if s < 3 or p % 2 == d:
                        src = q_all.at[z, p]
                        rcopy(src, src, qtx.at[d, s, p], qrx.at[d, s, p], nbr(d)).wait_send()
                for s in range(4):
                    if s < 3 or p % 2 == d:
                        rcopy(o_send.at[d, s, p], o_recv.at[d, s, p], otx.at[d, s, p], orx.at[d, s, p], nbr(d)).wait_send()
                        rcopy(ml_send.at[d, s, p], ml_recv.at[d, s, p], mtx.at[d, s, p], mrx.at[d, s, p], nbr(d)).wait_send()

        xm = rms_norm(hid[...], gain(g_mlp, l))
        a_m = xm

        def ff(f, _):
            gate_copy(l, f).wait()
            up_copy(l, f).wait()
            gt = dot(a_m, wg[f])
            up = dot(a_m, wu[f])
            act[f] = (gt * lax.logistic(gt) * up).astype(BF16)

            @pl.when(more)
            def _():
                gate_copy(l + 1, f).start()
                up_copy(l + 1, f).start()
            return 0

        lax.fori_loop(0, NF, ff, 0)
        cur[WD].wait()
        full = jnp.concatenate([act[f] for f in range(NF)], axis=1)
        for n in range(D // T):
            cols = slice(n * T, (n + 1) * T)
            hid[:, cols] = (hid[:, cols].astype(F32) + dot(full, wd[:, cols])).astype(BF16)
        prefetch(WD)
        return carry

    lax.fori_loop(0, n_layers, layer_body, 0)
    out[...] = hid[...]


def solution(mesh):
    n_dev = mesh.shape["sp"]

    def local_step(hidden, memory, mem_len, norm_self, norm_cross, norm_mlp, self_q, self_k, self_v, self_o,
                   cross_q, cross_k, cross_v, cross_o, mlp_gate, mlp_up, mlp_down):
        rows, D = hidden.shape
        mem_rows = memory.shape[0]
        L, heads, head_dim = self_o.shape[:3]
        FF = mlp_gate.shape[2]
        Dc = D // 2
        NP = Dc // 128
        Z = n_dev // 2
        KBS = Z * 2 * rows // T
        KBC = 2 * mem_rows // T
        NF = FF // T
        any_ = pl.BlockSpec(memory_space=pl.ANY)
        vmem = pl.BlockSpec(memory_space=pltpu.VMEM)
        smem = pl.BlockSpec(memory_space=pltpu.SMEM)
        dma = pltpu.SemaphoreType.DMA
        V = pltpu.VMEM
        scratch = [
            V((rows, D), BF16),
            V((Z, 2 * rows, D), BF16),
            V((2, mem_rows, D), BF16),
            V((KBS, NP, T, 128), BF16),
            V((KBS, NP, 128, T), BF16),
            V((KBC, NP, T, 128), BF16),
            V((KBC, NP, 128, T), BF16),
            V((KBC, T, 128), BF16),
            V((NP, 2 * rows, 128), BF16),
            V((Z, NP, 2 * rows, 128), BF16),
            V((2, max(KBS, KBC) * T, T), F32),
            V((8, T), F32),
            V((D, Dc), BF16), V((D, Dc), BF16), V((D, Dc), BF16), V((D, D), BF16),
            V((D, Dc), BF16), V((D, Dc), BF16), V((D, Dc), BF16), V((D, D), BF16),
            V((NF, D, T), BF16), V((NF, D, T), BF16), V((FF, D), BF16),
            V((17, 128, T), F32),
            V((17, 8, T), F32),
            V((2, 4, NP, 128, T), BF16),
            V((2, 4, NP, 8, T), F32),
            V((2, 4, NP, 128, T), BF16),
            V((2, 4, NP, 8, T), F32),
            V((2, 2, Dc, 128), BF16),
            V((2, 2, Dc, 128), BF16),
            V((2, rows, D), BF16),
            V((NF, rows, T), BF16),
            dma((2, 5, 2)), dma((2, 5, 2)), dma((Z, 2)), dma((Z, 2)),
            dma((2, 5, NP)), dma((2, 5, NP)),
            dma((2, 4, NP)), dma((2, 4, NP)), dma((2, 4, NP)), dma((2, 4, NP)),
            dma((4,)), dma((4,)), dma((9,)), dma((NF,)), dma((NF,)), dma((2,)),
        ]
        call = pl.pallas_call(
            functools.partial(kernel, n_dev, head_dim, L),
            out_shape=jax.ShapeDtypeStruct((rows, D), BF16),
            in_specs=[smem, any_, any_, vmem, vmem, vmem] + [any_] * 11,
            out_specs=vmem,
            scratch_shapes=scratch,
            compiler_params=pltpu.CompilerParams(
                collective_id=0, has_side_effects=True, vmem_limit_bytes=67043328),
            name="decoder",
        )
        return call(mem_len, hidden, memory, norm_self, norm_cross, norm_mlp,
                    self_q, self_k, self_v, self_o.reshape(L, D, D), cross_q, cross_k, cross_v,
                    cross_o.reshape(L, D, D), mlp_gate, mlp_up, mlp_down)

    row_spec = P(("dp", "sp"), None)
    return jax.shard_map(local_step, mesh=mesh, in_specs=(row_spec, row_spec, P("dp")) + (P(),) * 14,
                         out_specs=row_spec, check_vma=False)
```

```python
import functools
import math

import jax
import jax.numpy as jnp
from jax import lax
from jax.experimental import pallas as pl
from jax.experimental.pallas import tpu as pltpu
from jax.sharding import PartitionSpec as P

MESH = pl.DeviceIdType.MESH
EPS = 1e-6
NEG = -1e30
T = 256
F32 = jnp.float32
BF16 = jnp.bfloat16

def unpack(bits, count, *words):
    per = 84 // bits
    return [(words[i // per] >> (i % per * bits)) % 2 ** bits for i in range(count)]


GROUPS = unpack(6, 32, 0xc9a48a0a1a51649050800, 0xeb3ad3f3b91c11b8cb0ea, 0xc798b0)
ARRIVALS = unpack(6, 30, 0x692282e71a61651241c20, 0xef3704ae36d32c3eb28aa, 0xf24)
RETURNS = unpack(6, 20, 0xada4fb07c2e471b0848c3, 0xe92662cca)
COUNTS = unpack(6, 16, 0x62045930a102102102100, 0x810)
LAST = unpack(9, 12, 0x100149c4725110a24642a, 0x806010)


def table(values, bits):
    per = 30 // bits
    words = [sum(v << (bits * j) for j, v in enumerate(values[i:i + per])) for i in range(0, len(values), per)]

    def get(i):
        w = jnp.int32(words[0])
        for k, v in enumerate(words[1:], 1):
            w = jnp.where(i >= k * per, jnp.int32(v), w)
        return lax.rem(lax.shift_right_logical(w, lax.rem(i, per) * bits), 1 << bits)

    return get


def decode(v):
    return lax.rem(v, 8), lax.rem(v // 8, 2), lax.rem(v // 16, 4)


def dot(a, b):
    return jnp.dot(a, b, preferred_element_type=F32)


def fold_max(x):
    return jnp.max(x.reshape(x.shape[0] // 8, 8, x.shape[1]), axis=0)


def fold_sum(x):
    return jnp.sum(x.reshape(x.shape[0] // 8, 8, x.shape[1]), axis=0)


def one_head(qt, e):
    rest = jnp.zeros((64, qt.shape[1]), BF16)
    return jnp.concatenate([qt[0:64], rest] if e == 0 else [rest, qt[64:128]], axis=0)


def ones_row(cols):
    row = lax.broadcasted_iota(jnp.int32, (128, cols), 0)
    return jnp.where(row == 0, 1.0, 0.0).astype(BF16)


def scores(S, slot, keys, rhs, b):
    s = dot(keys(b), rhs)
    S[slot, b * T:(b + 1) * T, :] = s
    return fold_max(s)


def score_all(S, slot, keys, rhs, blocks):
    return functools.reduce(jnp.maximum, [scores(S, slot, keys, rhs, b) for b in range(blocks)])


def score_and_sum(S, slot, keys, rhs, slot_v, values, top, blocks, c):
    ahead = min(3, blocks)
    m = jnp.max(top, axis=0, keepdims=True)
    tops = [scores(S, slot, keys, rhs, b) for b in range(ahead)]
    part = jnp.zeros((8, T), F32)
    num = jnp.zeros((64, T), F32)
    for b in range(blocks):
        p = jnp.exp2((S[slot_v, b * T:(b + 1) * T, :] - m) * c)
        part = part + fold_sum(p)
        num = num + dot(values(b), p.astype(BF16))
        if b + ahead < blocks:
            tops.append(scores(S, slot, keys, rhs, b + ahead))
    return functools.reduce(jnp.maximum, tops), num, jnp.sum(part, axis=0, keepdims=True), m


def rms_norm(h, g):
    h = h.astype(F32)
    inv = lax.rsqrt(jnp.mean(h * h, axis=-1, keepdims=True) + EPS)
    return (h * inv * g).astype(BF16)


def kernel(n_dev, head_dim, n_layers,
           mem_len, hid_in, mem_in, g_self, g_cross, g_mlp,
           self_q, self_k, self_v, self_o, cross_q, cross_k, cross_v, cross_o, mlp_g, mlp_u, mlp_d,
           out,
           hid, x_all, mem, ks, vs, kc, vc, bias, qm, q_all, S, top_s,
           wq, wk, wv, wo, cq, ck, cv, co, wg, wu, wd,
           part, part_ml, o_send, ml_send, o_recv, ml_recv,
           s_num, s_max, s_sum, a_half, att, upd, xc,
           xtx, xrx, ptx, prx, qtx, qrx, otx, orx, mtx, mrx, dtx, drx, wsem, gsem, usem, isem):
    Z = n_dev // 2
    rows, D = hid.shape
    half = rows // 2
    NP = q_all.shape[1]
    KBC = kc.shape[0]
    NF = wg.shape[0]
    Dc = D // 2
    mem_rows = mem_in.shape[0]
    c_exp = math.log2(math.e) * head_dim ** -0.5

    me = lax.axis_index("sp")
    z = me // 2
    c = me % 2
    partner = z * 2 + (1 - c)

    def ring(k):
        return lax.rem(z + k + 2 * Z, Z)

    def nbr(d):
        return ring(1 - 2 * d) * 2 + c

    def rcopy(src, dst, ssem, rsem, dev):
        return pltpu.make_async_remote_copy(src_ref=src, dst_ref=dst, send_sem=ssem, recv_sem=rsem,
                                            device_id={"sp": dev}, device_id_type=MESH)

    my_rows = pl.multiple_of(c * rows, rows)
    my_cols = pl.multiple_of(c * Dc, Dc)
    other_cols = pl.multiple_of((1 - c) * Dc, Dc)

    barrier = pltpu.get_barrier_semaphore()
    for dev in (nbr(0), nbr(1), partner):
        pl.semaphore_signal(barrier, inc=1, device_id={"sp": dev}, device_id_type=MESH)

    def wcopies(l):
        cols = pl.ds(my_cols, Dc)
        w = [
            (self_k.at[l, :, cols], wk), (self_q.at[l, :, cols], wq), (self_v.at[l, :, cols], wv),
            (cross_k.at[l, :, cols], ck), (cross_v.at[l, :, cols], cv),
            (self_o.at[l], wo), (cross_q.at[l, :, cols], cq), (cross_o.at[l], co), (mlp_d.at[l], wd),
        ]
        return [pltpu.make_async_copy(s, d, wsem.at[i]) for i, (s, d) in enumerate(w)]

    WK, WQ, WV, CK, CV, WO, CQ, CO, WD = range(9)

    def gate_copy(l, f):
        return pltpu.make_async_copy(mlp_g.at[l, :, pl.ds(f * T, T)], wg.at[f], gsem.at[f])

    def up_copy(l, f):
        return pltpu.make_async_copy(mlp_u.at[l, :, pl.ds(f * T, T)], wu.at[f], usem.at[f])

    hid_copy = pltpu.make_async_copy(hid_in, hid, isem.at[0])
    mem_copy = pltpu.make_async_copy(mem_in, mem.at[c], isem.at[1])
    mem_swap = rcopy(mem_in, mem.at[c], dtx.at[3], drx.at[3], partner)
    hid_copy.start()
    first = wcopies(0)
    for i in (WQ, WK, WV):
        first[i].start()
    mem_copy.start()
    for i in (CK, CV, WO, CQ, CO):
        first[i].start()
    for f in range(NF):
        gate_copy(0, f).start()
        up_copy(0, f).start()
    first[WD].start()

    pl.semaphore_wait(barrier, 3)
    mem_swap.start()

    length = mem_len[0]
    for b in range(KBC):
        key = z * (2 * mem_rows) + b * T + lax.broadcasted_iota(jnp.int32, (T, 128), 0)
        lane = lax.broadcasted_iota(jnp.int32, (T, 128), 1)
        bias[b] = jnp.where(jnp.logical_and(lane == 0, key >= length), NEG, 0.0).astype(BF16)

    hid_copy.wait()

    def gain(ref, l):
        g = jnp.zeros((1, D), F32)
        for i in range(n_layers):
            g = jnp.where(l == i, ref[i:i + 1, :].astype(F32), g)
        return g

    def kv_block(x, wk_ref, wv_ref, kdst, vdst, b):
        k = dot(x, wk_ref[...]).astype(BF16)
        for p in range(NP):
            kdst[b, p] = k[:, p * 128:(p + 1) * 128]
        v = dot(x, wv_ref[...])
        for p in range(NP):
            vdst[b, p] = jnp.transpose(v[:, p * 128:(p + 1) * 128]).astype(BF16)

    def memory_block(b, _):
        per = mem_rows // T
        at = pl.ds(pl.multiple_of(lax.rem(b, per) * T, T), T)
        kv_block(mem[b // per, at, :], ck, cv, kc, vc, b)
        return 0

    def rows_of(a):
        return jnp.transpose(a.astype(F32)).astype(BF16)

    def swap_project(k, w_ref, ready):
        swap = rcopy(a_half.at[k, 1 - c], att.at[k], dtx.at[k], drx.at[k], partner)
        swap.start()
        ready.wait()
        own = rows_of(a_half[k, c])
        upd[...] = hid[...].astype(F32) + dot(own, w_ref[pl.ds(my_cols, Dc), :])
        swap.wait()
        hid[...] = (upd[...] + dot(rows_of(att[k]), w_ref[pl.ds(other_cols, Dc), :])).astype(BF16)

    group_of = table(GROUPS + GROUPS[-1:], 6)
    count_of = table(COUNTS, 6)
    arrival_of = table(ARRIVALS, 6)
    return_of = table(RETURNS, 6)
    last_of = table(LAST, 9)

    def layer_body(l, carry):
        more = l + 1 < n_layers
        cur = wcopies(l)
        nxt = wcopies(jnp.minimum(l + 1, n_layers - 1))

        def prefetch(*ids):
            @pl.when(more)
            def _():
                for i in ids:
                    nxt[i].start()

        x_all[z, pl.ds(my_rows, rows), :] = rms_norm(hid[...], gain(g_self, l))

        def xslot(o, h):
            return x_all.at[o, pl.ds(pl.multiple_of(c * rows + h * half, half), half), :]

        def pslot(o, h):
            return x_all.at[o, pl.ds(pl.multiple_of((1 - c) * rows + h * half, half), half), :]

        for h in range(2):
            src = xslot(z, h)
            for d in range(2):
                rcopy(src, src, xtx.at[d, 0, h], xrx.at[d, 1, h], nbr(d)).start()
            rcopy(src, src, ptx.at[z, h], prx.at[z, h], partner).start()

        def x_event(d, s, h):
            o = ring(-(1 - 2 * d) * s)
            src = xslot(o, h)

            @pl.when(jnp.logical_or(s <= 3, h == d))
            def _():
                rcopy(src, src, xtx.at[d, s, h], xrx.at[d, s, h], nbr(d)).wait_recv()

                @pl.when(jnp.logical_or(s < 3, jnp.logical_and(s == 3, h == d)))
                def _():
                    rcopy(src, src, xtx.at[d, s, h], xrx.at[d, s + 1, h], nbr(d)).start()
                rcopy(src, src, ptx.at[o, h], prx.at[o, h], partner).start()

        def partner_half(o):
            for h in range(2):
                dst = pslot(o, h)
                rcopy(dst, dst, ptx.at[o, h], prx.at[o, h], partner).wait_recv()

        delta = (lax.broadcasted_iota(jnp.int32, (T, T), 0) - lax.broadcasted_iota(jnp.int32, (T, T), 1))

        def attend(o, start):
            tops = {}

            def score(h):
                s = dot(ks[o, h // 2], qm[h])
                if start:
                    s = jnp.where(delta <= 0, s, NEG)
                S[0, h * T:(h + 1) * T, :] = s
                tops[h] = fold_max(s)

            def values(h):
                m = jnp.max(tops[h], axis=0, keepdims=True)
                if not start:
                    old = s_max[h:h + 1, :]
                    m = jnp.maximum(m, old)
                p = jnp.exp2((S[0, h * T:(h + 1) * T, :] - m) * c_exp)
                tot = jnp.sum(fold_sum(p), axis=0, keepdims=True)
                e = h % 2
                num = dot(vs[o, h // 2, e * 64:(e + 1) * 64, :], p.astype(BF16))
                if not start:
                    keep = jnp.exp2((old - m) * c_exp)
                    tot = tot + s_sum[h:h + 1, :] * keep
                    num = num + s_num[h] * keep
                s_max[h:h + 1, :] = m
                s_sum[h:h + 1, :] = tot
                s_num[h] = num

            n_heads = 2 * NP
            score(0)
            score(1)
            for h in range(n_heads):
                if h + 2 < n_heads:
                    score(h + 2)
                values(h)

        for i in (WQ, WK, WV):
            cur[i].wait()
        partner_half(z)
        q = dot(x_all[z], wq[...])
        for p in range(NP):
            qt = jnp.transpose(q[:, p * 128:(p + 1) * 128]).astype(BF16)
            for e in range(2):
                qm[2 * p + e] = one_head(qt, e)
        kv_block(x_all[z], wk, wv, ks, vs, z)
        attend(z, True)

        @pl.when(l == 0)
        def _():
            cur[CK].wait()
            cur[CV].wait()
            mem_copy.wait()
            mem_swap.wait()
            lax.fori_loop(0, KBC // 2, memory_block, 0)

        def attend_pair(s):
            def one(j, _):
                o = ring(s * (1 - 2 * j))

                @pl.when(o < z)
                def _():
                    attend(o, False)
                return 0

            lax.fori_loop(0, jnp.where(s == Z // 2, 1, 2), one, 0)

        def level(s, _):
            for d in range(2):
                x_event(d, s, 0)

            @pl.when(jnp.logical_and(l == 0, s == 1))
            def _():
                lax.fori_loop(KBC // 2, KBC, memory_block, 0)

            @pl.when(s >= 2)
            def _():
                attend_pair(s - 1)
            for d in range(2):
                x_event(d, s, 1)

            def block(j, _):
                o = ring(s * (1 - 2 * j))
                partner_half(o)

                @pl.when(o < z)
                def _():
                    kv_block(x_all[o], wk, wv, ks, vs, o)
                return 0

            lax.fori_loop(0, jnp.where(s == Z // 2, 1, 2), block, 0)

            @pl.when(s == Z // 2)
            def _():
                attend_pair(s)
            return 0

        lax.fori_loop(1, Z // 2 + 1, level, 0)
        prefetch(WK, WQ, WV)

        @pl.when(l == 0)
        def _():
            prefetch(CK, CV)

        for h in range(2 * NP):
            a = (s_num[h] / s_sum[h:h + 1, :]).astype(BF16)
            for j in range(2):
                a_half[0, j, h * 64:(h + 1) * 64, :] = a[:, j * 128:(j + 1) * 128]
        swap_project(0, wo, cur[WO])
        prefetch(WO)

        xc[c] = rms_norm(hid[...], gain(g_cross, l))
        swap = rcopy(xc.at[c], xc.at[c], dtx.at[2], drx.at[2], partner)
        swap.start()

        for h in range(2):
            for d in range(2):
                for s in range(4):
                    if s < 3 or h == d:
                        src = xslot(z, h)
                        rcopy(src, src, xtx.at[d, s, h], xrx.at[d, s, h], nbr(d)).wait_send()
            for o in range(Z):
                src = xslot(o, h)
                rcopy(src, src, ptx.at[o, h], prx.at[o, h], partner).wait_send()

        def project_q(i):
            q = dot(xc[i], cq[...])
            at = pl.ds(pl.multiple_of(i * rows, rows), rows)
            for p in range(NP):
                q_all[z, p, :, at] = jnp.transpose(q[:, p * 128:(p + 1) * 128]).astype(BF16)

        cur[CQ].wait()
        project_q(c)
        swap.wait()
        project_q(1 - c)
        prefetch(CQ)

        def q_own(p):
            for d in range(2):
                src = q_all.at[z, p]
                rcopy(src, src, qtx.at[d, 0, p], qrx.at[d, 1, p], nbr(d)).start()

        def arrival(i, _):
            s, d, p = decode(arrival_of(i))

            @pl.when(s == 0)
            def _():
                q_own(p)

            @pl.when(s >= 1)
            def _():
                src = q_all.at[ring(-(1 - 2 * d) * s), p]
                rcopy(src, src, qtx.at[d, s, p], qrx.at[d, s, p], nbr(d)).wait_recv()

                @pl.when(jnp.logical_or(s < 3, jnp.logical_and(s == 3, lax.rem(p, 2) == d)))
                def _():
                    rcopy(src, src, qtx.at[d, s, p], qrx.at[d, s + 1, p], nbr(d)).start()
            return 0

        one = ones_row(T)

        def head_rhs(o, p, e):
            return jnp.concatenate([one_head(q_all[o, p], e), one], axis=0)

        def keys_of(p):
            return lambda b: jnp.concatenate([kc[b, p], bias[b]], axis=1)

        def place(s, d, p):
            return p * 8 + jnp.where(s == 0, 0, jnp.where(s == 4, 7, 2 * s - 1 + d))

        def origin(s, d):
            return ring(jnp.where(d == 0, -s, s))

        def cross_groups(*groups):
            where = [(origin(s, d), p, place(s, d, p)) for s, d, p in groups]
            heads = [(w, e) for w in where[:-1] for e in range(2)] + [(where[-1], 0)]
            top = top_s[...]
            stats = []
            for ((o, p, to), e), ((on, pn, _), en) in zip(heads, heads[1:]):
                top, num, l, m = score_and_sum(
                    S, en, keys_of(pn), head_rhs(on, pn, en),
                    e, lambda b: vc[b, p, e * 64:(e + 1) * 64, :], top, KBC, c_exp)
                part[to, e * 64:(e + 1) * 64, :] = num
                stats.append((m, l))
                if e == 1:
                    part_ml[to] = jnp.concatenate(
                        [x[k][:, j * 128:(j + 1) * 128] for k in range(2) for j in range(2) for x in stats[-2:]], axis=0)
            top_s[...] = top

        def incoming(d, s, p):
            rcopy(o_send.at[d, s, p], o_recv.at[d, s, p], otx.at[d, s, p], orx.at[d, s, p], nbr(d)).wait_recv()
            rcopy(ml_send.at[d, s, p], ml_recv.at[d, s, p], mtx.at[d, s, p], mrx.at[d, s, p], nbr(d)).wait_recv()

        def scales(mls):
            m = functools.reduce(jnp.maximum, [x[0:4] for x in mls])
            w = [jnp.exp2((x[0:4] - m) * c_exp) for x in mls]
            return w, m, sum(x[4:8] * y for x, y in zip(mls, w))

        def tile(ref, e, j):
            return ref[e * 64:(e + 1) * 64, j * 128:(j + 1) * 128].astype(F32)

        def reduce_step(v):
            s, d_arr, p = decode(v)
            at = place(s, d_arr, p)
            d = jnp.where(s == 4, lax.rem(p, 2), 1 - d_arr)
            has_in = jnp.logical_and(s >= 1, jnp.logical_or(s < 3, jnp.logical_and(s == 3, lax.rem(p, 2) == d)))
            to = jnp.maximum(s - 1, 0)

            @pl.when(has_in)
            def _():
                incoming(d, s, p)
                (wa, wb), m, l = scales([part_ml[at], ml_recv[d, s, p]])
                ml_send[d, to, p] = jnp.concatenate([m, l], axis=0)
                for e in range(2):
                    for j in range(2):
                        r = slice(2 * j + e, 2 * j + e + 1)
                        o_send[d, to, p, e * 64:(e + 1) * 64, j * 128:(j + 1) * 128] = (
                            tile(part.at[at], e, j) * wa[r] + tile(o_recv.at[d, s, p], e, j) * wb[r]).astype(BF16)

            @pl.when(jnp.logical_and(s >= 1, jnp.logical_not(has_in)))
            def _():
                o_send[d, to, p] = part[at].astype(BF16)
                ml_send[d, to, p] = part_ml[at]

            @pl.when(s >= 1)
            def _():
                rcopy(ml_send.at[d, to, p], ml_recv.at[d, to, p], mtx.at[d, to, p], mrx.at[d, to, p], nbr(d)).start()
                rcopy(o_send.at[d, to, p], o_recv.at[d, to, p], otx.at[d, to, p], orx.at[d, to, p], nbr(d)).start()

            @pl.when(s == 0)
            def _():
                for dd in range(2):
                    incoming(dd, 0, p)
                w, m, l = scales([part_ml[at], ml_recv[0, 0, p], ml_recv[1, 0, p]])
                to_rows = pl.multiple_of(p * 128, 128)
                for e in range(2):
                    for j in range(2):
                        r = slice(2 * j + e, 2 * j + e + 1)
                        tot = (tile(part.at[at], e, j) * w[0][r] + tile(o_recv.at[0, 0, p], e, j) * w[1][r]
                               + tile(o_recv.at[1, 0, p], e, j) * w[2][r])
                        a_half[1, j, pl.ds(to_rows + e * 64, 64), :] = (tot / l[r]).astype(BF16)

        q_own(0)
        q_own(1)
        top_s[...] = score_all(S, 0, keys_of(GROUPS[0] // 16), head_rhs(z, GROUPS[0] // 16, 0), KBC)

        def step(k, at):
            ia, ir = at
            n = count_of(k)
            ja, jr = ia + lax.rem(n, 8), ir + n // 8
            lax.fori_loop(ia, ja, arrival, 0)

            def ret(i, _):
                reduce_step(return_of(i))
                return 0

            lax.fori_loop(ir, jr, ret, 0)
            cross_groups(*(decode(group_of(2 * k + i)) for i in range(3)))
            return ja, jr

        lax.fori_loop(0, len(COUNTS), step, (jnp.int32(0), jnp.int32(0)))

        @pl.when(more)
        def _():
            nxt[CK].wait()
            nxt[CV].wait()

        def finish(i, b):
            v = last_of(i)
            n = jnp.where(more, v // 64, 0)
            lax.fori_loop(b, jnp.minimum(b + n, KBC), memory_block, 0)
            reduce_step(lax.rem(v, 64))
            return b + n

        lax.fori_loop(0, len(LAST), finish, jnp.int32(0))

        @pl.when(l + 2 < n_layers)
        def _():
            after = wcopies(jnp.minimum(l + 2, n_layers - 1))
            after[CK].start()
            after[CV].start()

        swap_project(1, co, cur[CO])
        prefetch(CO)

        xm = rms_norm(hid[...], gain(g_mlp, l))

        for p in range(NP):
            for d in range(2):
                for s in range(4):
                    if s < 3 or p % 2 == d:
                        src = q_all.at[z, p]
                        rcopy(src, src, qtx.at[d, s, p], qrx.at[d, s, p], nbr(d)).wait_send()
                        rcopy(o_send.at[d, s, p], o_recv.at[d, s, p], otx.at[d, s, p], orx.at[d, s, p], nbr(d)).wait_send()
                        rcopy(ml_send.at[d, s, p], ml_recv.at[d, s, p], mtx.at[d, s, p], mrx.at[d, s, p], nbr(d)).wait_send()

        for f in range(NF):
            gate_copy(l, f).wait()
            up_copy(l, f).wait()
        cur[WD].wait()
        acts = []
        for f in range(NF):
            gt = dot(xm, wg[f])
            up = dot(xm, wu[f])
            acts.append((gt * lax.logistic(gt) * up).astype(BF16))
        full = jnp.concatenate(acts, axis=1)

        @pl.when(more)
        def _():
            for f in range(NF):
                gate_copy(l + 1, f).start()
                up_copy(l + 1, f).start()
        for n in range(D // T):
            cols = slice(n * T, (n + 1) * T)
            hid[:, cols] = (hid[:, cols].astype(F32) + dot(full, wd[:, cols])).astype(BF16)
        prefetch(WD)
        return carry

    lax.fori_loop(0, n_layers, layer_body, 0)
    out[...] = hid[...]


def solution(mesh):
    n_dev = mesh.shape["sp"]

    def local_step(hidden, memory, mem_len, norm_self, norm_cross, norm_mlp, self_q, self_k, self_v, self_o,
                   cross_q, cross_k, cross_v, cross_o, mlp_gate, mlp_up, mlp_down):
        rows, D = hidden.shape
        mem_rows = memory.shape[0]
        L, heads, head_dim = self_o.shape[:3]
        FF = mlp_gate.shape[2]
        Dc = D // 2
        NP = Dc // 128
        Z = n_dev // 2
        KBC = 2 * mem_rows // T
        NF = FF // T
        any_ = pl.BlockSpec(memory_space=pl.ANY)
        vmem = pl.BlockSpec(memory_space=pltpu.VMEM)
        smem = pl.BlockSpec(memory_space=pltpu.SMEM)
        dma = pltpu.SemaphoreType.DMA
        V = pltpu.VMEM
        scratch = [
            V((rows, D), BF16),
            V((Z, 2 * rows, D), BF16),
            V((2, mem_rows, D), BF16),
            V((Z, NP, T, 128), BF16),
            V((Z, NP, 128, T), BF16),
            V((KBC, NP, T, 128), BF16),
            V((KBC, NP, 128, T), BF16),
            V((KBC, T, 128), BF16),
            V((2 * NP, 128, T), BF16),
            V((Z, NP, 128, T), BF16),
            V((2, max(2 * NP, KBC) * T, T), F32),
            V((8, T), F32),
            V((D, Dc), BF16), V((D, Dc), BF16), V((D, Dc), BF16), V((D, D), BF16),
            V((D, Dc), BF16), V((D, Dc), BF16), V((D, Dc), BF16), V((D, D), BF16),
            V((NF, D, T), BF16), V((NF, D, T), BF16), V((FF, D), BF16),
            V((8 * NP, 128, T), F32),
            V((8 * NP, 8, 128), F32),
            V((2, 4, NP, 128, T), BF16),
            V((2, 4, NP, 8, 128), F32),
            V((2, 4, NP, 128, T), BF16),
            V((2, 4, NP, 8, 128), F32),
            V((2 * NP, 64, T), F32),
            V((8, T), F32), V((8, T), F32),
            V((2, 2, Dc, 128), BF16),
            V((2, Dc, 128), BF16),
            V((rows, D), F32),
            V((2, rows, D), BF16),
            dma((2, 5, 2)), dma((2, 5, 2)), dma((Z, 2)), dma((Z, 2)),
            dma((2, 5, NP)), dma((2, 5, NP)),
            dma((2, 4, NP)), dma((2, 4, NP)), dma((2, 4, NP)), dma((2, 4, NP)),
            dma((4,)), dma((4,)), dma((9,)), dma((NF,)), dma((NF,)), dma((2,)),
        ]
        call = pl.pallas_call(
            functools.partial(kernel, n_dev, head_dim, L),
            out_shape=jax.ShapeDtypeStruct((rows, D), BF16),
            in_specs=[smem, any_, any_, vmem, vmem, vmem] + [any_] * 11,
            out_specs=vmem,
            scratch_shapes=scratch,
            compiler_params=pltpu.CompilerParams(
                collective_id=0, has_side_effects=True, vmem_limit_bytes=67043328),
            name="decoder",
        )
        return call(mem_len, hidden, memory, norm_self, norm_cross, norm_mlp,
                    self_q, self_k, self_v, self_o.reshape(L, D, D), cross_q, cross_k, cross_v,
                    cross_o.reshape(L, D, D), mlp_gate, mlp_up, mlp_down)

    row_spec = P(("dp", "sp"), None)
    return jax.shard_map(local_step, mesh=mesh, in_specs=(row_spec, row_spec, P("dp")) + (P(),) * 14,
                         out_specs=row_spec, check_vma=False)
```

```python
import functools
import math

import jax
import jax.numpy as jnp
from jax import lax
from jax.experimental import pallas as pl
from jax.experimental.pallas import tpu as pltpu
from jax.sharding import PartitionSpec as P

MESH = pl.DeviceIdType.MESH
EPS = 1e-6
NEG = -1e30
T = 256
F32 = jnp.float32
BF16 = jnp.bfloat16

def unpack(bits, count, *words):
    per = 84 // bits
    return [(words[i // per] >> (i % per * bits)) % 2 ** bits for i in range(count)]


GROUPS = unpack(6, 32, 0xc9a48a0a1a51649050800, 0xeb3ad3f3b91c11b8cb0ea, 0xc798b0)
ARRIVALS = unpack(6, 30, 0x692282e71a61651241c20, 0xef3704ae36d32c3eb28aa, 0xf24)
RETURNS = unpack(6, 20, 0xada4fb07c2e471b0848c3, 0xe92662cca)
COUNTS = unpack(6, 16, 0x62045930a102102102100, 0x810)
LAST = unpack(9, 12, 0x100149c4725110a24642a, 0x806010)


def table(values, bits):
    per = 30 // bits
    words = [sum(v << (bits * j) for j, v in enumerate(values[i:i + per])) for i in range(0, len(values), per)]

    def get(i):
        w = jnp.int32(words[0])
        for k, v in enumerate(words[1:], 1):
            w = jnp.where(i >= k * per, jnp.int32(v), w)
        return lax.rem(lax.shift_right_logical(w, lax.rem(i, per) * bits), 1 << bits)

    return get


def decode(v):
    return lax.rem(v, 8), lax.rem(v // 8, 2), lax.rem(v // 16, 4)


def dot(a, b):
    return jnp.dot(a, b, preferred_element_type=F32)


def fold_max(x):
    return jnp.max(x.reshape(x.shape[0] // 8, 8, x.shape[1]), axis=0)


def fold_sum(x):
    return jnp.sum(x.reshape(x.shape[0] // 8, 8, x.shape[1]), axis=0)


def one_head(qt, e):
    rest = jnp.zeros((64, qt.shape[1]), BF16)
    return jnp.concatenate([qt[0:64], rest] if e == 0 else [rest, qt[64:128]], axis=0)


def ones_row(cols):
    row = lax.broadcasted_iota(jnp.int32, (128, cols), 0)
    return jnp.where(row == 0, 1.0, 0.0).astype(BF16)


def scores(S, slot, keys, rhs, b):
    s = dot(keys(b), rhs)
    S[slot, b * T:(b + 1) * T, :] = s
    return fold_max(s)


def score_all(S, slot, keys, rhs, blocks):
    return functools.reduce(jnp.maximum, [scores(S, slot, keys, rhs, b) for b in range(blocks)])


def score_and_sum(S, slot, keys, rhs, slot_v, values, top, blocks, c):
    ahead = min(3, blocks)
    m = jnp.max(top, axis=0, keepdims=True)
    tops = [scores(S, slot, keys, rhs, b) for b in range(ahead)]
    part = jnp.zeros((8, T), F32)
    num = jnp.zeros((64, T), F32)
    for b in range(blocks):
        p = jnp.exp2((S[slot_v, b * T:(b + 1) * T, :] - m) * c)
        part = part + fold_sum(p)
        num = num + dot(values(b), p.astype(BF16))
        if b + ahead < blocks:
            tops.append(scores(S, slot, keys, rhs, b + ahead))
    return functools.reduce(jnp.maximum, tops), num, jnp.sum(part, axis=0, keepdims=True), m


def rms_norm(h, g):
    h = h.astype(F32)
    inv = lax.rsqrt(jnp.mean(h * h, axis=-1, keepdims=True) + EPS)
    return (h * inv * g).astype(BF16)


def kernel(n_dev, head_dim, n_layers,
           mem_len, hid_in, mem_in, g_self, g_cross, g_mlp,
           self_q, self_k, self_v, self_o, cross_q, cross_k, cross_v, cross_o, mlp_g, mlp_u, mlp_d,
           out,
           hid, x_all, mem, ks, vs, kc, vc, bias, qm, q_all, S, top_s,
           wq, wk, wv, wo, cq, ck, cv, co, wg, wu, wd,
           part, part_ml, o_send, ml_send, o_recv, ml_recv,
           s_num, s_max, s_sum, a_half, att, upd, xc,
           xtx, xrx, ptx, prx, qtx, qrx, otx, orx, mtx, mrx, ctx, crx, dtx, drx, wsem, gsem, usem, isem):
    Z = n_dev // 2
    rows, D = hid.shape
    half = rows // 2
    NP = q_all.shape[1]
    KBC = kc.shape[0]
    NF = wg.shape[0]
    Dc = D // 2
    mem_rows = mem_in.shape[0]
    c_exp = math.log2(math.e) * head_dim ** -0.5

    me = lax.axis_index("sp")
    z = me // 2
    c = me % 2
    partner = z * 2 + (1 - c)

    def ring(k):
        return lax.rem(z + k * (1 - 2 * c) + 2 * Z, Z)

    def nbr(d):
        return ring(1 - 2 * d) * 2 + c

    def rcopy(src, dst, ssem, rsem, dev):
        return pltpu.make_async_remote_copy(src_ref=src, dst_ref=dst, send_sem=ssem, recv_sem=rsem,
                                            device_id={"sp": dev}, device_id_type=MESH)

    my_rows = pl.multiple_of(c * rows, rows)
    my_cols = pl.multiple_of(c * Dc, Dc)
    other_cols = pl.multiple_of((1 - c) * Dc, Dc)

    barrier = pltpu.get_barrier_semaphore()
    for dev in (nbr(0), nbr(1), partner):
        pl.semaphore_signal(barrier, inc=1, device_id={"sp": dev}, device_id_type=MESH)

    def wcopies(l):
        cols = pl.ds(my_cols, Dc)
        w = [
            (self_k.at[l, :, cols], wk), (self_q.at[l, :, cols], wq), (self_v.at[l, :, cols], wv),
            (cross_k.at[l, :, cols], ck), (cross_v.at[l, :, cols], cv),
            (self_o.at[l], wo), (cross_q.at[l, :, cols], cq), (cross_o.at[l], co), (mlp_d.at[l], wd),
        ]
        return [pltpu.make_async_copy(s, d, wsem.at[i]) for i, (s, d) in enumerate(w)]

    WK, WQ, WV, CK, CV, WO, CQ, CO, WD = range(9)

    def gate_copy(l, f):
        return pltpu.make_async_copy(mlp_g.at[l, :, pl.ds(f * T, T)], wg.at[f], gsem.at[f])

    def up_copy(l, f):
        return pltpu.make_async_copy(mlp_u.at[l, :, pl.ds(f * T, T)], wu.at[f], usem.at[f])

    hid_copy = pltpu.make_async_copy(hid_in, hid, isem.at[0])
    mem_copy = pltpu.make_async_copy(mem_in, mem.at[c], isem.at[1])
    mem_swap = rcopy(mem_in, mem.at[c], dtx.at[3], drx.at[3], partner)
    hid_copy.start()
    first = wcopies(0)
    for i in (WQ, WK, WV):
        first[i].start()
    mem_copy.start()
    for i in (CK, CV, WO, CQ, CO):
        first[i].start()
    for f in range(NF):
        gate_copy(0, f).start()
        up_copy(0, f).start()
    first[WD].start()

    pl.semaphore_wait(barrier, 3)
    hid_copy.wait()

    def gain(ref, l):
        g = jnp.zeros((1, D), F32)
        for i in range(n_layers):
            g = jnp.where(l == i, ref[i:i + 1, :].astype(F32), g)
        return g

    def kv_block(x, wk_ref, wv_ref, kdst, vdst, b):
        v = dot(x, wv_ref[...])
        k = dot(x, wk_ref[...]).astype(BF16)
        for p in range(NP):
            vdst[b, p] = jnp.transpose(v[:, p * 128:(p + 1) * 128]).astype(BF16)
        for p in range(NP):
            kdst[b, p] = k[:, p * 128:(p + 1) * 128]

    def memory_block(b, _):
        per = mem_rows // T
        at = pl.ds(pl.multiple_of(lax.rem(b, per) * T, T), T)
        kv_block(mem[b // per, at, :], ck, cv, kc, vc, b)
        return 0

    def key_mask():
        length = mem_len[0]
        for b in range(KBC):
            key = z * (2 * mem_rows) + b * T + lax.broadcasted_iota(jnp.int32, (T, 128), 0)
            lane = lax.broadcasted_iota(jnp.int32, (T, 128), 1)
            bias[b] = jnp.where(jnp.logical_and(lane == 0, key >= length), NEG, 0.0).astype(BF16)

    def rows_of(a):
        return jnp.transpose(a.astype(F32)).astype(BF16)

    def swap_project(w_ref, ready):
        swap = rcopy(a_half.at[0, 1 - c], att.at[0], dtx.at[0], drx.at[0], partner)
        swap.start()
        ready.wait()
        own = rows_of(a_half[0, c])
        upd[...] = hid[...].astype(F32) + dot(own, w_ref[pl.ds(my_cols, Dc), :])
        swap.wait()
        hid[...] = (upd[...] + dot(rows_of(att[0]), w_ref[pl.ds(other_cols, Dc), :])).astype(BF16)

    def pair_rows(p):
        return pl.ds(pl.multiple_of(p * 128, 128), 128)

    def pair_swap(p):
        return rcopy(a_half.at[1, 1 - c, pair_rows(p)], att.at[1, pair_rows(p)], ctx.at[p], crx.at[p], partner)

    def pair_project(a, base, p):
        w = co[pl.ds(pl.multiple_of(base + p * 128, 128), 128), :]
        upd[...] += dot(rows_of(a), w)

    group_of = table(GROUPS + GROUPS[-1:], 6)
    count_of = table(COUNTS, 6)
    arrival_of = table(ARRIVALS, 6)
    return_of = table(RETURNS, 6)
    last_of = table(LAST, 9)

    def layer_body(l, carry):
        more = l + 1 < n_layers
        cur = wcopies(l)
        nxt = wcopies(jnp.minimum(l + 1, n_layers - 1))

        def prefetch(*ids):
            @pl.when(more)
            def _():
                for i in ids:
                    nxt[i].start()

        x_all[z, pl.ds(my_rows, rows), :] = rms_norm(hid[...], gain(g_self, l))

        def xslot(o, h):
            return x_all.at[o, pl.ds(pl.multiple_of(c * rows + h * half, half), half), :]

        def pslot(o, h):
            return x_all.at[o, pl.ds(pl.multiple_of((1 - c) * rows + h * half, half), half), :]

        for h in range(2):
            src = xslot(z, h)
            for d in range(2):
                rcopy(src, src, xtx.at[d, 0, h], xrx.at[d, 1, h], nbr(d)).start()
            rcopy(src, src, ptx.at[z, h], prx.at[z, h], partner).start()

        @pl.when(l == 0)
        def _():
            mem_swap.start()
            key_mask()

        def x_event(d, s, h):
            o = ring(-(1 - 2 * d) * s)
            src = xslot(o, h)

            @pl.when(jnp.logical_or(s <= 3, h == d))
            def _():
                rcopy(src, src, xtx.at[d, s, h], xrx.at[d, s, h], nbr(d)).wait_recv()

                @pl.when(jnp.logical_or(s < 3, jnp.logical_and(s == 3, h == d)))
                def _():
                    rcopy(src, src, xtx.at[d, s, h], xrx.at[d, s + 1, h], nbr(d)).start()
                rcopy(src, src, ptx.at[o, h], prx.at[o, h], partner).start()

        def partner_half(o):
            for h in range(2):
                dst = pslot(o, h)
                rcopy(dst, dst, ptx.at[o, h], prx.at[o, h], partner).wait_recv()

        delta = (lax.broadcasted_iota(jnp.int32, (T, T), 0) - lax.broadcasted_iota(jnp.int32, (T, T), 1))

        def attend(o, start):
            tops = {}

            def score(h):
                s = dot(ks[o, h // 2], qm[h])
                if start:
                    s = jnp.where(delta <= 0, s, NEG)
                S[0, h * T:(h + 1) * T, :] = s
                tops[h] = fold_max(s)

            def values(h):
                m = jnp.max(tops[h], axis=0, keepdims=True)
                if not start:
                    old = s_max[h:h + 1, :]
                    m = jnp.maximum(m, old)
                p = jnp.exp2((S[0, h * T:(h + 1) * T, :] - m) * c_exp)
                tot = jnp.sum(fold_sum(p), axis=0, keepdims=True)
                e = h % 2
                num = dot(vs[o, h // 2, e * 64:(e + 1) * 64, :], p.astype(BF16))
                if not start:
                    keep = jnp.exp2((old - m) * c_exp)
                    tot = tot + s_sum[h:h + 1, :] * keep
                    num = num + s_num[h] * keep
                s_max[h:h + 1, :] = m
                s_sum[h:h + 1, :] = tot
                s_num[h] = num

            for h in range(2 * NP):
                score(h)
            for h in range(2 * NP):
                values(h)

        for i in (WQ, WK, WV):
            cur[i].wait()
        partner_half(z)
        q = dot(x_all[z], wq[...])
        for p in range(NP):
            qt = jnp.transpose(q[:, p * 128:(p + 1) * 128]).astype(BF16)
            for e in range(2):
                qm[2 * p + e] = one_head(qt, e)
        kv_block(x_all[z], wk, wv, ks, vs, z)
        attend(z, True)

        def memory_part(i):
            @pl.when(l == 0)
            def _():
                @pl.when(i == 0)
                def _():
                    cur[CK].wait()
                    cur[CV].wait()
                    mem_copy.wait()
                    mem_swap.wait()
                lax.fori_loop(KBC * i // 4, KBC * (i + 1) // 4, memory_block, 0)

        def attend_pair(s):
            def one(j, _):
                o = ring(s * (1 - 2 * j))

                @pl.when(o < z)
                def _():
                    attend(o, False)
                return 0

            lax.fori_loop(0, jnp.where(s == Z // 2, 1, 2), one, 0)

        def level(s, _):
            for d in range(2):
                x_event(d, s, 0)

            @pl.when(s == 1)
            def _():
                memory_part(0)

            @pl.when(s >= 2)
            def _():
                attend_pair(s - 1)
            for d in range(2):
                x_event(d, s, 1)

            def block(j, _):
                o = ring(s * (1 - 2 * j))
                partner_half(o)

                @pl.when(o < z)
                def _():
                    kv_block(x_all[o], wk, wv, ks, vs, o)
                return 0

            lax.fori_loop(0, jnp.where(s == Z // 2, 1, 2), block, 0)

            @pl.when(s == Z // 2)
            def _():
                attend_pair(s)

            @pl.when(s < Z // 2)
            def _():
                memory_part(s)
            return 0

        lax.fori_loop(1, Z // 2 + 1, level, 0)
        prefetch(WK, WQ, WV)

        @pl.when(l == 0)
        def _():
            prefetch(CK, CV)

        for h in range(2 * NP):
            a = (s_num[h] / s_sum[h:h + 1, :]).astype(BF16)
            for j in range(2):
                a_half[0, j, h * 64:(h + 1) * 64, :] = a[:, j * 128:(j + 1) * 128]
        swap_project(wo, cur[WO])
        prefetch(WO)

        xc[c] = rms_norm(hid[...], gain(g_cross, l))
        swap = rcopy(xc.at[c], xc.at[c], dtx.at[2], drx.at[2], partner)
        swap.start()

        for h in range(2):
            for d in range(2):
                for s in range(4):
                    if s < 3 or h == d:
                        src = xslot(z, h)
                        rcopy(src, src, xtx.at[d, s, h], xrx.at[d, s, h], nbr(d)).wait_send()
            for o in range(Z):
                src = xslot(o, h)
                rcopy(src, src, ptx.at[o, h], prx.at[o, h], partner).wait_send()

        def project_q(i):
            q = dot(xc[i], cq[...])
            at = pl.ds(pl.multiple_of(i * rows, rows), rows)
            for p in range(NP):
                q_all[z, p, :, at] = jnp.transpose(q[:, p * 128:(p + 1) * 128]).astype(BF16)

        cur[CQ].wait()
        project_q(c)
        swap.wait()
        project_q(1 - c)
        prefetch(CQ)

        def q_own(p):
            for d in range(2):
                src = q_all.at[z, p]
                rcopy(src, src, qtx.at[d, 0, p], qrx.at[d, 1, p], nbr(d)).start()

        def arrival(i, _):
            s, d, p = decode(arrival_of(i))

            @pl.when(s == 0)
            def _():
                q_own(p)

            @pl.when(s >= 1)
            def _():
                src = q_all.at[ring(-(1 - 2 * d) * s), p]
                rcopy(src, src, qtx.at[d, s, p], qrx.at[d, s, p], nbr(d)).wait_recv()

                @pl.when(jnp.logical_or(s < 3, jnp.logical_and(s == 3, lax.rem(p, 2) == d)))
                def _():
                    rcopy(src, src, qtx.at[d, s, p], qrx.at[d, s + 1, p], nbr(d)).start()
            return 0

        one = ones_row(T)

        def head_rhs(o, p, e):
            return jnp.concatenate([one_head(q_all[o, p], e), one], axis=0)

        def keys_of(p):
            return lambda b: jnp.concatenate([kc[b, p], bias[b]], axis=1)

        def place(s, d, p):
            return p * 8 + jnp.where(s == 0, 0, jnp.where(s == 4, 7, 2 * s - 1 + d))

        def origin(s, d):
            return ring(jnp.where(d == 0, -s, s))

        def cross_groups(*groups):
            where = [(origin(s, d), p, place(s, d, p)) for s, d, p in groups]
            heads = [(w, e) for w in where[:-1] for e in range(2)] + [(where[-1], 0)]
            top = top_s[...]
            stats = []
            for ((o, p, to), e), ((on, pn, _), en) in zip(heads, heads[1:]):
                top, num, l, m = score_and_sum(
                    S, en, keys_of(pn), head_rhs(on, pn, en),
                    e, lambda b: vc[b, p, e * 64:(e + 1) * 64, :], top, KBC, c_exp)
                part[to, e * 64:(e + 1) * 64, :] = num
                stats.append((m, l))
                if e == 1:
                    part_ml[to] = jnp.concatenate(
                        [x[k][:, j * 128:(j + 1) * 128] for k in range(2) for j in range(2) for x in stats[-2:]], axis=0)
            top_s[...] = top

        def incoming(d, s, p):
            rcopy(o_send.at[d, s, p], o_recv.at[d, s, p], otx.at[d, s, p], orx.at[d, s, p], nbr(d)).wait_recv()
            rcopy(ml_send.at[d, s, p], ml_recv.at[d, s, p], mtx.at[d, s, p], mrx.at[d, s, p], nbr(d)).wait_recv()

        def scales(mls):
            m = functools.reduce(jnp.maximum, [x[0:4] for x in mls])
            w = [jnp.exp2((x[0:4] - m) * c_exp) for x in mls]
            return w, m, sum(x[4:8] * y for x, y in zip(mls, w))

        def tile(ref, e, j):
            return ref[e * 64:(e + 1) * 64, j * 128:(j + 1) * 128].astype(F32)

        def reduce_step(v):
            s, d_arr, p = decode(v)
            at = place(s, d_arr, p)
            d = jnp.where(s == 4, lax.rem(p, 2), 1 - d_arr)
            has_in = jnp.logical_and(s >= 1, jnp.logical_or(s < 3, jnp.logical_and(s == 3, lax.rem(p, 2) == d)))
            to = jnp.maximum(s - 1, 0)

            @pl.when(has_in)
            def _():
                incoming(d, s, p)
                (wa, wb), m, l = scales([part_ml[at], ml_recv[d, s, p]])
                ml_send[d, to, p] = jnp.concatenate([m, l], axis=0)
                for e in range(2):
                    for j in range(2):
                        r = slice(2 * j + e, 2 * j + e + 1)
                        o_send[d, to, p, e * 64:(e + 1) * 64, j * 128:(j + 1) * 128] = (
                            tile(part.at[at], e, j) * wa[r] + tile(o_recv.at[d, s, p], e, j) * wb[r]).astype(BF16)

            @pl.when(jnp.logical_and(s >= 1, jnp.logical_not(has_in)))
            def _():
                o_send[d, to, p] = part[at].astype(BF16)
                ml_send[d, to, p] = part_ml[at]

            @pl.when(s >= 1)
            def _():
                rcopy(ml_send.at[d, to, p], ml_recv.at[d, to, p], mtx.at[d, to, p], mrx.at[d, to, p], nbr(d)).start()
                rcopy(o_send.at[d, to, p], o_recv.at[d, to, p], otx.at[d, to, p], orx.at[d, to, p], nbr(d)).start()

            @pl.when(s == 0)
            def _():
                for dd in range(2):
                    incoming(dd, 0, p)
                w, m, l = scales([part_ml[at], ml_recv[0, 0, p], ml_recv[1, 0, p]])
                to_rows = pl.multiple_of(p * 128, 128)
                for e in range(2):
                    for j in range(2):
                        r = slice(2 * j + e, 2 * j + e + 1)
                        tot = (tile(part.at[at], e, j) * w[0][r] + tile(o_recv.at[0, 0, p], e, j) * w[1][r]
                               + tile(o_recv.at[1, 0, p], e, j) * w[2][r])
                        a_half[1, j, pl.ds(to_rows + e * 64, 64), :] = (tot / l[r]).astype(BF16)

        q_own(0)
        q_own(1)
        top_s[...] = score_all(S, 0, keys_of(GROUPS[0] // 16), head_rhs(z, GROUPS[0] // 16, 0), KBC)

        def step(k, at):
            ia, ir = at
            n = count_of(k)
            ja, jr = ia + lax.rem(n, 8), ir + n // 8
            lax.fori_loop(ia, ja, arrival, 0)

            def ret(i, _):
                reduce_step(return_of(i))
                return 0

            lax.fori_loop(ir, jr, ret, 0)
            cross_groups(*(decode(group_of(2 * k + i)) for i in range(3)))
            return ja, jr

        lax.fori_loop(0, len(COUNTS), step, (jnp.int32(0), jnp.int32(0)))

        @pl.when(more)
        def _():
            nxt[CK].wait()
            nxt[CV].wait()

        def finish(i, b):
            v = last_of(i)
            n = jnp.where(more, v // 64, 0)
            lax.fori_loop(b, jnp.minimum(b + n, KBC), memory_block, 0)
            reduce_step(lax.rem(v, 64))

            @pl.when(lax.rem(v, 8) == 0)
            def _():
                p = lax.rem(v // 16, 4)
                pair_swap(p).start()
                pair_project(a_half[1, c, pair_rows(p)], my_cols, p)
            return b + n

        cur[CO].wait()
        upd[...] = hid[...].astype(F32)

        lax.fori_loop(0, len(LAST), finish, jnp.int32(0))

        @pl.when(l + 2 < n_layers)
        def _():
            after = wcopies(jnp.minimum(l + 2, n_layers - 1))
            after[CK].start()
            after[CV].start()

        for v in LAST[-NP:]:
            p = v % 64 // 16
            pair_swap(p).wait()
            pair_project(att[1, pair_rows(p)], other_cols, p)
        hid[...] = upd[...].astype(BF16)
        prefetch(CO)

        xm = rms_norm(hid[...], gain(g_mlp, l))

        for p in range(NP):
            for d in range(2):
                for s in range(4):
                    if s < 3 or p % 2 == d:
                        src = q_all.at[z, p]
                        rcopy(src, src, qtx.at[d, s, p], qrx.at[d, s, p], nbr(d)).wait_send()
                        rcopy(o_send.at[d, s, p], o_recv.at[d, s, p], otx.at[d, s, p], orx.at[d, s, p], nbr(d)).wait_send()
                        rcopy(ml_send.at[d, s, p], ml_recv.at[d, s, p], mtx.at[d, s, p], mrx.at[d, s, p], nbr(d)).wait_send()

        for f in range(NF):
            gate_copy(l, f).wait()
            up_copy(l, f).wait()
        cur[WD].wait()
        acts = []
        for f in range(NF):
            gt = dot(xm, wg[f])
            up = dot(xm, wu[f])
            acts.append((gt * lax.logistic(gt) * up).astype(BF16))
        full = jnp.concatenate(acts, axis=1)

        @pl.when(more)
        def _():
            for f in range(NF):
                gate_copy(l + 1, f).start()
                up_copy(l + 1, f).start()
        for n in range(D // T):
            cols = slice(n * T, (n + 1) * T)
            hid[:, cols] = (hid[:, cols].astype(F32) + dot(full, wd[:, cols])).astype(BF16)
        prefetch(WD)
        return carry

    lax.fori_loop(0, n_layers, layer_body, 0)
    out[...] = hid[...]


def solution(mesh):
    n_dev = mesh.shape["sp"]

    def local_step(hidden, memory, mem_len, norm_self, norm_cross, norm_mlp, self_q, self_k, self_v, self_o,
                   cross_q, cross_k, cross_v, cross_o, mlp_gate, mlp_up, mlp_down):
        rows, D = hidden.shape
        mem_rows = memory.shape[0]
        L, heads, head_dim = self_o.shape[:3]
        FF = mlp_gate.shape[2]
        Dc = D // 2
        NP = Dc // 128
        Z = n_dev // 2
        KBC = 2 * mem_rows // T
        NF = FF // T
        any_ = pl.BlockSpec(memory_space=pl.ANY)
        vmem = pl.BlockSpec(memory_space=pltpu.VMEM)
        smem = pl.BlockSpec(memory_space=pltpu.SMEM)
        dma = pltpu.SemaphoreType.DMA
        V = pltpu.VMEM
        scratch = [
            V((rows, D), BF16),
            V((Z, 2 * rows, D), BF16),
            V((2, mem_rows, D), BF16),
            V((Z, NP, T, 128), BF16),
            V((Z, NP, 128, T), BF16),
            V((KBC, NP, T, 128), BF16),
            V((KBC, NP, 128, T), BF16),
            V((KBC, T, 128), BF16),
            V((2 * NP, 128, T), BF16),
            V((Z, NP, 128, T), BF16),
            V((2, max(2 * NP, KBC) * T, T), F32),
            V((8, T), F32),
            V((D, Dc), BF16), V((D, Dc), BF16), V((D, Dc), BF16), V((D, D), BF16),
            V((D, Dc), BF16), V((D, Dc), BF16), V((D, Dc), BF16), V((D, D), BF16),
            V((NF, D, T), BF16), V((NF, D, T), BF16), V((FF, D), BF16),
            V((8 * NP, 128, T), F32),
            V((8 * NP, 8, 128), F32),
            V((2, 4, NP, 128, T), BF16),
            V((2, 4, NP, 8, 128), F32),
            V((2, 4, NP, 128, T), BF16),
            V((2, 4, NP, 8, 128), F32),
            V((2 * NP, 64, T), F32),
            V((8, T), F32), V((8, T), F32),
            V((2, 2, Dc, 128), BF16),
            V((2, Dc, 128), BF16),
            V((rows, D), F32),
            V((2, rows, D), BF16),
            dma((2, 5, 2)), dma((2, 5, 2)), dma((Z, 2)), dma((Z, 2)),
            dma((2, 5, NP)), dma((2, 5, NP)),
            dma((2, 4, NP)), dma((2, 4, NP)), dma((2, 4, NP)), dma((2, 4, NP)),
            dma((NP,)), dma((NP,)),
            dma((4,)), dma((4,)), dma((9,)), dma((NF,)), dma((NF,)), dma((2,)),
        ]
        call = pl.pallas_call(
            functools.partial(kernel, n_dev, head_dim, L),
            out_shape=jax.ShapeDtypeStruct((rows, D), BF16),
            in_specs=[smem, any_, any_, vmem, vmem, vmem] + [any_] * 11,
            out_specs=vmem,
            scratch_shapes=scratch,
            compiler_params=pltpu.CompilerParams(
                collective_id=0, has_side_effects=True, vmem_limit_bytes=67043328),
            name="decoder",
        )
        return call(mem_len, hidden, memory, norm_self, norm_cross, norm_mlp,
                    self_q, self_k, self_v, self_o.reshape(L, D, D), cross_q, cross_k, cross_v,
                    cross_o.reshape(L, D, D), mlp_gate, mlp_up, mlp_down)

    row_spec = P(("dp", "sp"), None)
    return jax.shard_map(local_step, mesh=mesh, in_specs=(row_spec, row_spec, P("dp")) + (P(),) * 14,
                         out_specs=row_spec, check_vma=False)
```

```python
import functools
import math

import jax
import jax.numpy as jnp
from jax import lax
from jax.experimental import pallas as pl
from jax.experimental.pallas import tpu as pltpu
from jax.sharding import PartitionSpec as P

MESH = pl.DeviceIdType.MESH
EPS = 1e-6
NEG = -1e30
T = 256
F32 = jnp.float32
BF16 = jnp.bfloat16

def unpack(bits, count, *words):
    per = 84 // bits
    return [(words[i // per] >> (i % per * bits)) % 2 ** bits for i in range(count)]


GROUPS = unpack(6, 32, 0xe9ac790a1651260050c00, 0xaf3893f2473b10b8db0ca, 0xcaaa52)
ARRIVALS = unpack(6, 30, 0x89229a0b1e61651241830, 0xf1caa4ec48cb4f20dbea9, 0xaf3)
RETURNS = unpack(6, 19, 0xcd368b064f1cec211b8c3, 0xa4baae2)
COUNTS = unpack(6, 16, 0x42149348b0c30c1102042, 0x420)
LAST = unpack(9, 13, 0x293892422193c9845432, 0x100c00110)


def table(values, bits):
    per = 30 // bits
    words = [sum(v << (bits * j) for j, v in enumerate(values[i:i + per])) for i in range(0, len(values), per)]

    def get(i):
        w = jnp.int32(words[0])
        for k, v in enumerate(words[1:], 1):
            w = jnp.where(i >= k * per, jnp.int32(v), w)
        return lax.rem(lax.shift_right_logical(w, lax.rem(i, per) * bits), 1 << bits)

    return get


def decode(v):
    return lax.rem(v, 8), lax.rem(v // 8, 2), lax.rem(v // 16, 4)


def dot(a, b):
    return jnp.dot(a, b, preferred_element_type=F32)


def fold_max(x):
    return jnp.max(x.reshape(x.shape[0] // 8, 8, x.shape[1]), axis=0)


def fold_sum(x):
    return jnp.sum(x.reshape(x.shape[0] // 8, 8, x.shape[1]), axis=0)


def one_head(qt, e):
    rest = jnp.zeros((64, qt.shape[1]), BF16)
    return jnp.concatenate([qt[0:64], rest] if e == 0 else [rest, qt[64:128]], axis=0)


def ones_row(cols):
    row = lax.broadcasted_iota(jnp.int32, (128, cols), 0)
    return jnp.where(row == 0, 1.0, 0.0).astype(BF16)


def scores(S, slot, keys, rhs, b):
    s = dot(keys(b), rhs)
    S[slot, b * T:(b + 1) * T, :] = s
    return fold_max(s)


def score_all(S, slot, keys, rhs, blocks):
    return functools.reduce(jnp.maximum, [scores(S, slot, keys, rhs, b) for b in range(blocks)])


def score_and_sum(S, slot, keys, rhs, slot_v, values, top, blocks, c):
    ahead = min(3, blocks)
    m = jnp.max(top, axis=0, keepdims=True)
    tops = [scores(S, slot, keys, rhs, b) for b in range(ahead)]
    part = jnp.zeros((8, T), F32)
    num = jnp.zeros((64, T), F32)
    for b in range(blocks):
        p = jnp.exp2((S[slot_v, b * T:(b + 1) * T, :] - m) * c)
        part = part + fold_sum(p)
        num = num + dot(values(b), p.astype(BF16))
        if b + ahead < blocks:
            tops.append(scores(S, slot, keys, rhs, b + ahead))
    return functools.reduce(jnp.maximum, tops), num, jnp.sum(part, axis=0, keepdims=True), m


def rms_norm(h, g):
    h = h.astype(F32)
    inv = lax.rsqrt(jnp.mean(h * h, axis=-1, keepdims=True) + EPS)
    return (h * inv * g).astype(BF16)


def kernel(n_dev, head_dim, n_layers,
           mem_len, hid_in, mem_in, g_self, g_cross, g_mlp,
           self_q, self_k, self_v, self_o, cross_q, cross_k, cross_v, cross_o, mlp_g, mlp_u, mlp_d,
           out,
           hid, x_all, mem, ks, vs, kc, vc, bias, qm, q_all, S, top_s,
           wq, wk, wv, wo, cq, ck, cv, co, wg, wu, wd,
           part, part_ml, o_send, ml_send, o_recv, ml_recv,
           s_num, s_max, s_sum, a_half, att, upd, xc,
           xtx, xrx, ptx, prx, qtx, qrx, otx, orx, mtx, mrx, ctx, crx, dtx, drx, wsem, gsem, usem, isem):
    Z = n_dev // 2
    rows, D = hid.shape
    piece = rows // 4
    NP = q_all.shape[1]
    KBC = kc.shape[0]
    NF = wg.shape[0]
    Dc = D // 2
    mem_rows = mem_in.shape[0]
    c_exp = math.log2(math.e) * head_dim ** -0.5

    me = lax.axis_index("sp")
    z = me // 2
    c = me % 2
    partner = z * 2 + (1 - c)

    def ring(k):
        return lax.rem(z + k * (1 - 2 * c) + 2 * Z, Z)

    def nbr(d):
        return ring(1 - 2 * d) * 2 + c

    def rcopy(src, dst, ssem, rsem, dev):
        return pltpu.make_async_remote_copy(src_ref=src, dst_ref=dst, send_sem=ssem, recv_sem=rsem,
                                            device_id={"sp": dev}, device_id_type=MESH)

    has_mem = z * (2 * mem_rows) < n_dev * mem_rows * 3 // 4
    my_rows = pl.multiple_of(c * rows, rows)
    my_cols = pl.multiple_of(c * Dc, Dc)
    other_cols = pl.multiple_of((1 - c) * Dc, Dc)

    barrier = pltpu.get_barrier_semaphore()
    for dev in (nbr(0), nbr(1), partner):
        pl.semaphore_signal(barrier, inc=1, device_id={"sp": dev}, device_id_type=MESH)

    def wcopies(l):
        cols = pl.ds(my_cols, Dc)
        w = [
            (self_k.at[l, :, cols], wk), (self_q.at[l, :, cols], wq), (self_v.at[l, :, cols], wv),
            (cross_k.at[l, :, cols], ck), (cross_v.at[l, :, cols], cv),
            (self_o.at[l], wo), (cross_q.at[l, :, cols], cq), (cross_o.at[l], co), (mlp_d.at[l], wd),
        ]
        return [pltpu.make_async_copy(s, d, wsem.at[i]) for i, (s, d) in enumerate(w)]

    WK, WQ, WV, CK, CV, WO, CQ, CO, WD = range(9)

    def gate_copy(l, f):
        return pltpu.make_async_copy(mlp_g.at[l, :, pl.ds(f * T, T)], wg.at[f], gsem.at[f])

    def up_copy(l, f):
        return pltpu.make_async_copy(mlp_u.at[l, :, pl.ds(f * T, T)], wu.at[f], usem.at[f])

    hid_copy = pltpu.make_async_copy(hid_in, hid, isem.at[0])
    mem_copy = pltpu.make_async_copy(mem_in, mem.at[c], isem.at[1])
    mem_swap = rcopy(mem_in, mem.at[c], dtx.at[3], drx.at[3], partner)
    hid_copy.start()
    first = wcopies(0)
    for i in (WQ, WK, WV):
        first[i].start()
    mem_copy.start()
    for i in (CK, CV, WO, CQ, CO):
        first[i].start()
    for f in range(NF):
        gate_copy(0, f).start()
        up_copy(0, f).start()
    first[WD].start()

    pl.semaphore_wait(barrier, 3)
    hid_copy.wait()

    def gain(ref, l):
        g = jnp.zeros((1, D), F32)
        for i in range(n_layers):
            g = jnp.where(l == i, ref[i:i + 1, :].astype(F32), g)
        return g

    def kv_block(x, wk_ref, wv_ref, kdst, vdst, b):
        v = dot(x, wv_ref[...])
        k = dot(x, wk_ref[...]).astype(BF16)
        for p in range(NP):
            vdst[b, p] = jnp.transpose(v[:, p * 128:(p + 1) * 128]).astype(BF16)
        for p in range(NP):
            kdst[b, p] = k[:, p * 128:(p + 1) * 128]

    def memory_block(b, _):
        per = mem_rows // T
        at = pl.ds(pl.multiple_of(lax.rem(b, per) * T, T), T)
        kv_block(mem[b // per, at, :], ck, cv, kc, vc, b)
        return 0

    def key_mask():
        length = mem_len[0]
        for b in range(KBC):
            key = z * (2 * mem_rows) + b * T + lax.broadcasted_iota(jnp.int32, (T, 128), 0)
            lane = lax.broadcasted_iota(jnp.int32, (T, 128), 1)
            bias[b] = jnp.where(jnp.logical_and(lane == 0, key >= length), NEG, 0.0).astype(BF16)

    def empty_parts():
        for i in range(part.shape[0]):
            part[i] = jnp.zeros(part.shape[1:], F32)
            row = lax.broadcasted_iota(jnp.int32, part_ml.shape[1:], 0)
            part_ml[i] = jnp.where(row < 4, NEG, 0.0)

    def rows_of(a):
        return jnp.transpose(a.astype(F32)).astype(BF16)

    def swap_project(w_ref, ready):
        swap = rcopy(a_half.at[0, 1 - c], att.at[0], dtx.at[0], drx.at[0], partner)
        swap.start()
        ready.wait()
        own = rows_of(a_half[0, c])
        upd[...] = hid[...].astype(F32) + dot(own, w_ref[pl.ds(my_cols, Dc), :])
        swap.wait()
        hid[...] = (upd[...] + dot(rows_of(att[0]), w_ref[pl.ds(other_cols, Dc), :])).astype(BF16)

    def pair_rows(p):
        return pl.ds(pl.multiple_of(p * 128, 128), 128)

    def pair_swap(p):
        return rcopy(a_half.at[1, 1 - c, pair_rows(p)], att.at[1, pair_rows(p)], ctx.at[p], crx.at[p], partner)

    def pair_project(a, base, p):
        w = co[pl.ds(pl.multiple_of(base + p * 128, 128), 128), :]
        upd[...] += dot(rows_of(a), w)

    group_of = table(GROUPS + GROUPS[-1:], 6)
    count_of = table(COUNTS, 6)
    arrival_of = table(ARRIVALS, 6)
    return_of = table(RETURNS, 6)
    last_of = table(LAST, 9)

    def layer_body(l, carry):
        more = l + 1 < n_layers
        cur = wcopies(l)
        nxt = wcopies(jnp.minimum(l + 1, n_layers - 1))

        def prefetch(*ids):
            @pl.when(more)
            def _():
                for i in ids:
                    nxt[i].start()

        x_all[z, pl.ds(my_rows, rows), :] = rms_norm(hid[...], gain(g_self, l))

        def xslot(o, h):
            return x_all.at[o, pl.ds(pl.multiple_of(c * rows + h * piece, piece), piece), :]

        def pslot(o, h):
            return x_all.at[o, pl.ds(pl.multiple_of((1 - c) * rows + h * piece, piece), piece), :]

        for h in range(4):
            src = xslot(z, h)
            for d in range(2):
                rcopy(src, src, xtx.at[d, 0, h], xrx.at[d, 1, h], nbr(d)).start()
            rcopy(src, src, ptx.at[z, h], prx.at[z, h], partner).start()

        @pl.when(l == 0)
        def _():
            mem_swap.start()
            key_mask()
            pl.when(jnp.logical_not(has_mem))(empty_parts)

        def x_event(d, s, h):
            o = ring(-(1 - 2 * d) * s)
            src = xslot(o, h)

            @pl.when(jnp.logical_or(s <= 3, h % 2 == d))
            def _():
                rcopy(src, src, xtx.at[d, s, h], xrx.at[d, s, h], nbr(d)).wait_recv()

                @pl.when(jnp.logical_or(s < 3, jnp.logical_and(s == 3, h % 2 == d)))
                def _():
                    rcopy(src, src, xtx.at[d, s, h], xrx.at[d, s + 1, h], nbr(d)).start()
                rcopy(src, src, ptx.at[o, h], prx.at[o, h], partner).start()

        def partner_rows(o):
            for h in range(4):
                dst = pslot(o, h)
                rcopy(dst, dst, ptx.at[o, h], prx.at[o, h], partner).wait_recv()

        delta = (lax.broadcasted_iota(jnp.int32, (T, T), 0) - lax.broadcasted_iota(jnp.int32, (T, T), 1))

        def attend(o, start):
            tops = {}

            def score(h):
                s = dot(ks[o, h // 2], qm[h])
                if start:
                    s = jnp.where(delta <= 0, s, NEG)
                S[0, h * T:(h + 1) * T, :] = s
                tops[h] = fold_max(s)

            def values(h):
                m = jnp.max(tops[h], axis=0, keepdims=True)
                if not start:
                    old = s_max[h:h + 1, :]
                    m = jnp.maximum(m, old)
                p = jnp.exp2((S[0, h * T:(h + 1) * T, :] - m) * c_exp)
                tot = jnp.sum(fold_sum(p), axis=0, keepdims=True)
                e = h % 2
                num = dot(vs[o, h // 2, e * 64:(e + 1) * 64, :], p.astype(BF16))
                if not start:
                    keep = jnp.exp2((old - m) * c_exp)
                    tot = tot + s_sum[h:h + 1, :] * keep
                    num = num + s_num[h] * keep
                s_max[h:h + 1, :] = m
                s_sum[h:h + 1, :] = tot
                s_num[h] = num

            for h in range(2 * NP):
                score(h)
            for h in range(2 * NP):
                values(h)

        for i in (WQ, WK, WV):
            cur[i].wait()
        partner_rows(z)
        q = dot(x_all[z], wq[...])
        for p in range(NP):
            qt = jnp.transpose(q[:, p * 128:(p + 1) * 128]).astype(BF16)
            for e in range(2):
                qm[2 * p + e] = one_head(qt, e)
        kv_block(x_all[z], wk, wv, ks, vs, z)
        attend(z, True)

        def memory_part(i):
            @pl.when(l == 0)
            def _():
                @pl.when(i == 0)
                def _():
                    cur[CK].wait()
                    cur[CV].wait()
                    mem_copy.wait()
                    mem_swap.wait()
                lax.fori_loop(KBC * i // 4, jnp.where(has_mem, KBC * (i + 1) // 4, 0), memory_block, 0)

        def attend_one(s, sign):
            o = ring(s * sign)

            @pl.when(o < z)
            def _():
                attend(o, False)

        def level(s, _):
            def arrivals(h):
                for d in range(2):
                    x_event(d, s, h)

            arrivals(0)

            @pl.when(s == 1)
            def _():
                memory_part(0)

            @pl.when(s >= 2)
            def _():
                attend_one(s - 1, 1)
            arrivals(1)

            @pl.when(s >= 2)
            def _():
                attend_one(s - 1, -1)
            arrivals(2)
            arrivals(3)

            def block(j, _):
                o = ring(s * (1 - 2 * j))
                partner_rows(o)

                @pl.when(o < z)
                def _():
                    kv_block(x_all[o], wk, wv, ks, vs, o)
                return 0

            lax.fori_loop(0, jnp.where(s == Z // 2, 1, 2), block, 0)

            @pl.when(s < Z // 2)
            def _():
                memory_part(s)
            return 0

        lax.fori_loop(1, Z // 2 + 1, level, 0)
        attend_one(Z // 2, 1)
        prefetch(WK, WQ, WV)

        @pl.when(l == 0)
        def _():
            prefetch(CK, CV)

        for h in range(2 * NP):
            a = (s_num[h] / s_sum[h:h + 1, :]).astype(BF16)
            for j in range(2):
                a_half[0, j, h * 64:(h + 1) * 64, :] = a[:, j * 128:(j + 1) * 128]
        swap_project(wo, cur[WO])
        prefetch(WO)

        xc[c] = rms_norm(hid[...], gain(g_cross, l))
        swap = rcopy(xc.at[c], xc.at[c], dtx.at[2], drx.at[2], partner)
        swap.start()

        for h in range(4):
            for d in range(2):
                for s in range(4):
                    if s < 3 or h % 2 == d:
                        src = xslot(z, h)
                        rcopy(src, src, xtx.at[d, s, h], xrx.at[d, s, h], nbr(d)).wait_send()
            for o in range(Z):
                src = xslot(o, h)
                rcopy(src, src, ptx.at[o, h], prx.at[o, h], partner).wait_send()

        def project_q(i):
            q = dot(xc[i], cq[...])
            at = pl.ds(pl.multiple_of(i * rows, rows), rows)
            for p in range(NP):
                q_all[z, p, :, at] = jnp.transpose(q[:, p * 128:(p + 1) * 128]).astype(BF16)

        cur[CQ].wait()
        project_q(c)
        swap.wait()
        project_q(1 - c)
        prefetch(CQ)

        def q_own(p):
            for d in range(2):
                src = q_all.at[z, p]
                rcopy(src, src, qtx.at[d, 0, p], qrx.at[d, 1, p], nbr(d)).start()

        def arrival(i, _):
            s, d, p = decode(arrival_of(i))

            @pl.when(s == 0)
            def _():
                q_own(p)

            @pl.when(s >= 1)
            def _():
                src = q_all.at[ring(-(1 - 2 * d) * s), p]
                rcopy(src, src, qtx.at[d, s, p], qrx.at[d, s, p], nbr(d)).wait_recv()

                @pl.when(jnp.logical_or(s < 3, jnp.logical_and(s == 3, lax.rem(p, 2) == d)))
                def _():
                    rcopy(src, src, qtx.at[d, s, p], qrx.at[d, s + 1, p], nbr(d)).start()
            return 0

        one = ones_row(T)

        def head_rhs(o, p, e):
            return jnp.concatenate([one_head(q_all[o, p], e), one], axis=0)

        def keys_of(p):
            return lambda b: jnp.concatenate([kc[b, p], bias[b]], axis=1)

        def place(s, d, p):
            return p * 8 + jnp.where(s == 0, 0, jnp.where(s == 4, 7, 2 * s - 1 + d))

        def origin(s, d):
            return ring(jnp.where(d == 0, -s, s))

        def cross_groups(*groups):
            where = [(origin(s, d), p, place(s, d, p)) for s, d, p in groups]
            heads = [(w, e) for w in where[:-1] for e in range(2)] + [(where[-1], 0)]
            top = top_s[...]
            stats = []
            for ((o, p, to), e), ((on, pn, _), en) in zip(heads, heads[1:]):
                top, num, l, m = score_and_sum(
                    S, en, keys_of(pn), head_rhs(on, pn, en),
                    e, lambda b: vc[b, p, e * 64:(e + 1) * 64, :], top, KBC, c_exp)
                part[to, e * 64:(e + 1) * 64, :] = num
                stats.append((m, l))
                if e == 1:
                    part_ml[to] = jnp.concatenate(
                        [x[k][:, j * 128:(j + 1) * 128] for k in range(2) for j in range(2) for x in stats[-2:]], axis=0)
            top_s[...] = top

        def incoming(d, s, p):
            rcopy(o_send.at[d, s, p], o_recv.at[d, s, p], otx.at[d, s, p], orx.at[d, s, p], nbr(d)).wait_recv()
            rcopy(ml_send.at[d, s, p], ml_recv.at[d, s, p], mtx.at[d, s, p], mrx.at[d, s, p], nbr(d)).wait_recv()

        def scales(mls):
            m = functools.reduce(jnp.maximum, [x[0:4] for x in mls])
            w = [jnp.exp2((x[0:4] - m) * c_exp) for x in mls]
            return w, m, sum(x[4:8] * y for x, y in zip(mls, w))

        def tile(ref, e, j):
            return ref[e * 64:(e + 1) * 64, j * 128:(j + 1) * 128].astype(F32)

        def reduce_step(v):
            s, d_arr, p = decode(v)
            at = place(s, d_arr, p)
            d = jnp.where(s == 4, lax.rem(p, 2), 1 - d_arr)
            has_in = jnp.logical_and(s >= 1, jnp.logical_or(s < 3, jnp.logical_and(s == 3, lax.rem(p, 2) == d)))
            to = jnp.maximum(s - 1, 0)

            @pl.when(has_in)
            def _():
                incoming(d, s, p)
                (wa, wb), m, l = scales([part_ml[at], ml_recv[d, s, p]])
                ml_send[d, to, p] = jnp.concatenate([m, l], axis=0)
                for e in range(2):
                    for j in range(2):
                        r = slice(2 * j + e, 2 * j + e + 1)
                        o_send[d, to, p, e * 64:(e + 1) * 64, j * 128:(j + 1) * 128] = (
                            tile(part.at[at], e, j) * wa[r] + tile(o_recv.at[d, s, p], e, j) * wb[r]).astype(BF16)

            @pl.when(jnp.logical_and(s >= 1, jnp.logical_not(has_in)))
            def _():
                o_send[d, to, p] = part[at].astype(BF16)
                ml_send[d, to, p] = part_ml[at]

            @pl.when(s >= 1)
            def _():
                rcopy(ml_send.at[d, to, p], ml_recv.at[d, to, p], mtx.at[d, to, p], mrx.at[d, to, p], nbr(d)).start()
                rcopy(o_send.at[d, to, p], o_recv.at[d, to, p], otx.at[d, to, p], orx.at[d, to, p], nbr(d)).start()

            @pl.when(s == 0)
            def _():
                for dd in range(2):
                    incoming(dd, 0, p)
                w, m, l = scales([part_ml[at], ml_recv[0, 0, p], ml_recv[1, 0, p]])
                to_rows = pl.multiple_of(p * 128, 128)
                for e in range(2):
                    for j in range(2):
                        r = slice(2 * j + e, 2 * j + e + 1)
                        tot = (tile(part.at[at], e, j) * w[0][r] + tile(o_recv.at[0, 0, p], e, j) * w[1][r]
                               + tile(o_recv.at[1, 0, p], e, j) * w[2][r])
                        a_half[1, j, pl.ds(to_rows + e * 64, 64), :] = (tot / l[r]).astype(BF16)

        q_own(0)
        q_own(1)
        @pl.when(has_mem)
        def _():
            top_s[...] = score_all(S, 0, keys_of(GROUPS[0] // 16), head_rhs(z, GROUPS[0] // 16, 0), KBC)

        def step(k, at):
            ia, ir = at
            n = count_of(k)
            ja, jr = ia + lax.rem(n, 8), ir + n // 8
            lax.fori_loop(ia, ja, arrival, 0)

            def ret(i, _):
                reduce_step(return_of(i))
                return 0

            lax.fori_loop(ir, jr, ret, 0)
            groups = [decode(group_of(2 * k + i)) for i in range(3)]
            pl.when(has_mem)(lambda: cross_groups(*groups))
            return ja, jr

        lax.fori_loop(0, len(COUNTS), step, (jnp.int32(0), jnp.int32(0)))

        @pl.when(more)
        def _():
            nxt[CK].wait()
            nxt[CV].wait()

        def finish(i, b):
            v = last_of(i)
            n = jnp.where(jnp.logical_and(more, has_mem), v // 64, 0)
            lax.fori_loop(b, jnp.minimum(b + n, KBC), memory_block, 0)
            reduce_step(lax.rem(v, 64))

            @pl.when(lax.rem(v, 8) == 0)
            def _():
                p = lax.rem(v // 16, 4)
                pair_swap(p).start()
                pair_project(a_half[1, c, pair_rows(p)], my_cols, p)
            return b + n

        cur[CO].wait()
        upd[...] = hid[...].astype(F32)

        lax.fori_loop(0, len(LAST), finish, jnp.int32(0))

        @pl.when(l + 2 < n_layers)
        def _():
            after = wcopies(jnp.minimum(l + 2, n_layers - 1))
            after[CK].start()
            after[CV].start()

        for v in LAST[-NP:]:
            p = v % 64 // 16
            pair_swap(p).wait()
            pair_project(att[1, pair_rows(p)], other_cols, p)
        hid[...] = upd[...].astype(BF16)
        prefetch(CO)

        xm = rms_norm(hid[...], gain(g_mlp, l))

        for p in range(NP):
            for d in range(2):
                for s in range(4):
                    if s < 3 or p % 2 == d:
                        src = q_all.at[z, p]
                        rcopy(src, src, qtx.at[d, s, p], qrx.at[d, s, p], nbr(d)).wait_send()
                        rcopy(o_send.at[d, s, p], o_recv.at[d, s, p], otx.at[d, s, p], orx.at[d, s, p], nbr(d)).wait_send()
                        rcopy(ml_send.at[d, s, p], ml_recv.at[d, s, p], mtx.at[d, s, p], mrx.at[d, s, p], nbr(d)).wait_send()

        for f in range(NF):
            gate_copy(l, f).wait()
            up_copy(l, f).wait()
        cur[WD].wait()
        acts = []
        for f in range(NF):
            gt = dot(xm, wg[f])
            up = dot(xm, wu[f])
            acts.append((gt * lax.logistic(gt) * up).astype(BF16))
        full = jnp.concatenate(acts, axis=1)

        @pl.when(more)
        def _():
            for f in range(NF):
                gate_copy(l + 1, f).start()
                up_copy(l + 1, f).start()
        for n in range(D // T):
            cols = slice(n * T, (n + 1) * T)
            hid[:, cols] = (hid[:, cols].astype(F32) + dot(full, wd[:, cols])).astype(BF16)
        prefetch(WD)
        return carry

    lax.fori_loop(0, n_layers, layer_body, 0)
    out[...] = hid[...]


def solution(mesh):
    n_dev = mesh.shape["sp"]

    def local_step(hidden, memory, mem_len, norm_self, norm_cross, norm_mlp, self_q, self_k, self_v, self_o,
                   cross_q, cross_k, cross_v, cross_o, mlp_gate, mlp_up, mlp_down):
        rows, D = hidden.shape
        mem_rows = memory.shape[0]
        L, heads, head_dim = self_o.shape[:3]
        FF = mlp_gate.shape[2]
        Dc = D // 2
        NP = Dc // 128
        Z = n_dev // 2
        KBC = 2 * mem_rows // T
        NF = FF // T
        any_ = pl.BlockSpec(memory_space=pl.ANY)
        vmem = pl.BlockSpec(memory_space=pltpu.VMEM)
        smem = pl.BlockSpec(memory_space=pltpu.SMEM)
        dma = pltpu.SemaphoreType.DMA
        V = pltpu.VMEM
        scratch = [
            V((rows, D), BF16),
            V((Z, 2 * rows, D), BF16),
            V((2, mem_rows, D), BF16),
            V((Z, NP, T, 128), BF16),
            V((Z, NP, 128, T), BF16),
            V((KBC, NP, T, 128), BF16),
            V((KBC, NP, 128, T), BF16),
            V((KBC, T, 128), BF16),
            V((2 * NP, 128, T), BF16),
            V((Z, NP, 128, T), BF16),
            V((2, max(2 * NP, KBC) * T, T), F32),
            V((8, T), F32),
            V((D, Dc), BF16), V((D, Dc), BF16), V((D, Dc), BF16), V((D, D), BF16),
            V((D, Dc), BF16), V((D, Dc), BF16), V((D, Dc), BF16), V((D, D), BF16),
            V((NF, D, T), BF16), V((NF, D, T), BF16), V((FF, D), BF16),
            V((8 * NP, 128, T), F32),
            V((8 * NP, 8, 128), F32),
            V((2, 4, NP, 128, T), BF16),
            V((2, 4, NP, 8, 128), F32),
            V((2, 4, NP, 128, T), BF16),
            V((2, 4, NP, 8, 128), F32),
            V((2 * NP, 64, T), F32),
            V((8, T), F32), V((8, T), F32),
            V((2, 2, Dc, 128), BF16),
            V((2, Dc, 128), BF16),
            V((rows, D), F32),
            V((2, rows, D), BF16),
            dma((2, 5, 4)), dma((2, 5, 4)), dma((Z, 4)), dma((Z, 4)),
            dma((2, 5, NP)), dma((2, 5, NP)),
            dma((2, 4, NP)), dma((2, 4, NP)), dma((2, 4, NP)), dma((2, 4, NP)),
            dma((NP,)), dma((NP,)),
            dma((4,)), dma((4,)), dma((9,)), dma((NF,)), dma((NF,)), dma((2,)),
        ]
        call = pl.pallas_call(
            functools.partial(kernel, n_dev, head_dim, L),
            out_shape=jax.ShapeDtypeStruct((rows, D), BF16),
            in_specs=[smem, any_, any_, vmem, vmem, vmem] + [any_] * 11,
            out_specs=vmem,
            scratch_shapes=scratch,
            compiler_params=pltpu.CompilerParams(
                collective_id=0, has_side_effects=True, vmem_limit_bytes=67043328),
            name="decoder",
        )
        return call(mem_len, hidden, memory, norm_self, norm_cross, norm_mlp,
                    self_q, self_k, self_v, self_o.reshape(L, D, D), cross_q, cross_k, cross_v,
                    cross_o.reshape(L, D, D), mlp_gate, mlp_up, mlp_down)

    row_spec = P(("dp", "sp"), None)
    return jax.shard_map(local_step, mesh=mesh, in_specs=(row_spec, row_spec, P("dp")) + (P(),) * 14,
                         out_specs=row_spec, check_vma=False)
```

```python
import functools
import math

import jax
import jax.numpy as jnp
from jax import lax
from jax.experimental import pallas as pl
from jax.experimental.pallas import tpu as pltpu
from jax.sharding import PartitionSpec as P

MESH = pl.DeviceIdType.MESH
EPS = 1e-6
NEG = -1e30
T = 256
F32 = jnp.float32
BF16 = jnp.bfloat16

def unpack(bits, count, *words):
    per = 84 // bits
    return [(words[i // per] >> (i % per * bits)) % 2 ** bits for i in range(count)]


GROUPS = unpack(6, 32, 0x89a4b9099c51270060010, 0xaeacd3f3b91c10b8db0ca, 0xa61eb2)
ARRIVALS = unpack(6, 30, 0x88a49a0b9c59851241c20, 0x4ea904cfb70ba630dbeb2, 0xafc)
RETURNS = unpack(6, 19, 0x89307b6bc2dc90211b8c3, 0x3a4b32ab)
COUNTS = unpack(6, 16, 0x22945350b0830c20c20c0, 0x420)
LAST = unpack(9, 13, 0x311c885525124864642a, 0x181808090)


def table(values, bits):
    per = 30 // bits
    words = [sum(v << (bits * j) for j, v in enumerate(values[i:i + per])) for i in range(0, len(values), per)]

    def get(i):
        w = jnp.int32(words[0])
        for k, v in enumerate(words[1:], 1):
            w = jnp.where(i >= k * per, jnp.int32(v), w)
        return lax.rem(lax.shift_right_logical(w, lax.rem(i, per) * bits), 1 << bits)

    return get


def decode(v):
    return lax.rem(v, 8), lax.rem(v // 8, 2), lax.rem(v // 16, 4)


def dot(a, b):
    return jnp.dot(a, b, preferred_element_type=F32)


def fold_max(x):
    return jnp.max(x.reshape(x.shape[0] // 8, 8, x.shape[1]), axis=0)


def fold_sum(x):
    return jnp.sum(x.reshape(x.shape[0] // 8, 8, x.shape[1]), axis=0)


def one_head(qt, e):
    rest = jnp.zeros((64, qt.shape[1]), BF16)
    return jnp.concatenate([qt[0:64], rest] if e == 0 else [rest, qt[64:128]], axis=0)


def ones_row(cols):
    row = lax.broadcasted_iota(jnp.int32, (128, cols), 0)
    return jnp.where(row == 0, 1.0, 0.0).astype(BF16)


def scores(S, slot, keys, rhs, b):
    s = dot(keys(b), rhs)
    S[slot, b * T:(b + 1) * T, :] = s
    return fold_max(s)


def score_all(S, slot, keys, rhs, blocks):
    return functools.reduce(jnp.maximum, [scores(S, slot, keys, rhs, b) for b in range(blocks)])


def score_and_sum(S, slot, keys, rhs, slot_v, values, top, blocks, c):
    ahead = min(3, blocks)
    m = jnp.max(top, axis=0, keepdims=True)
    tops = [scores(S, slot, keys, rhs, b) for b in range(ahead)]
    part = jnp.zeros((8, T), F32)
    num = jnp.zeros((64, T), F32)
    for b in range(blocks):
        p = jnp.exp2((S[slot_v, b * T:(b + 1) * T, :] - m) * c)
        part = part + fold_sum(p)
        num = num + dot(values(b), p.astype(BF16))
        if b + ahead < blocks:
            tops.append(scores(S, slot, keys, rhs, b + ahead))
    return functools.reduce(jnp.maximum, tops), num, jnp.sum(part, axis=0, keepdims=True), m


def rms_norm(h, g):
    h = h.astype(F32)
    inv = lax.rsqrt(jnp.mean(h * h, axis=-1, keepdims=True) + EPS)
    return (h * inv * g).astype(BF16)


def kernel(n_dev, head_dim, n_layers,
           mem_len, hid_in, mem_in, g_self, g_cross, g_mlp,
           self_q, self_k, self_v, self_o, cross_q, cross_k, cross_v, cross_o, mlp_g, mlp_u, mlp_d,
           out,
           hid, x_all, mem, ks, vs, kc, vc, bias, qm, q_all, S, top_s,
           wq, wk, wv, wo, cq, ck, cv, co, wg, wu, wd,
           part, part_ml, o_send, ml_send, o_recv, ml_recv,
           s_num, s_max, s_sum, a_half, att, att_c, hid_p,
           xtx, xrx, ptx, prx, qtx, qrx, otx, orx, mtx, mrx, ctx, crx, dtx, drx, wsem, gsem, usem, isem):
    Z = n_dev // 2
    rows, D = hid.shape
    piece = rows // 4
    NP = q_all.shape[1]
    KBC = kc.shape[0]
    NF = wg.shape[0]
    Dc = D // 2
    mem_rows = mem_in.shape[0]
    c_exp = math.log2(math.e) * head_dim ** -0.5
    assert KBC <= Z

    me = lax.axis_index("sp")
    z = me // 2
    c = me % 2
    partner = z * 2 + (1 - c)

    def ring(k):
        return lax.rem(z + k * (1 - 2 * c) + 2 * Z, Z)

    def nbr(d):
        return ring(1 - 2 * d) * 2 + c

    def rcopy(src, dst, ssem, rsem, dev):
        return pltpu.make_async_remote_copy(src_ref=src, dst_ref=dst, send_sem=ssem, recv_sem=rsem,
                                            device_id={"sp": dev}, device_id_type=MESH)

    has_mem = z * (2 * mem_rows) < n_dev * mem_rows * 3 // 4
    my_rows = pl.multiple_of(c * rows, rows)
    my_cols = pl.multiple_of(c * Dc, Dc)
    other_cols = pl.multiple_of((1 - c) * Dc, Dc)

    barrier = pltpu.get_barrier_semaphore()
    for dev in (nbr(0), nbr(1), partner):
        pl.semaphore_signal(barrier, inc=1, device_id={"sp": dev}, device_id_type=MESH)

    def wcopies(l):
        mine = pl.ds(my_cols, Dc)
        w = [
            (self_k.at[l, :, mine], wk), (self_q.at[l, :, mine], wq), (self_v.at[l, :, mine], wv),
            (cross_k.at[l, :, mine], ck), (cross_v.at[l, :, mine], cv),
            (self_o.at[l], wo), (cross_q.at[l, :, mine], cq), (cross_o.at[l], co), (mlp_d.at[l], wd),
        ]
        return [pltpu.make_async_copy(s, d, wsem.at[i]) for i, (s, d) in enumerate(w)]

    WK, WQ, WV, CK, CV, WO, CQ, CO, WD = range(9)

    def gate_copy(l, f):
        return pltpu.make_async_copy(mlp_g.at[l, :, pl.ds(f * T, T)], wg.at[f], gsem.at[f])

    def up_copy(l, f):
        return pltpu.make_async_copy(mlp_u.at[l, :, pl.ds(f * T, T)], wu.at[f], usem.at[f])

    hid_copy = pltpu.make_async_copy(hid_in, hid, isem.at[0])
    mem_copy = pltpu.make_async_copy(mem_in, mem.at[c], isem.at[1])
    mem_swap = rcopy(mem_in, mem.at[c], dtx.at[3], drx.at[3], partner)
    hid_copy.start()
    first = wcopies(0)
    for i in (WQ, WK, WV):
        first[i].start()
    mem_copy.start()
    for i in (CK, CV, WO, CQ, CO):
        first[i].start()
    for f in range(NF):
        gate_copy(0, f).start()
        up_copy(0, f).start()
    first[WD].start()

    hid_copy.wait()

    def gain(ref, l):
        g = jnp.zeros((1, D), F32)
        for i in range(n_layers):
            g = jnp.where(l == i, ref[i:i + 1, :].astype(F32), g)
        return g

    def kv_blocks(x, wk_ref, wv_ref, kdst, vdst, *at):
        v = dot(x, wv_ref[...])
        k = dot(x, wk_ref[...]).astype(BF16)
        for i, b in enumerate(at):
            r = slice(i * T, (i + 1) * T)
            for p in range(NP):
                vdst[b, p] = jnp.transpose(v[r, p * 128:(p + 1) * 128]).astype(BF16)
            for p in range(NP):
                kdst[b, p] = k[r, p * 128:(p + 1) * 128]

    def memory_block(b, _):
        per = mem_rows // T
        at = pl.ds(pl.multiple_of(lax.rem(b, per) * T, T), T)
        kv_blocks(mem[b // per, at, :], ck, cv, kc, vc, b)
        return 0

    def memory_pair(i):
        per = mem_rows // (2 * T)
        at = pl.ds(pl.multiple_of(lax.rem(i, per) * 2 * T, 2 * T), 2 * T)
        kv_blocks(mem[i // per, at, :], ck, cv, kc, vc, 2 * i, 2 * i + 1)

    def key_mask():
        length = mem_len[0]
        for b in range(KBC):
            key = z * (2 * mem_rows) + b * T + lax.broadcasted_iota(jnp.int32, (T, 128), 0)
            lane = lax.broadcasted_iota(jnp.int32, (T, 128), 1)
            bias[b] = jnp.where(jnp.logical_and(lane == 0, key >= length), NEG, 0.0).astype(BF16)

    def empty_parts():
        for i in range(part.shape[0]):
            part[i] = jnp.zeros(part.shape[1:], F32)
            row = lax.broadcasted_iota(jnp.int32, part_ml.shape[1:], 0)
            part_ml[i] = jnp.where(row < 4, NEG, 0.0)

    def rows_of(a):
        return jnp.transpose(a.astype(F32)).astype(BF16)

    CT = range(D // T)

    def cols(n):
        return slice(n * T, (n + 1) * T)

    def upd(j, n):
        return S.at[0, pl.ds(pl.multiple_of((j * len(CT) + n) * rows, rows), rows), :]

    def swap_project(w_ref, ready):
        swap = rcopy(a_half.at[0], att, dtx.at[0], drx.at[0], partner)
        swap.start()
        ready.wait()
        for j in range(2):
            own = rows_of(a_half[0, j])
            for n in CT:
                upd(j, n)[...] = dot(own, w_ref[pl.ds(my_cols, Dc), cols(n)])
        hid_swap().wait()
        swap.wait()
        for j in range(2):
            others = rows_of(att[j])
            for n in CT:
                own, other = upd(j, n)[...], dot(others, w_ref[pl.ds(other_cols, Dc), cols(n)])
                before = jnp.where(c == j, hid[:, cols(n)], hid_p[:, cols(n)]).astype(F32)
                upd(j, n)[...] = before + jnp.where(c == 0, own, other) + jnp.where(c == 0, other, own)
        for n in CT:
            hid[:, cols(n)] = upd(c, n)[...].astype(BF16)

    def hid_swap():
        return rcopy(hid, hid_p, dtx.at[2], drx.at[2], partner)

    def pair_rows(p):
        return pl.ds(pl.multiple_of(p * 128, 128), 128)

    def pair_swap(p):
        return rcopy(a_half.at[1, 1 - c, pair_rows(p)], att_c.at[pair_rows(p)], ctx.at[p], crx.at[p], partner)

    def pair_project(a, base, p):
        a = rows_of(a)
        for n in CT:
            upd(0, n)[...] += dot(a, co[pl.ds(pl.multiple_of(base + p * 128, 128), 128), cols(n)])

    group_of = table(GROUPS + GROUPS[-1:], 6)
    count_of = table(COUNTS, 6)
    arrival_of = table(ARRIVALS, 6)
    return_of = table(RETURNS, 6)
    last_of = table(LAST, 9)

    def layer_body(l, carry):
        more = l + 1 < n_layers
        cur = wcopies(l)
        nxt = wcopies(jnp.minimum(l + 1, n_layers - 1))

        def prefetch(*ids):
            @pl.when(more)
            def _():
                for i in ids:
                    nxt[i].start()

        x_all[z, pl.ds(my_rows, rows), :] = rms_norm(hid[...], gain(g_self, l))

        @pl.when(l == 0)
        def _():
            pl.semaphore_wait(barrier, 3)

        def xslot(o, h):
            return x_all.at[o, pl.ds(pl.multiple_of(c * rows + h * piece, piece), piece), :]

        def pslot(o, h):
            return x_all.at[o, pl.ds(pl.multiple_of((1 - c) * rows + h * piece, piece), piece), :]

        for h in range(4):
            src = xslot(z, h)
            for d in range(2):
                rcopy(src, src, xtx.at[d, 0, h], xrx.at[d, 1, h], nbr(d)).start()
            rcopy(src, src, ptx.at[z, h], prx.at[z, h], partner).start()

        hid_swap().start()

        @pl.when(l == 0)
        def _():
            mem_swap.start()
            key_mask()
            pl.when(jnp.logical_not(has_mem))(empty_parts)

        def x_event(d, s, h):
            o = ring(-(1 - 2 * d) * s)
            src = xslot(o, h)

            @pl.when(jnp.logical_or(s <= 3, h % 2 == d))
            def _():
                rcopy(src, src, xtx.at[d, s, h], xrx.at[d, s, h], nbr(d)).wait_recv()

                @pl.when(jnp.logical_or(s < 3, jnp.logical_and(s == 3, h % 2 == d)))
                def _():
                    rcopy(src, src, xtx.at[d, s, h], xrx.at[d, s + 1, h], nbr(d)).start()
                rcopy(src, src, ptx.at[o, h], prx.at[o, h], partner).start()

        def partner_rows(o):
            for h in range(4):
                dst = pslot(o, h)
                rcopy(dst, dst, ptx.at[o, h], prx.at[o, h], partner).wait_recv()

        delta = (lax.broadcasted_iota(jnp.int32, (T, T), 0) - lax.broadcasted_iota(jnp.int32, (T, T), 1))

        def attend(start, *blocks):
            tops = []
            for h in range(2 * NP):
                top = None
                for i, o in enumerate(blocks):
                    s = dot(ks[o, h // 2], qm[h])
                    if start:
                        s = jnp.where(delta <= 0, s, NEG)
                    S[i, h * T:(h + 1) * T, :] = s
                    top = fold_max(s) if top is None else jnp.maximum(top, fold_max(s))
                tops.append(top)
            for h in range(2 * NP):
                m = jnp.max(tops[h], axis=0, keepdims=True)
                e = h % 2
                if not start:
                    old = s_max[h:h + 1, :]
                    m = jnp.maximum(m, old)
                part_sum = jnp.zeros((8, T), F32)
                num = jnp.zeros((64, T), F32)
                for i, o in enumerate(blocks):
                    p = jnp.exp2((S[i, h * T:(h + 1) * T, :] - m) * c_exp)
                    part_sum = part_sum + fold_sum(p)
                    num = num + dot(vs[o, h // 2, e * 64:(e + 1) * 64, :], p.astype(BF16))
                tot = jnp.sum(part_sum, axis=0, keepdims=True)
                if not start:
                    keep = jnp.exp2((old - m) * c_exp)
                    tot = tot + s_sum[h:h + 1, :] * keep
                    num = num + s_num[h] * keep
                s_max[h:h + 1, :] = m
                s_sum[h:h + 1, :] = tot
                s_num[h] = num

        for i in (WQ, WK, WV):
            cur[i].wait()
        partner_rows(z)
        q = dot(x_all[z], wq[...])
        for p in range(NP):
            qt = jnp.transpose(q[:, p * 128:(p + 1) * 128]).astype(BF16)
            for e in range(2):
                qm[2 * p + e] = one_head(qt, e)
        kv_blocks(x_all[z], wk, wv, ks, vs, z)
        attend(True, z)

        def memory_part(i):
            @pl.when(l == 0)
            def _():
                @pl.when(i == 0)
                def _():
                    cur[CK].wait()
                    cur[CV].wait()
                    mem_copy.wait()
                    mem_swap.wait()
            pl.when(jnp.logical_and(has_mem, i < KBC // 2))(lambda: memory_pair(i))

        def earlier(s, one, two):
            o, q = ring(s), ring(-s)
            pl.when(jnp.logical_and(o < z, q < z))(lambda: two(o, q))
            pl.when(jnp.logical_xor(o < z, q < z))(lambda: one(jnp.minimum(o, q)))

        def attend_level(s):
            earlier(s, lambda o: attend(False, o), lambda o, q: attend(False, o, q))

        def project_level(s):
            earlier(s, lambda o: kv_blocks(x_all[o], wk, wv, ks, vs, o),
                    lambda o, q: kv_blocks(jnp.concatenate([x_all[o], x_all[q]], axis=0), wk, wv, ks, vs, o, q))

        def level(s, _):
            def arrivals(h):
                for d in range(2):
                    x_event(d, s, h)

            arrivals(0)
            arrivals(1)

            @pl.when(s == 1)
            def _():
                memory_part(0)

            @pl.when(s >= 2)
            def _():
                attend_level(s - 1)
            arrivals(2)
            arrivals(3)
            for o in (ring(s), ring(-s)):
                partner_rows(o)
            project_level(s)
            memory_part(s)
            return 0

        lax.fori_loop(1, Z // 2, level, 0)
        far = ring(Z // 2)
        for h in range(4):
            x_event(h % 2, Z // 2, h)
            if h == 1:
                attend_level(Z // 2 - 1)
        partner_rows(far)

        @pl.when(far < z)
        def _():
            kv_blocks(x_all[far], wk, wv, ks, vs, far)
            attend(False, far)
        prefetch(WK, WQ, WV)

        @pl.when(l == 0)
        def _():
            prefetch(CK, CV)

        for h in range(2 * NP):
            a = (s_num[h] / s_sum[h:h + 1, :]).astype(BF16)
            for j in range(2):
                a_half[0, j, h * 64:(h + 1) * 64, :] = a[:, j * 128:(j + 1) * 128]
        swap_project(wo, cur[WO])
        prefetch(WO)

        for h in range(4):
            for d in range(2):
                for s in range(4):
                    if s < 3 or h % 2 == d:
                        src = xslot(z, h)
                        rcopy(src, src, xtx.at[d, s, h], xrx.at[d, s, h], nbr(d)).wait_send()
            for o in range(Z):
                src = xslot(o, h)
                rcopy(src, src, ptx.at[o, h], prx.at[o, h], partner).wait_send()

        for j in range(2):
            mine = jnp.concatenate([upd(j, n)[...].astype(BF16) for n in CT], axis=1)
            x = rms_norm(mine, gain(g_cross, l))
            if j == 0:
                cur[CQ].wait()
            q = dot(x, cq[...])
            for p in range(NP):
                q_all[z, p, :, j * rows:(j + 1) * rows] = jnp.transpose(q[:, p * 128:(p + 1) * 128]).astype(BF16)
        prefetch(CQ)

        def q_own(p):
            for d in range(2):
                src = q_all.at[z, p]
                rcopy(src, src, qtx.at[d, 0, p], qrx.at[d, 1, p], nbr(d)).start()

        def arrival(i, _):
            s, d, p = decode(arrival_of(i))

            @pl.when(s == 0)
            def _():
                q_own(p)

            @pl.when(s >= 1)
            def _():
                src = q_all.at[ring(-(1 - 2 * d) * s), p]
                rcopy(src, src, qtx.at[d, s, p], qrx.at[d, s, p], nbr(d)).wait_recv()

                @pl.when(jnp.logical_or(s < 3, jnp.logical_and(s == 3, lax.rem(p, 2) == d)))
                def _():
                    rcopy(src, src, qtx.at[d, s, p], qrx.at[d, s + 1, p], nbr(d)).start()
            return 0

        one = ones_row(T)

        def head_rhs(o, p, e):
            return jnp.concatenate([one_head(q_all[o, p], e), one], axis=0)

        def keys_of(p):
            return lambda b: jnp.concatenate([kc[b, p], bias[b]], axis=1)

        def place(s, d, p):
            return p * 8 + jnp.where(s == 0, 0, jnp.where(s == 4, 7, 2 * s - 1 + d))

        def origin(s, d):
            return ring(jnp.where(d == 0, -s, s))

        def cross_groups(*groups):
            where = [(origin(s, d), p, place(s, d, p)) for s, d, p in groups]
            heads = [(w, e) for w in where[:-1] for e in range(2)] + [(where[-1], 0)]
            top = top_s[...]
            stats = []
            for ((o, p, to), e), ((on, pn, _), en) in zip(heads, heads[1:]):
                top, num, l, m = score_and_sum(
                    S, en, keys_of(pn), head_rhs(on, pn, en),
                    e, lambda b: vc[b, p, e * 64:(e + 1) * 64, :], top, KBC, c_exp)
                part[to, e * 64:(e + 1) * 64, :] = num
                stats.append((m, l))
                if e == 1:
                    part_ml[to] = jnp.concatenate(
                        [x[k][:, j * 128:(j + 1) * 128] for k in range(2) for j in range(2) for x in stats[-2:]], axis=0)
            top_s[...] = top

        def incoming(d, s, p):
            rcopy(o_send.at[d, s, p], o_recv.at[d, s, p], otx.at[d, s, p], orx.at[d, s, p], nbr(d)).wait_recv()
            rcopy(ml_send.at[d, s, p], ml_recv.at[d, s, p], mtx.at[d, s, p], mrx.at[d, s, p], nbr(d)).wait_recv()

        def scales(mls):
            m = functools.reduce(jnp.maximum, [x[0:4] for x in mls])
            w = [jnp.exp2((x[0:4] - m) * c_exp) for x in mls]
            return w, m, sum(x[4:8] * y for x, y in zip(mls, w))

        def tile(ref, e, j):
            return ref[e * 64:(e + 1) * 64, j * 128:(j + 1) * 128].astype(F32)

        def reduce_step(v):
            s, d_arr, p = decode(v)
            at = place(s, d_arr, p)
            d = jnp.where(s == 4, lax.rem(p, 2), 1 - d_arr)
            has_in = jnp.logical_and(s >= 1, jnp.logical_or(s < 3, jnp.logical_and(s == 3, lax.rem(p, 2) == d)))
            to = jnp.maximum(s - 1, 0)

            @pl.when(has_in)
            def _():
                incoming(d, s, p)
                (wa, wb), m, l = scales([part_ml[at], ml_recv[d, s, p]])
                ml_send[d, to, p] = jnp.concatenate([m, l], axis=0)
                for e in range(2):
                    for j in range(2):
                        r = slice(2 * j + e, 2 * j + e + 1)
                        o_send[d, to, p, e * 64:(e + 1) * 64, j * 128:(j + 1) * 128] = (
                            tile(part.at[at], e, j) * wa[r] + tile(o_recv.at[d, s, p], e, j) * wb[r]).astype(BF16)

            @pl.when(jnp.logical_and(s >= 1, jnp.logical_not(has_in)))
            def _():
                o_send[d, to, p] = part[at].astype(BF16)
                ml_send[d, to, p] = part_ml[at]

            @pl.when(s >= 1)
            def _():
                rcopy(ml_send.at[d, to, p], ml_recv.at[d, to, p], mtx.at[d, to, p], mrx.at[d, to, p], nbr(d)).start()
                rcopy(o_send.at[d, to, p], o_recv.at[d, to, p], otx.at[d, to, p], orx.at[d, to, p], nbr(d)).start()

            @pl.when(s == 0)
            def _():
                for dd in range(2):
                    incoming(dd, 0, p)
                w, m, l = scales([part_ml[at], ml_recv[0, 0, p], ml_recv[1, 0, p]])
                to_rows = pl.multiple_of(p * 128, 128)
                for e in range(2):
                    for j in range(2):
                        r = slice(2 * j + e, 2 * j + e + 1)
                        tot = (tile(part.at[at], e, j) * w[0][r] + tile(o_recv.at[0, 0, p], e, j) * w[1][r]
                               + tile(o_recv.at[1, 0, p], e, j) * w[2][r])
                        a_half[1, j, pl.ds(to_rows + e * 64, 64), :] = (tot / l[r]).astype(BF16)

        q_own(0)
        q_own(1)
        @pl.when(has_mem)
        def _():
            top_s[...] = score_all(S, 0, keys_of(GROUPS[0] // 16), head_rhs(z, GROUPS[0] // 16, 0), KBC)

        def step(k, at):
            ia, ir = at
            n = count_of(k)
            ja, jr = ia + lax.rem(n, 8), ir + n // 8
            lax.fori_loop(ia, ja, arrival, 0)

            def ret(i, _):
                reduce_step(return_of(i))
                return 0

            lax.fori_loop(ir, jr, ret, 0)
            groups = [decode(group_of(2 * k + i)) for i in range(3)]
            pl.when(has_mem)(lambda: cross_groups(*groups))
            return ja, jr

        lax.fori_loop(0, len(COUNTS), step, (jnp.int32(0), jnp.int32(0)))

        @pl.when(more)
        def _():
            nxt[CK].wait()
            nxt[CV].wait()

        def finish(i, b):
            v = last_of(i)
            n = jnp.where(jnp.logical_and(more, has_mem), v // 64, 0)
            lax.fori_loop(b, jnp.minimum(b + n, KBC), memory_block, 0)
            reduce_step(lax.rem(v, 64))

            @pl.when(lax.rem(v, 8) == 0)
            def _():
                p = lax.rem(v // 16, 4)
                pair_swap(p).start()
                pair_project(a_half[1, c, pair_rows(p)], my_cols, p)
            return b + n

        cur[CO].wait()
        for n in CT:
            upd(0, n)[...] = hid[:, cols(n)].astype(F32)

        lax.fori_loop(0, len(LAST), finish, jnp.int32(0))

        @pl.when(l + 2 < n_layers)
        def _():
            after = wcopies(jnp.minimum(l + 2, n_layers - 1))
            after[CK].start()
            after[CV].start()

        for v in LAST[-NP:]:
            p = v % 64 // 16
            pair_swap(p).wait()
            pair_project(att_c[pair_rows(p)], other_cols, p)
        for n in CT:
            hid[:, cols(n)] = upd(0, n)[...].astype(BF16)
        prefetch(CO)

        xm = rms_norm(hid[...], gain(g_mlp, l))

        for p in range(NP):
            for d in range(2):
                for s in range(4):
                    if s < 3 or p % 2 == d:
                        src = q_all.at[z, p]
                        rcopy(src, src, qtx.at[d, s, p], qrx.at[d, s, p], nbr(d)).wait_send()
                        rcopy(o_send.at[d, s, p], o_recv.at[d, s, p], otx.at[d, s, p], orx.at[d, s, p], nbr(d)).wait_send()
                        rcopy(ml_send.at[d, s, p], ml_recv.at[d, s, p], mtx.at[d, s, p], mrx.at[d, s, p], nbr(d)).wait_send()

        for f in range(NF):
            gate_copy(l, f).wait()
            up_copy(l, f).wait()
        cur[WD].wait()
        acts = []
        for f in range(NF):
            gt = dot(xm, wg[f])
            up = dot(xm, wu[f])
            acts.append((gt * lax.logistic(gt) * up).astype(BF16))
        full = jnp.concatenate(acts, axis=1)

        @pl.when(more)
        def _():
            for f in range(NF):
                gate_copy(l + 1, f).start()
                up_copy(l + 1, f).start()
        for n in CT:
            hid[:, cols(n)] = (hid[:, cols(n)].astype(F32) + dot(full, wd[:, cols(n)])).astype(BF16)
        prefetch(WD)
        return carry

    lax.fori_loop(0, n_layers, layer_body, 0)
    out[...] = hid[...].astype(F32)


def solution(mesh):
    n_dev = mesh.shape["sp"]

    def local_step(hidden, memory, mem_len, norm_self, norm_cross, norm_mlp, self_q, self_k, self_v, self_o,
                   cross_q, cross_k, cross_v, cross_o, mlp_gate, mlp_up, mlp_down):
        rows, D = hidden.shape
        mem_rows = memory.shape[0]
        L, heads, head_dim = self_o.shape[:3]
        FF = mlp_gate.shape[2]
        Dc = D // 2
        NP = Dc // 128
        Z = n_dev // 2
        KBC = 2 * mem_rows // T
        NF = FF // T
        any_ = pl.BlockSpec(memory_space=pl.ANY)
        vmem = pl.BlockSpec(memory_space=pltpu.VMEM)
        smem = pl.BlockSpec(memory_space=pltpu.SMEM)
        dma = pltpu.SemaphoreType.DMA
        V = pltpu.VMEM
        scratch = [
            V((rows, D), BF16),
            V((Z, 2 * rows, D), BF16),
            V((2, mem_rows, D), BF16),
            V((Z, NP, T, 128), BF16),
            V((Z, NP, 128, T), BF16),
            V((KBC, NP, T, 128), BF16),
            V((KBC, NP, 128, T), BF16),
            V((KBC, T, 128), BF16),
            V((2 * NP, 128, T), BF16),
            V((Z, NP, 128, T), BF16),
            V((2, max(2 * NP, KBC) * T, T), F32),
            V((8, T), F32),
            V((D, Dc), BF16), V((D, Dc), BF16), V((D, Dc), BF16), V((D, D), BF16),
            V((D, Dc), BF16), V((D, Dc), BF16), V((D, Dc), BF16), V((D, D), BF16),
            V((NF, D, T), BF16), V((NF, D, T), BF16), V((FF, D), BF16),
            V((8 * NP, 128, T), F32),
            V((8 * NP, 8, 128), F32),
            V((2, 4, NP, 128, T), BF16),
            V((2, 4, NP, 8, 128), F32),
            V((2, 4, NP, 128, T), BF16),
            V((2, 4, NP, 8, 128), F32),
            V((2 * NP, 64, T), F32),
            V((8, T), F32), V((8, T), F32),
            V((2, 2, Dc, 128), BF16),
            V((2, Dc, 128), BF16), V((Dc, 128), BF16),
            V((rows, D), BF16),
            dma((2, 5, 4)), dma((2, 5, 4)), dma((Z, 4)), dma((Z, 4)),
            dma((2, 5, NP)), dma((2, 5, NP)),
            dma((2, 4, NP)), dma((2, 4, NP)), dma((2, 4, NP)), dma((2, 4, NP)),
            dma((NP,)), dma((NP,)),
            dma((4,)), dma((4,)), dma((9,)), dma((NF,)), dma((NF,)), dma((2,)),
        ]
        call = pl.pallas_call(
            functools.partial(kernel, n_dev, head_dim, L),
            out_shape=jax.ShapeDtypeStruct((rows, D), F32),
            in_specs=[smem, any_, any_, vmem, vmem, vmem] + [any_] * 11,
            out_specs=vmem,
            scratch_shapes=scratch,
            compiler_params=pltpu.CompilerParams(
                collective_id=0, has_side_effects=True, vmem_limit_bytes=67043328),
            name="decoder",
        )
        return call(mem_len, hidden, memory, norm_self, norm_cross, norm_mlp,
                    self_q, self_k, self_v, self_o.reshape(L, D, D), cross_q, cross_k, cross_v,
                    cross_o.reshape(L, D, D), mlp_gate, mlp_up, mlp_down).astype(BF16)

    row_spec = P(("dp", "sp"), None)
    return jax.shard_map(local_step, mesh=mesh, in_specs=(row_spec, row_spec, P("dp")) + (P(),) * 14,
                         out_specs=row_spec, check_vma=False)
```

```python
import functools
import math

import jax
import jax.numpy as jnp
from jax import lax
from jax.experimental import pallas as pl
from jax.experimental.pallas import tpu as pltpu
from jax.sharding import PartitionSpec as P

MESH = pl.DeviceIdType.MESH
EPS = 1e-6
NEG = -1e30
T = 256
F32 = jnp.float32
BF16 = jnp.bfloat16

def unpack(bits, count, *words):
    per = 84 // bits
    return [(words[i // per] >> (i % per * bits)) % 2 ** bits for i in range(count)]


GROUPS = unpack(6, 32, 0xea2682c59851260040c10, 0xab3ad3f0b93b7048c36ca, 0xa72e52)
ARRIVALS = unpack(6, 30, 0xe229a0b9c61651241c20, 0xa9391cef310b8e96f24ba, 0xafc)
RETURNS = unpack(6, 20, 0x8ab6932fcec291c1230db, 0xa81e92cca)
COUNTS = unpack(6, 16, 0x6116534cc0440c1102081, 0x818)
LAST = unpack(9, 12, 0x90389e452a128824e419, 0xc00020)


def table(values, bits):
    per = 30 // bits
    words = [sum(v << (bits * j) for j, v in enumerate(values[i:i + per])) for i in range(0, len(values), per)]

    def get(i):
        w = jnp.int32(words[0])
        for k, v in enumerate(words[1:], 1):
            w = jnp.where(i >= k * per, jnp.int32(v), w)
        return lax.rem(lax.shift_right_logical(w, lax.rem(i, per) * bits), 1 << bits)

    return get


def decode(v):
    return lax.rem(v, 8), lax.rem(v // 8, 2), lax.rem(v // 16, 4)


def dot(a, b):
    return jnp.dot(a, b, preferred_element_type=F32)


def fold_max(x):
    return jnp.max(x.reshape(x.shape[0] // 8, 8, x.shape[1]), axis=0)


def fold_sum(x):
    return jnp.sum(x.reshape(x.shape[0] // 8, 8, x.shape[1]), axis=0)


def one_head(qt, e):
    rest = jnp.zeros((64, qt.shape[1]), BF16)
    return jnp.concatenate([qt[0:64], rest] if e == 0 else [rest, qt[64:128]], axis=0)


def ones_row(cols):
    row = lax.broadcasted_iota(jnp.int32, (128, cols), 0)
    return jnp.where(row == 0, 1.0, 0.0).astype(BF16)


def scores(S, slot, keys, rhs, b):
    s = dot(keys(b), rhs)
    S[slot, b * T:(b + 1) * T, :] = s
    return fold_max(s)


def score_all(S, slot, keys, rhs, blocks):
    return functools.reduce(jnp.maximum, [scores(S, slot, keys, rhs, b) for b in range(blocks)])


def score_and_sum(S, slot, keys, rhs, slot_v, values, top, blocks, c):
    ahead = min(3, blocks)
    m = jnp.max(top, axis=0, keepdims=True)
    tops = [scores(S, slot, keys, rhs, b) for b in range(ahead)]
    part = jnp.zeros((8, T), F32)
    num = jnp.zeros((64, T), F32)
    for b in range(blocks):
        p = jnp.exp2((S[slot_v, b * T:(b + 1) * T, :] - m) * c)
        part = part + fold_sum(p)
        num = num + dot(values(b), p.astype(BF16))
        if b + ahead < blocks:
            tops.append(scores(S, slot, keys, rhs, b + ahead))
    return functools.reduce(jnp.maximum, tops), num, jnp.sum(part, axis=0, keepdims=True), m


def rms_norm(h, g):
    h = h.astype(F32)
    inv = lax.rsqrt(jnp.mean(h * h, axis=-1, keepdims=True) + EPS)
    return (h * inv * g).astype(BF16)


def kernel(n_dev, head_dim, n_layers,
           mem_len, hid_in, mem_in, g_self, g_cross, g_mlp,
           self_q, self_k, self_v, self_o, cross_q, cross_k, cross_v, cross_o, mlp_g, mlp_u, mlp_d,
           out,
           hid, x_all, mem, ks, vs, kc, vc, bias, qm, q_all, S, top_s,
           wq, wk, wv, wo, cq, ck, cv, co, wg, wu, wd,
           part, part_ml, o_send, ml_send, o_recv, ml_recv,
           s_num, s_max, s_sum, a_half, att, att_c, hid_p,
           xtx, xrx, ptx, prx, qtx, qrx, otx, orx, mtx, mrx, ctx, crx, dtx, drx, wsem, gsem, usem, isem):
    Z = n_dev // 2
    rows, D = hid.shape
    piece = rows // 4
    NP = q_all.shape[1]
    KBC = kc.shape[0]
    NF = wg.shape[0]
    Dc = D // 2
    mem_rows = mem_in.shape[0]
    c_exp = math.log2(math.e) * head_dim ** -0.5
    assert KBC <= Z

    me = lax.axis_index("sp")
    z = me // 2
    c = me % 2
    partner = z * 2 + (1 - c)

    def ring(k):
        return lax.rem(z + k * (1 - 2 * c) + 2 * Z, Z)

    def nbr(d):
        return ring(1 - 2 * d) * 2 + c

    def rcopy(src, dst, ssem, rsem, dev):
        return pltpu.make_async_remote_copy(src_ref=src, dst_ref=dst, send_sem=ssem, recv_sem=rsem,
                                            device_id={"sp": dev}, device_id_type=MESH)

    has_mem = z * (2 * mem_rows) < n_dev * mem_rows * 3 // 4
    my_rows = pl.multiple_of(c * rows, rows)
    my_cols = pl.multiple_of(c * Dc, Dc)
    other_cols = pl.multiple_of((1 - c) * Dc, Dc)

    barrier = pltpu.get_barrier_semaphore()
    for dev in (nbr(0), nbr(1), partner):
        pl.semaphore_signal(barrier, inc=1, device_id={"sp": dev}, device_id_type=MESH)

    def wcopies(l):
        mine = pl.ds(my_cols, Dc)
        w = [
            (self_k.at[l, :, mine], wk), (self_q.at[l, :, mine], wq), (self_v.at[l, :, mine], wv),
            (cross_k.at[l, :, mine], ck), (cross_v.at[l, :, mine], cv),
            (self_o.at[l], wo), (cross_q.at[l, :, mine], cq), (cross_o.at[l], co), (mlp_d.at[l], wd),
        ]
        return [pltpu.make_async_copy(s, d, wsem.at[i]) for i, (s, d) in enumerate(w)]

    WK, WQ, WV, CK, CV, WO, CQ, CO, WD = range(9)

    def gate_copy(l, f):
        return pltpu.make_async_copy(mlp_g.at[l, :, pl.ds(f * T, T)], wg.at[f], gsem.at[f])

    def up_copy(l, f):
        return pltpu.make_async_copy(mlp_u.at[l, :, pl.ds(f * T, T)], wu.at[f], usem.at[f])

    hid_copy = pltpu.make_async_copy(hid_in, hid, isem.at[0])
    mem_copy = pltpu.make_async_copy(mem_in, mem.at[c], isem.at[1])
    mem_swap = rcopy(mem_in, mem.at[c], dtx.at[3], drx.at[3], partner)
    hid_copy.start()
    first = wcopies(0)
    for i in (WQ, WK, WV):
        first[i].start()
    mem_copy.start()
    for i in (CK, CV):
        first[i].start()

    hid_copy.wait()

    def gain(ref, l):
        g = jnp.zeros((1, D), F32)
        for i in range(n_layers):
            g = jnp.where(l == i, ref[i:i + 1, :].astype(F32), g)
        return g

    def kv_blocks(x, wk_ref, wv_ref, kdst, vdst, *at):
        v = dot(x, wv_ref[...])
        k = dot(x, wk_ref[...]).astype(BF16)
        for i, b in enumerate(at):
            r = slice(i * T, (i + 1) * T)
            for p in range(NP):
                vdst[b, p] = jnp.transpose(v[r, p * 128:(p + 1) * 128]).astype(BF16)
            for p in range(NP):
                kdst[b, p] = k[r, p * 128:(p + 1) * 128]

    def memory_block(b, _):
        per = mem_rows // T
        at = pl.ds(pl.multiple_of(lax.rem(b, per) * T, T), T)
        kv_blocks(mem[b // per, at, :], ck, cv, kc, vc, b)
        return 0

    def memory_pair(i):
        per = mem_rows // (2 * T)
        at = pl.ds(pl.multiple_of(lax.rem(i, per) * 2 * T, 2 * T), 2 * T)
        kv_blocks(mem[i // per, at, :], ck, cv, kc, vc, 2 * i, 2 * i + 1)

    def key_mask():
        length = mem_len[0]
        for b in range(KBC):
            key = z * (2 * mem_rows) + b * T + lax.broadcasted_iota(jnp.int32, (T, 128), 0)
            lane = lax.broadcasted_iota(jnp.int32, (T, 128), 1)
            bias[b] = jnp.where(jnp.logical_and(lane == 0, key >= length), NEG, 0.0).astype(BF16)

    def empty_parts():
        for i in range(part.shape[0]):
            part[i] = jnp.zeros(part.shape[1:], F32)
            row = lax.broadcasted_iota(jnp.int32, part_ml.shape[1:], 0)
            part_ml[i] = jnp.where(row < 4, NEG, 0.0)

    def rows_of(a):
        return jnp.transpose(a.astype(F32)).astype(BF16)

    CT = range(D // T)

    def cols(n):
        return slice(n * T, (n + 1) * T)

    def upd(j, n):
        return S.at[0, pl.ds(pl.multiple_of((j * len(CT) + n) * rows, rows), rows), :]

    def swap_project(w_ref, ready):
        swap = rcopy(a_half.at[0], att, dtx.at[0], drx.at[0], partner)
        swap.start()
        ready.wait()
        for j in range(2):
            own = rows_of(a_half[0, j])
            for n in CT:
                upd(j, n)[...] = dot(own, w_ref[pl.ds(my_cols, Dc), cols(n)])
        hid_swap().wait()
        swap.wait()
        for j in range(2):
            others = rows_of(att[j])
            for n in CT:
                own, other = upd(j, n)[...], dot(others, w_ref[pl.ds(other_cols, Dc), cols(n)])
                before = jnp.where(c == j, hid[:, cols(n)], hid_p[:, cols(n)]).astype(F32)
                upd(j, n)[...] = before + jnp.where(c == 0, own, other) + jnp.where(c == 0, other, own)
        for n in CT:
            hid[:, cols(n)] = upd(c, n)[...].astype(BF16)

    def hid_swap():
        return rcopy(hid, hid_p, dtx.at[2], drx.at[2], partner)

    def pair_rows(p):
        return pl.ds(pl.multiple_of(p * 128, 128), 128)

    def pair_swap(p):
        return rcopy(a_half.at[1, 1 - c, pair_rows(p)], att_c.at[pair_rows(p)], ctx.at[p], crx.at[p], partner)

    def pair_project(a, base, p):
        a = rows_of(a)
        for n in CT:
            upd(0, n)[...] += dot(a, co[pl.ds(pl.multiple_of(base + p * 128, 128), 128), cols(n)])

    group_of = table(GROUPS + GROUPS[-1:], 6)
    count_of = table(COUNTS, 6)
    arrival_of = table(ARRIVALS, 6)
    return_of = table(RETURNS, 6)
    last_of = table(LAST, 9)

    def drain_ring():
        for p in range(NP):
            for d in range(2):
                for s in range(4):
                    if s < 3 or p % 2 == d:
                        src = q_all.at[z, p]
                        rcopy(src, src, qtx.at[d, s, p], qrx.at[d, s, p], nbr(d)).wait_send()
                        rcopy(o_send.at[d, s, p], o_recv.at[d, s, p], otx.at[d, s, p], orx.at[d, s, p], nbr(d)).wait_send()
                        rcopy(ml_send.at[d, s, p], ml_recv.at[d, s, p], mtx.at[d, s, p], mrx.at[d, s, p], nbr(d)).wait_send()

    def layer_body(l, carry):
        more = l + 1 < n_layers
        cur = wcopies(l)
        nxt = wcopies(jnp.minimum(l + 1, n_layers - 1))

        def prefetch(*ids):
            @pl.when(more)
            def _():
                for i in ids:
                    nxt[i].start()

        x_all[z, pl.ds(my_rows, rows), :] = rms_norm(hid[...], gain(g_self, l))

        @pl.when(l == 0)
        def _():
            pl.semaphore_wait(barrier, 3)

        def xslot(o, h):
            return x_all.at[o, pl.ds(pl.multiple_of(c * rows + h * piece, piece), piece), :]

        def pslot(o, h):
            return x_all.at[o, pl.ds(pl.multiple_of((1 - c) * rows + h * piece, piece), piece), :]

        for h in range(4):
            src = xslot(z, h)
            for d in range(2):
                rcopy(src, src, xtx.at[d, 0, h], xrx.at[d, 1, h], nbr(d)).start()
            rcopy(src, src, ptx.at[z, h], prx.at[z, h], partner).start()

        hid_swap().start()
        @pl.when(l == 0)
        def _():
            mem_swap.start()
            key_mask()
            pl.when(jnp.logical_not(has_mem))(empty_parts)

        pl.when(l > 0)(drain_ring)
        for i in (WO, CQ, CO, WD):
            cur[i].start()
        for f in range(NF):
            gate_copy(l, f).start()
            up_copy(l, f).start()


        def x_event(d, s, h):
            o = ring(-(1 - 2 * d) * s)
            src = xslot(o, h)

            @pl.when(jnp.logical_or(s <= 3, h % 2 == d))
            def _():
                rcopy(src, src, xtx.at[d, s, h], xrx.at[d, s, h], nbr(d)).wait_recv()

                @pl.when(jnp.logical_or(s < 3, jnp.logical_and(s == 3, h % 2 == d)))
                def _():
                    rcopy(src, src, xtx.at[d, s, h], xrx.at[d, s + 1, h], nbr(d)).start()
                rcopy(src, src, ptx.at[o, h], prx.at[o, h], partner).start()

        def partner_rows(o):
            for h in range(4):
                dst = pslot(o, h)
                rcopy(dst, dst, ptx.at[o, h], prx.at[o, h], partner).wait_recv()

        delta = (lax.broadcasted_iota(jnp.int32, (T, T), 0) - lax.broadcasted_iota(jnp.int32, (T, T), 1))

        def attend(start, *blocks):
            tops = []
            for h in range(2 * NP):
                top = None
                for i, o in enumerate(blocks):
                    s = dot(ks[o, h // 2], qm[h])
                    if start:
                        s = jnp.where(delta <= 0, s, NEG)
                    S[i, h * T:(h + 1) * T, :] = s
                    top = fold_max(s) if top is None else jnp.maximum(top, fold_max(s))
                tops.append(top)
            for h in range(2 * NP):
                m = jnp.max(tops[h], axis=0, keepdims=True)
                e = h % 2
                if not start:
                    old = s_max[h:h + 1, :]
                    m = jnp.maximum(m, old)
                part_sum = jnp.zeros((8, T), F32)
                num = jnp.zeros((64, T), F32)
                for i, o in enumerate(blocks):
                    p = jnp.exp2((S[i, h * T:(h + 1) * T, :] - m) * c_exp)
                    part_sum = part_sum + fold_sum(p)
                    num = num + dot(vs[o, h // 2, e * 64:(e + 1) * 64, :], p.astype(BF16))
                tot = jnp.sum(part_sum, axis=0, keepdims=True)
                if not start:
                    keep = jnp.exp2((old - m) * c_exp)
                    tot = tot + s_sum[h:h + 1, :] * keep
                    num = num + s_num[h] * keep
                s_max[h:h + 1, :] = m
                s_sum[h:h + 1, :] = tot
                s_num[h] = num

        for i in (WQ, WK, WV):
            cur[i].wait()
        partner_rows(z)
        q = dot(x_all[z], wq[...])
        for p in range(NP):
            qt = jnp.transpose(q[:, p * 128:(p + 1) * 128]).astype(BF16)
            for e in range(2):
                qm[2 * p + e] = one_head(qt, e)
        kv_blocks(x_all[z], wk, wv, ks, vs, z)
        attend(True, z)

        def memory_part(i):
            @pl.when(l == 0)
            def _():
                @pl.when(i == 0)
                def _():
                    cur[CK].wait()
                    cur[CV].wait()
                    mem_copy.wait()
                    mem_swap.wait()
            pl.when(jnp.logical_and(has_mem, i < KBC // 2))(lambda: memory_pair(i))

        def earlier(s, one, two):
            o, q = ring(s), ring(-s)
            pl.when(jnp.logical_and(o < z, q < z))(lambda: two(o, q))
            pl.when(jnp.logical_xor(o < z, q < z))(lambda: one(jnp.minimum(o, q)))

        def attend_level(s):
            earlier(s, lambda o: attend(False, o), lambda o, q: attend(False, o, q))

        def project_level(s):
            earlier(s, lambda o: kv_blocks(x_all[o], wk, wv, ks, vs, o),
                    lambda o, q: kv_blocks(jnp.concatenate([x_all[o], x_all[q]], axis=0), wk, wv, ks, vs, o, q))

        def level(s, _):
            def arrivals(h):
                for d in range(2):
                    x_event(d, s, h)

            arrivals(0)
            arrivals(1)

            @pl.when(s == 1)
            def _():
                memory_part(0)

            @pl.when(s >= 2)
            def _():
                attend_level(s - 1)
            arrivals(2)
            arrivals(3)
            for o in (ring(s), ring(-s)):
                partner_rows(o)
            project_level(s)
            memory_part(s)
            return 0

        lax.fori_loop(1, Z // 2, level, 0)
        far = ring(Z // 2)
        for h in range(4):
            x_event(h % 2, Z // 2, h)
            if h == 1:
                attend_level(Z // 2 - 1)
        partner_rows(far)

        @pl.when(far < z)
        def _():
            kv_blocks(x_all[far], wk, wv, ks, vs, far)
            attend(False, far)
        for h in range(2 * NP):
            a = (s_num[h] / s_sum[h:h + 1, :]).astype(BF16)
            for j in range(2):
                a_half[0, j, h * 64:(h + 1) * 64, :] = a[:, j * 128:(j + 1) * 128]
        swap_project(wo, cur[WO])

        for j in range(2):
            mine = jnp.concatenate([upd(j, n)[...].astype(BF16) for n in CT], axis=1)
            x = rms_norm(mine, gain(g_cross, l))
            if j == 0:
                cur[CQ].wait()
            q = dot(x, cq[...])
            for p in range(NP):
                q_all[z, p, :, j * rows:(j + 1) * rows] = jnp.transpose(q[:, p * 128:(p + 1) * 128]).astype(BF16)

        def q_own(p):
            for d in range(2):
                src = q_all.at[z, p]
                rcopy(src, src, qtx.at[d, 0, p], qrx.at[d, 1, p], nbr(d)).start()

        def arrival(i, _):
            s, d, p = decode(arrival_of(i))

            @pl.when(s == 0)
            def _():
                q_own(p)

            @pl.when(s >= 1)
            def _():
                src = q_all.at[ring(-(1 - 2 * d) * s), p]
                rcopy(src, src, qtx.at[d, s, p], qrx.at[d, s, p], nbr(d)).wait_recv()

                @pl.when(jnp.logical_or(s < 3, jnp.logical_and(s == 3, lax.rem(p, 2) == d)))
                def _():
                    rcopy(src, src, qtx.at[d, s, p], qrx.at[d, s + 1, p], nbr(d)).start()
            return 0

        one = ones_row(T)

        def head_rhs(o, p, e):
            return jnp.concatenate([one_head(q_all[o, p], e), one], axis=0)

        def keys_of(p):
            return lambda b: jnp.concatenate([kc[b, p], bias[b]], axis=1)

        def place(s, d, p):
            return p * 8 + jnp.where(s == 0, 0, jnp.where(s == 4, 7, 2 * s - 1 + d))

        def origin(s, d):
            return ring(jnp.where(d == 0, -s, s))

        def cross_groups(*groups):
            where = [(origin(s, d), p, place(s, d, p)) for s, d, p in groups]
            heads = [(w, e) for w in where[:-1] for e in range(2)] + [(where[-1], 0)]
            top = top_s[...]
            stats = []
            for ((o, p, to), e), ((on, pn, _), en) in zip(heads, heads[1:]):
                top, num, l, m = score_and_sum(
                    S, en, keys_of(pn), head_rhs(on, pn, en),
                    e, lambda b: vc[b, p, e * 64:(e + 1) * 64, :], top, KBC, c_exp)
                part[to, e * 64:(e + 1) * 64, :] = num
                stats.append((m, l))
                if e == 1:
                    part_ml[to] = jnp.concatenate(
                        [x[k][:, j * 128:(j + 1) * 128] for k in range(2) for j in range(2) for x in stats[-2:]], axis=0)
            top_s[...] = top

        def incoming(d, s, p):
            rcopy(o_send.at[d, s, p], o_recv.at[d, s, p], otx.at[d, s, p], orx.at[d, s, p], nbr(d)).wait_recv()
            rcopy(ml_send.at[d, s, p], ml_recv.at[d, s, p], mtx.at[d, s, p], mrx.at[d, s, p], nbr(d)).wait_recv()

        def scales(mls):
            m = functools.reduce(jnp.maximum, [x[0:4] for x in mls])
            w = [jnp.exp2((x[0:4] - m) * c_exp) for x in mls]
            return w, m, sum(x[4:8] * y for x, y in zip(mls, w))

        def tile(ref, e, j):
            return ref[e * 64:(e + 1) * 64, j * 128:(j + 1) * 128].astype(F32)

        def reduce_step(v):
            s, d_arr, p = decode(v)
            at = place(s, d_arr, p)
            d = jnp.where(s == 4, lax.rem(p, 2), 1 - d_arr)
            has_in = jnp.logical_and(s >= 1, jnp.logical_or(s < 3, jnp.logical_and(s == 3, lax.rem(p, 2) == d)))
            to = jnp.maximum(s - 1, 0)

            def send():
                rcopy(o_send.at[d, to, p], o_recv.at[d, to, p], otx.at[d, to, p], orx.at[d, to, p], nbr(d)).start()
                rcopy(ml_send.at[d, to, p], ml_recv.at[d, to, p], mtx.at[d, to, p], mrx.at[d, to, p], nbr(d)).start()

            @pl.when(has_in)
            def _():
                incoming(d, s, p)
                (wa, wb), m, l = scales([part_ml[at], ml_recv[d, s, p]])
                ml_send[d, to, p] = jnp.concatenate([m, l], axis=0)
                for e in range(2):
                    for j in range(2):
                        r = slice(2 * j + e, 2 * j + e + 1)
                        o_send[d, to, p, e * 64:(e + 1) * 64, j * 128:(j + 1) * 128] = (
                            tile(part.at[at], e, j) * wa[r] + tile(o_recv.at[d, s, p], e, j) * wb[r]).astype(BF16)
                send()

            @pl.when(jnp.logical_and(s >= 1, jnp.logical_not(has_in)))
            def _():
                o_send[d, to, p] = part[at].astype(BF16)
                ml_send[d, to, p] = part_ml[at]
                send()

            @pl.when(s == 0)
            def _():
                for dd in range(2):
                    incoming(dd, 0, p)
                w, m, l = scales([part_ml[at], ml_recv[0, 0, p], ml_recv[1, 0, p]])
                to_rows = pl.multiple_of(p * 128, 128)
                for e in range(2):
                    for j in range(2):
                        r = slice(2 * j + e, 2 * j + e + 1)
                        tot = (tile(part.at[at], e, j) * w[0][r] + tile(o_recv.at[0, 0, p], e, j) * w[1][r]
                               + tile(o_recv.at[1, 0, p], e, j) * w[2][r])
                        a_half[1, j, pl.ds(to_rows + e * 64, 64), :] = (tot / l[r]).astype(BF16)

        q_own(0)
        q_own(1)
        @pl.when(has_mem)
        def _():
            top_s[...] = score_all(S, 0, keys_of(GROUPS[0] // 16), head_rhs(z, GROUPS[0] // 16, 0), KBC)

        for h in range(4):
            for d in range(2):
                for s in range(4):
                    if s < 3 or h % 2 == d:
                        src = xslot(z, h)
                        rcopy(src, src, xtx.at[d, s, h], xrx.at[d, s, h], nbr(d)).wait_send()
            for o in range(Z):
                src = xslot(o, h)
                rcopy(src, src, ptx.at[o, h], prx.at[o, h], partner).wait_send()
        for f in range(NF):
            gate_copy(l, f).wait()
            up_copy(l, f).wait()
        for i in (WD, CO):
            cur[i].wait()
        prefetch(WK, WQ, WV)

        @pl.when(l == 0)
        def _():
            prefetch(CK, CV)

        def step(k, at):
            ia, ir = at
            n = count_of(k)
            ja, jr = ia + lax.rem(n, 8), ir + n // 8
            lax.fori_loop(ia, ja, arrival, 0)

            def ret(i, _):
                reduce_step(return_of(i))
                return 0

            lax.fori_loop(ir, jr, ret, 0)
            groups = [decode(group_of(2 * k + i)) for i in range(3)]
            pl.when(has_mem)(lambda: cross_groups(*groups))
            return ja, jr

        lax.fori_loop(0, len(COUNTS), step, (jnp.int32(0), jnp.int32(0)))

        @pl.when(more)
        def _():
            nxt[CK].wait()
            nxt[CV].wait()

        def finish(i, b):
            v = last_of(i)
            n = jnp.where(jnp.logical_and(more, has_mem), v // 64, 0)
            lax.fori_loop(b, jnp.minimum(b + n, KBC), memory_block, 0)
            reduce_step(lax.rem(v, 64))

            @pl.when(lax.rem(v, 8) == 0)
            def _():
                p = lax.rem(v // 16, 4)
                pair_swap(p).start()
                pair_project(a_half[1, c, pair_rows(p)], my_cols, p)
            return b + n

        for n in CT:
            upd(0, n)[...] = hid[:, cols(n)].astype(F32)

        lax.fori_loop(0, len(LAST), finish, jnp.int32(0))

        @pl.when(l + 2 < n_layers)
        def _():
            after = wcopies(jnp.minimum(l + 2, n_layers - 1))
            after[CK].start()
            after[CV].start()

        for v in LAST[-NP:]:
            p = v % 64 // 16
            pair_swap(p).wait()
            pair_project(att_c[pair_rows(p)], other_cols, p)
        for n in CT:
            hid[:, cols(n)] = upd(0, n)[...].astype(BF16)

        xm = rms_norm(hid[...], gain(g_mlp, l))

        acts = []
        for f in range(NF):
            gt = dot(xm, wg[f])
            up = dot(xm, wu[f])
            acts.append((gt * lax.logistic(gt) * up).astype(BF16))
        full = jnp.concatenate(acts, axis=1)

        for n in CT:
            hid[:, cols(n)] = (hid[:, cols(n)].astype(F32) + dot(full, wd[:, cols(n)])).astype(BF16)
        return carry

    lax.fori_loop(0, n_layers, layer_body, 0)
    drain_ring()
    out[...] = hid[...]


def solution(mesh):
    n_dev = mesh.shape["sp"]

    def local_step(hidden, memory, mem_len, norm_self, norm_cross, norm_mlp, self_q, self_k, self_v, self_o,
                   cross_q, cross_k, cross_v, cross_o, mlp_gate, mlp_up, mlp_down):
        rows, D = hidden.shape
        mem_rows = memory.shape[0]
        L, heads, head_dim = self_o.shape[:3]
        FF = mlp_gate.shape[2]
        Dc = D // 2
        NP = Dc // 128
        Z = n_dev // 2
        KBC = 2 * mem_rows // T
        NF = FF // T
        any_ = pl.BlockSpec(memory_space=pl.ANY)
        vmem = pl.BlockSpec(memory_space=pltpu.VMEM)
        smem = pl.BlockSpec(memory_space=pltpu.SMEM)
        dma = pltpu.SemaphoreType.DMA
        V = pltpu.VMEM
        scratch = [
            V((rows, D), BF16),
            V((Z, 2 * rows, D), BF16),
            V((2, mem_rows, D), BF16),
            V((Z, NP, T, 128), BF16),
            V((Z, NP, 128, T), BF16),
            V((KBC, NP, T, 128), BF16),
            V((KBC, NP, 128, T), BF16),
            V((KBC, T, 128), BF16),
            V((2 * NP, 128, T), BF16),
            V((Z, NP, 128, T), BF16),
            V((2, max(2 * NP, KBC) * T, T), F32),
            V((8, T), F32),
            V((D, Dc), BF16), V((D, Dc), BF16), V((D, Dc), BF16), V((D, D), BF16),
            V((D, Dc), BF16), V((D, Dc), BF16), V((D, Dc), BF16), V((D, D), BF16),
            V((NF, D, T), BF16), V((NF, D, T), BF16), V((FF, D), BF16),
            V((8 * NP, 128, T), F32),
            V((8 * NP, 8, 128), F32),
            V((2, 4, NP, 128, T), BF16),
            V((2, 4, NP, 8, 128), F32),
            V((2, 4, NP, 128, T), BF16),
            V((2, 4, NP, 8, 128), F32),
            V((2 * NP, 64, T), F32),
            V((8, T), F32), V((8, T), F32),
            V((2, 2, Dc, 128), BF16),
            V((2, Dc, 128), BF16), V((Dc, 128), BF16),
            V((rows, D), BF16),
            dma((2, 5, 4)), dma((2, 5, 4)), dma((Z, 4)), dma((Z, 4)),
            dma((2, 5, NP)), dma((2, 5, NP)),
            dma((2, 4, NP)), dma((2, 4, NP)), dma((2, 4, NP)), dma((2, 4, NP)),
            dma((NP,)), dma((NP,)),
            dma((4,)), dma((4,)), dma((9,)), dma((NF,)), dma((NF,)), dma((2,)),
        ]
        call = pl.pallas_call(
            functools.partial(kernel, n_dev, head_dim, L),
            out_shape=jax.ShapeDtypeStruct((rows, D), BF16),
            in_specs=[smem, any_, any_, vmem, vmem, vmem] + [any_] * 11,
            out_specs=vmem,
            scratch_shapes=scratch,
            compiler_params=pltpu.CompilerParams(
                collective_id=0, has_side_effects=True, vmem_limit_bytes=67043328),
            name="decoder",
        )
        return call(mem_len, hidden, memory, norm_self, norm_cross, norm_mlp,
                    self_q, self_k, self_v, self_o.reshape(L, D, D), cross_q, cross_k, cross_v,
                    cross_o.reshape(L, D, D), mlp_gate, mlp_up, mlp_down)

    row_spec = P(("dp", "sp"), None)
    return jax.shard_map(local_step, mesh=mesh, in_specs=(row_spec, row_spec, P("dp")) + (P(),) * 14,
                         out_specs=row_spec, check_vma=False)
```

```python
import functools
import math

import jax
import jax.numpy as jnp
from jax import lax
from jax.experimental import pallas as pl
from jax.experimental.pallas import tpu as pltpu
from jax.sharding import PartitionSpec as P

MESH = pl.DeviceIdType.MESH
EPS = 1e-6
NEG = -1e30
T = 256
F32 = jnp.float32
BF16 = jnp.bfloat16

def unpack(bits, count, *words):
    per = 84 // bits
    return [(words[i // per] >> (i % per * bits)) % 2 ** bits for i in range(count)]


GROUPS = unpack(6, 32, 0xea2682c59851260040c10, 0xab3ad3f0b93b7048c36ca, 0xa72e52)
ARRIVALS = unpack(6, 30, 0xe229a0b9c61651241c20, 0xa9391cef310b8e96f24ba, 0xafc)
RETURNS = unpack(6, 20, 0x8ab6932fcec291c1230db, 0xa81e92cca)
COUNTS = unpack(6, 16, 0x6116534cc0440c1102081, 0x818)
LAST = unpack(9, 12, 0x90389e452a128824e419, 0xc00020)


def table(values, bits):
    per = 30 // bits
    words = [sum(v << (bits * j) for j, v in enumerate(values[i:i + per])) for i in range(0, len(values), per)]

    def get(i):
        w = jnp.int32(words[0])
        for k, v in enumerate(words[1:], 1):
            w = jnp.where(i >= k * per, jnp.int32(v), w)
        return lax.rem(lax.shift_right_logical(w, lax.rem(i, per) * bits), 1 << bits)

    return get


def decode(v):
    return lax.rem(v, 8), lax.rem(v // 8, 2), lax.rem(v // 16, 4)


def dot(a, b):
    return jnp.dot(a, b, preferred_element_type=F32)


def fold_max(x):
    return jnp.max(x.reshape(x.shape[0] // 8, 8, x.shape[1]), axis=0)


def fold_sum(x):
    return jnp.sum(x.reshape(x.shape[0] // 8, 8, x.shape[1]), axis=0)


def one_head(qt, e):
    rest = jnp.zeros((64, qt.shape[1]), BF16)
    return jnp.concatenate([qt[0:64], rest] if e == 0 else [rest, qt[64:128]], axis=0)


def ones_row(cols):
    row = lax.broadcasted_iota(jnp.int32, (128, cols), 0)
    return jnp.where(row == 0, 1.0, 0.0).astype(BF16)


def scores(S, slot, keys, rhs, b):
    s = dot(keys(b), rhs)
    S[slot, b * T:(b + 1) * T, :] = s
    return fold_max(s)


def score_all(S, slot, keys, rhs, blocks):
    return functools.reduce(jnp.maximum, [scores(S, slot, keys, rhs, b) for b in range(blocks)])


def score_and_sum(S, slot, keys, rhs, slot_v, values, top, blocks, c):
    ahead = min(3, blocks)
    hi, lo = two_terms(jnp.max(top, axis=0, keepdims=True))
    m = hi.astype(F32) + lo.astype(F32)
    tops = [scores(S, slot, keys, rhs, b) for b in range(ahead)]
    part = jnp.zeros((8, T), F32)
    num = jnp.zeros((64, T), F32)
    for b in range(blocks):
        p = jnp.exp2((S[slot_v, b * T:(b + 1) * T, :] - m) * c)
        part = part + fold_sum(p)
        num = num + dot(values(b), p.astype(BF16))
        if b + ahead < blocks:
            tops.append(scores(S, slot, keys, rhs, b + ahead))
    return functools.reduce(jnp.maximum, tops), num, jnp.sum(part, axis=0, keepdims=True), m


def two_terms(x):
    hi = x.astype(BF16)
    return hi, (x - hi.astype(F32)).astype(BF16)


def rms_norm(h, g):
    h = h.astype(F32)
    inv = lax.rsqrt(jnp.mean(h * h, axis=-1, keepdims=True) + EPS)
    return (h * inv * g).astype(BF16)


def kernel(n_dev, head_dim, n_layers,
           mem_len, hid_in, mem_in, g_self, g_cross, g_mlp,
           self_q, self_k, self_v, self_o, cross_q, cross_k, cross_v, cross_o, mlp_g, mlp_u, mlp_d,
           out,
           hid, x_all, mem, ks, vs, kc, vc, bias, qm, q_all, S, top_s,
           wq, wk, wv, wo, cq, ck, cv, co, wg, wu, wd,
           part, part_ml, o_send, o_recv,
           s_num, s_max, s_sum, a_half, att, att_c, hid_p,
           xtx, xrx, ptx, prx, qtx, qrx, otx, orx, ctx, crx, dtx, drx, wsem, isem):
    Z = n_dev // 2
    rows, D = hid.shape
    piece = rows // 4
    NP = q_all.shape[1]
    KBC = kc.shape[0]
    NF = wg.shape[1] // T
    Dc = D // 2
    mem_rows = mem_in.shape[0]
    c_exp = math.log2(math.e) * head_dim ** -0.5
    assert KBC <= Z

    me = lax.axis_index("sp")
    z = me // 2
    c = me % 2
    partner = z * 2 + (1 - c)

    def ring(k):
        return lax.rem(z + k * (1 - 2 * c) + 2 * Z, Z)

    def nbr(d):
        return ring(1 - 2 * d) * 2 + c

    def rcopy(src, dst, ssem, rsem, dev):
        return pltpu.make_async_remote_copy(src_ref=src, dst_ref=dst, send_sem=ssem, recv_sem=rsem,
                                            device_id={"sp": dev}, device_id_type=MESH)

    has_mem = z * (2 * mem_rows) < n_dev * mem_rows * 3 // 4
    my_rows = pl.multiple_of(c * rows, rows)
    my_cols = pl.multiple_of(c * Dc, Dc)
    other_cols = pl.multiple_of((1 - c) * Dc, Dc)

    barrier = pltpu.get_barrier_semaphore()
    for dev in (nbr(0), nbr(1), partner):
        pl.semaphore_signal(barrier, inc=1, device_id={"sp": dev}, device_id_type=MESH)

    def wcopies(l):
        mine = pl.ds(my_cols, Dc)
        w = [
            (self_k.at[l, :, mine], wk), (self_q.at[l, :, mine], wq), (self_v.at[l, :, mine], wv),
            (cross_k.at[l, :, mine], ck), (cross_v.at[l, :, mine], cv),
            (self_o.at[l], wo), (cross_q.at[l, :, mine], cq), (cross_o.at[l], co),
            (mlp_g.at[l], wg), (mlp_u.at[l], wu), (mlp_d.at[l], wd),
        ]
        return [pltpu.make_async_copy(s, d, wsem.at[i]) for i, (s, d) in enumerate(w)]

    WK, WQ, WV, CK, CV, WO, CQ, CO, WG, WU, WD = range(11)

    hid_copy = pltpu.make_async_copy(hid_in, hid, isem.at[0])
    mem_copy = pltpu.make_async_copy(mem_in, mem.at[c], isem.at[1])
    mem_swap = rcopy(mem_in, mem.at[c], dtx.at[3], drx.at[3], partner)
    hid_copy.start()
    first = wcopies(0)
    for i in (WQ, WK, WV):
        first[i].start()
    mem_copy.start()
    for i in (CK, CV):
        first[i].start()

    hid_copy.wait()

    def gain(ref, l):
        g = jnp.zeros((1, D), F32)
        for i in range(n_layers):
            g = jnp.where(l == i, ref[i:i + 1, :].astype(F32), g)
        return g

    def kv_blocks(x, wk_ref, wv_ref, kdst, vdst, *at):
        v = dot(x, wv_ref[...])
        k = dot(x, wk_ref[...]).astype(BF16)
        for i, b in enumerate(at):
            r = slice(i * T, (i + 1) * T)
            for p in range(NP):
                vdst[b, p] = jnp.transpose(v[r, p * 128:(p + 1) * 128]).astype(BF16)
            for p in range(NP):
                kdst[b, p] = k[r, p * 128:(p + 1) * 128]

    def memory_block(b, _):
        per = mem_rows // T
        at = pl.ds(pl.multiple_of(lax.rem(b, per) * T, T), T)
        kv_blocks(mem[b // per, at, :], ck, cv, kc, vc, b)
        return 0

    def memory_pair(i):
        per = mem_rows // (2 * T)
        at = pl.ds(pl.multiple_of(lax.rem(i, per) * 2 * T, 2 * T), 2 * T)
        kv_blocks(mem[i // per, at, :], ck, cv, kc, vc, 2 * i, 2 * i + 1)

    def key_mask():
        length = mem_len[0]
        for b in range(KBC):
            key = z * (2 * mem_rows) + b * T + lax.broadcasted_iota(jnp.int32, (T, 128), 0)
            lane = lax.broadcasted_iota(jnp.int32, (T, 128), 1)
            bias[b] = jnp.where(jnp.logical_and(lane == 0, key >= length), NEG, 0.0).astype(BF16)

    def empty_parts():
        for i in range(part.shape[0]):
            part[i] = jnp.zeros(part.shape[1:], F32)
            row = lax.broadcasted_iota(jnp.int32, part_ml.shape[1:], 0)
            part_ml[i] = jnp.where(row < 4, NEG, 0.0)

    def rows_of(a):
        return jnp.transpose(a.astype(F32)).astype(BF16)

    CT = range(D // T)

    def cols(n):
        return slice(n * T, (n + 1) * T)

    def upd(j, n):
        return S.at[0, pl.ds(pl.multiple_of((j * len(CT) + n) * rows, rows), rows), :]

    def swap_project(w_ref, ready):
        swap = rcopy(a_half.at[0], att, dtx.at[0], drx.at[0], partner)
        swap.start()
        ready.wait()
        for j in range(2):
            own = rows_of(a_half[0, j])
            for n in CT:
                upd(j, n)[...] = dot(own, w_ref[pl.ds(my_cols, Dc), cols(n)])
        hid_swap().wait()
        swap.wait()
        for j in range(2):
            others = rows_of(att[j])
            for n in CT:
                own, other = upd(j, n)[...], dot(others, w_ref[pl.ds(other_cols, Dc), cols(n)])
                before = jnp.where(c == j, hid[:, cols(n)], hid_p[:, cols(n)]).astype(F32)
                upd(j, n)[...] = before + jnp.where(c == 0, own, other) + jnp.where(c == 0, other, own)
        for n in CT:
            hid[:, cols(n)] = upd(c, n)[...].astype(BF16)

    def hid_swap():
        return rcopy(hid, hid_p, dtx.at[2], drx.at[2], partner)

    def pair_rows(p):
        return pl.ds(pl.multiple_of(p * 128, 128), 128)

    def pair_swap(p):
        return rcopy(a_half.at[1, 1 - c, pair_rows(p)], att_c.at[pair_rows(p)], ctx.at[p], crx.at[p], partner)

    def pair_project(a, base, p):
        a = rows_of(a)
        for n in CT:
            upd(0, n)[...] += dot(a, co[pl.ds(pl.multiple_of(base + p * 128, 128), 128), cols(n)])

    group_of = table(GROUPS + GROUPS[-1:], 6)
    count_of = table(COUNTS, 6)
    arrival_of = table(ARRIVALS, 6)
    return_of = table(RETURNS, 6)
    last_of = table(LAST, 9)

    def drain_ring():
        for p in range(NP):
            pair_swap(p).wait_send()
        for d in range(2):
            for s in range(4):
                pairs = pl.ds(0, NP if s < 3 else NP // 2)
                src, part_out = q_all.at[z, pairs], o_send.at[d, s, pairs]
                rcopy(src, src, qtx.at[d, s], qrx.at[d, s, 0], nbr(d)).wait_send()
                rcopy(part_out, o_recv.at[d, s, pairs], otx.at[d, s], orx.at[d, s, 0], nbr(d)).wait_send()

    def layer_body(l, carry):
        more = l + 1 < n_layers
        cur = wcopies(l)
        nxt = wcopies(jnp.minimum(l + 1, n_layers - 1))

        def prefetch(*ids):
            @pl.when(more)
            def _():
                for i in ids:
                    nxt[i].start()

        x_all[z, pl.ds(my_rows, rows), :] = rms_norm(hid[...], gain(g_self, l))

        @pl.when(l == 0)
        def _():
            pl.semaphore_wait(barrier, 3)

        def xslot(o, h):
            return x_all.at[o, pl.ds(pl.multiple_of(c * rows + h * piece, piece), piece), :]

        for h in range(4):
            src = xslot(z, h)
            for d in range(2):
                rcopy(src, src, xtx.at[d, 0], xrx.at[d, 1, h], nbr(d)).start()
            rcopy(src, src, ptx.at[z], prx.at[z], partner).start()

        hid_swap().start()
        @pl.when(l == 0)
        def _():
            mem_swap.start()
            key_mask()
            pl.when(jnp.logical_not(has_mem))(empty_parts)

        pl.when(l > 0)(drain_ring)
        for i in (WO, CQ, CO, WG, WU, WD):
            cur[i].start()


        def x_event(d, s, h):
            o = ring(-(1 - 2 * d) * s)
            src = xslot(o, h)

            @pl.when(jnp.logical_or(s <= 3, h % 2 == d))
            def _():
                rcopy(src, src, xtx.at[d, s], xrx.at[d, s, h], nbr(d)).wait_recv()

                @pl.when(jnp.logical_or(s < 3, jnp.logical_and(s == 3, h % 2 == d)))
                def _():
                    rcopy(src, src, xtx.at[d, s], xrx.at[d, s + 1, h], nbr(d)).start()
                rcopy(src, src, ptx.at[o], prx.at[o], partner).start()

        def partner_rows(o):
            dst = x_all.at[o, pl.ds(pl.multiple_of((1 - c) * rows, rows), rows), :]
            rcopy(dst, dst, ptx.at[o], prx.at[o], partner).wait_recv()

        delta = (lax.broadcasted_iota(jnp.int32, (T, T), 0) - lax.broadcasted_iota(jnp.int32, (T, T), 1))

        def attend(start, *blocks):
            tops = []
            for h in range(2 * NP):
                top = None
                for i, o in enumerate(blocks):
                    s = dot(ks[o, h // 2], qm[h])
                    if start:
                        s = jnp.where(delta <= 0, s, NEG)
                    S[i, h * T:(h + 1) * T, :] = s
                    top = fold_max(s) if top is None else jnp.maximum(top, fold_max(s))
                tops.append(top)
            for h in range(2 * NP):
                m = jnp.max(tops[h], axis=0, keepdims=True)
                e = h % 2
                if not start:
                    old = s_max[h:h + 1, :]
                    m = jnp.maximum(m, old)
                part_sum = jnp.zeros((8, T), F32)
                num = jnp.zeros((64, T), F32)
                for i, o in enumerate(blocks):
                    p = jnp.exp2((S[i, h * T:(h + 1) * T, :] - m) * c_exp)
                    part_sum = part_sum + fold_sum(p)
                    num = num + dot(vs[o, h // 2, e * 64:(e + 1) * 64, :], p.astype(BF16))
                tot = jnp.sum(part_sum, axis=0, keepdims=True)
                if not start:
                    keep = jnp.exp2((old - m) * c_exp)
                    tot = tot + s_sum[h:h + 1, :] * keep
                    num = num + s_num[h] * keep
                s_max[h:h + 1, :] = m
                s_sum[h:h + 1, :] = tot
                s_num[h] = num

        for i in (WQ, WK, WV):
            cur[i].wait()
        partner_rows(z)
        q = dot(x_all[z], wq[...])
        for p in range(NP):
            qt = jnp.transpose(q[:, p * 128:(p + 1) * 128]).astype(BF16)
            for e in range(2):
                qm[2 * p + e] = one_head(qt, e)
        kv_blocks(x_all[z], wk, wv, ks, vs, z)
        attend(True, z)

        def memory_part(i):
            @pl.when(l == 0)
            def _():
                @pl.when(i == 0)
                def _():
                    cur[CK].wait()
                    cur[CV].wait()
                    mem_copy.wait()
                    mem_swap.wait()
            pl.when(jnp.logical_and(has_mem, i < KBC // 2))(lambda: memory_pair(i))

        def earlier(s, one, two):
            o, q = ring(s), ring(-s)
            pl.when(jnp.logical_and(o < z, q < z))(lambda: two(o, q))
            pl.when(jnp.logical_xor(o < z, q < z))(lambda: one(jnp.minimum(o, q)))

        def attend_level(s):
            earlier(s, lambda o: attend(False, o), lambda o, q: attend(False, o, q))

        def project_level(s):
            earlier(s, lambda o: kv_blocks(x_all[o], wk, wv, ks, vs, o),
                    lambda o, q: kv_blocks(jnp.concatenate([x_all[o], x_all[q]], axis=0), wk, wv, ks, vs, o, q))

        def level(s, _):
            def arrivals(h):
                for d in range(2):
                    x_event(d, s, h)

            arrivals(0)
            arrivals(1)

            @pl.when(s == 1)
            def _():
                memory_part(0)

            @pl.when(s >= 2)
            def _():
                attend_level(s - 1)
            arrivals(2)
            arrivals(3)
            for o in (ring(s), ring(-s)):
                partner_rows(o)
            project_level(s)
            memory_part(s)
            return 0

        lax.fori_loop(1, Z // 2, level, 0)
        far = ring(Z // 2)
        for h in range(4):
            x_event(h % 2, Z // 2, h)
            if h == 1:
                attend_level(Z // 2 - 1)
        partner_rows(far)

        @pl.when(far < z)
        def _():
            kv_blocks(x_all[far], wk, wv, ks, vs, far)
            attend(False, far)
        for h in range(2 * NP):
            a = (s_num[h] / s_sum[h:h + 1, :]).astype(BF16)
            for j in range(2):
                a_half[0, j, h * 64:(h + 1) * 64, :] = a[:, j * 128:(j + 1) * 128]
        swap_project(wo, cur[WO])

        for j in range(2):
            mine = jnp.concatenate([upd(j, n)[...].astype(BF16) for n in CT], axis=1)
            x = rms_norm(mine, gain(g_cross, l))
            if j == 0:
                cur[CQ].wait()
            q = dot(x, cq[...])
            for p in range(NP):
                q_all[z, p, :, j * rows:(j + 1) * rows] = jnp.transpose(q[:, p * 128:(p + 1) * 128]).astype(BF16)

        def q_own(p):
            for d in range(2):
                src = q_all.at[z, p]
                rcopy(src, src, qtx.at[d, 0], qrx.at[d, 1, p], nbr(d)).start()

        def arrival(i, _):
            s, d, p = decode(arrival_of(i))

            @pl.when(s == 0)
            def _():
                q_own(p)

            @pl.when(s >= 1)
            def _():
                src = q_all.at[ring(-(1 - 2 * d) * s), p]
                rcopy(src, src, qtx.at[d, s], qrx.at[d, s, p], nbr(d)).wait_recv()

                @pl.when(jnp.logical_or(s < 3, jnp.logical_and(s == 3, lax.rem(p, 2) == d)))
                def _():
                    rcopy(src, src, qtx.at[d, s], qrx.at[d, s + 1, p], nbr(d)).start()
            return 0

        one = ones_row(T)

        def head_rhs(o, p, e):
            return jnp.concatenate([one_head(q_all[o, p], e), one], axis=0)

        def keys_of(p):
            return lambda b: jnp.concatenate([kc[b, p], bias[b]], axis=1)

        def place(s, d, p):
            return p * 8 + jnp.where(s == 0, 0, jnp.where(s == 4, 7, 2 * s - 1 + d))

        def origin(s, d):
            return ring(jnp.where(d == 0, -s, s))

        def cross_groups(*groups):
            where = [(origin(s, d), p, place(s, d, p)) for s, d, p in groups]
            heads = [(w, e) for w in where[:-1] for e in range(2)] + [(where[-1], 0)]
            top = top_s[...]
            stats = []
            for ((o, p, to), e), ((on, pn, _), en) in zip(heads, heads[1:]):
                top, num, l, m = score_and_sum(
                    S, en, keys_of(pn), head_rhs(on, pn, en),
                    e, lambda b: vc[b, p, e * 64:(e + 1) * 64, :], top, KBC, c_exp)
                part[to, e * 64:(e + 1) * 64, :] = num
                stats.append((m, l))
                if e == 1:
                    part_ml[to] = jnp.concatenate(
                        [x[k][:, j * 128:(j + 1) * 128] for k in range(2) for j in range(2) for x in stats[-2:]], axis=0)
            top_s[...] = top

        def incoming(d, s, p):
            rcopy(o_send.at[d, s, p], o_recv.at[d, s, p], otx.at[d, s], orx.at[d, s, p], nbr(d)).wait_recv()

        def stats_in(d, s, p):
            x = o_recv[d, s, p, 128:136, :].astype(F32)
            return x[:, 0:128] + x[:, 128:256]

        def stats_out(d, s, p, x):
            o_send[d, s, p, 128:136, :] = jnp.concatenate(two_terms(x), axis=1)

        def scales(mls):
            m = functools.reduce(jnp.maximum, [x[0:4] for x in mls])
            w = [jnp.exp2((x[0:4] - m) * c_exp) for x in mls]
            return w, m, sum(x[4:8] * y for x, y in zip(mls, w))

        def tile(ref, e, j):
            return ref[e * 64:(e + 1) * 64, j * 128:(j + 1) * 128].astype(F32)

        def reduce_step(v):
            s, d_arr, p = decode(v)
            at = place(s, d_arr, p)
            d = jnp.where(s == 4, lax.rem(p, 2), 1 - d_arr)
            has_in = jnp.logical_and(s >= 1, jnp.logical_or(s < 3, jnp.logical_and(s == 3, lax.rem(p, 2) == d)))
            to = jnp.maximum(s - 1, 0)

            def send():
                rcopy(o_send.at[d, to, p], o_recv.at[d, to, p], otx.at[d, to], orx.at[d, to, p], nbr(d)).start()

            @pl.when(has_in)
            def _():
                incoming(d, s, p)
                (wa, wb), m, l = scales([part_ml[at], stats_in(d, s, p)])
                stats_out(d, to, p, jnp.concatenate([m, l], axis=0))
                for e in range(2):
                    for j in range(2):
                        r = slice(2 * j + e, 2 * j + e + 1)
                        o_send[d, to, p, e * 64:(e + 1) * 64, j * 128:(j + 1) * 128] = (
                            tile(part.at[at], e, j) * wa[r] + tile(o_recv.at[d, s, p], e, j) * wb[r]).astype(BF16)
                send()

            @pl.when(jnp.logical_and(s >= 1, jnp.logical_not(has_in)))
            def _():
                o_send[d, to, p, 0:128, :] = part[at].astype(BF16)
                stats_out(d, to, p, part_ml[at])
                send()

            @pl.when(s == 0)
            def _():
                for dd in range(2):
                    incoming(dd, 0, p)
                w, m, l = scales([part_ml[at], stats_in(0, 0, p), stats_in(1, 0, p)])
                to_rows = pl.multiple_of(p * 128, 128)
                for e in range(2):
                    for j in range(2):
                        r = slice(2 * j + e, 2 * j + e + 1)
                        tot = (tile(part.at[at], e, j) * w[0][r] + tile(o_recv.at[0, 0, p], e, j) * w[1][r]
                               + tile(o_recv.at[1, 0, p], e, j) * w[2][r])
                        a_half[1, j, pl.ds(to_rows + e * 64, 64), :] = (tot / l[r]).astype(BF16)

        q_own(0)
        q_own(1)
        @pl.when(has_mem)
        def _():
            top_s[...] = score_all(S, 0, keys_of(GROUPS[0] // 16), head_rhs(z, GROUPS[0] // 16, 0), KBC)

        for d in range(2):
            for s in range(4):
                src = x_all.at[z, pl.ds(my_rows, rows if s < 3 else rows // 2), :]
                rcopy(src, src, xtx.at[d, s], xrx.at[d, s, 0], nbr(d)).wait_send()
        for o in range(Z):
            src = x_all.at[o, pl.ds(my_rows, rows), :]
            rcopy(src, src, ptx.at[o], prx.at[o], partner).wait_send()
        for i in (WG, WU, WD, CO):
            cur[i].wait()
        prefetch(WK, WQ, WV)

        @pl.when(l == 0)
        def _():
            prefetch(CK, CV)

        def step(k, at):
            ia, ir = at
            n = count_of(k)
            ja, jr = ia + lax.rem(n, 8), ir + n // 8
            lax.fori_loop(ia, ja, arrival, 0)

            def ret(i, _):
                reduce_step(return_of(i))
                return 0

            lax.fori_loop(ir, jr, ret, 0)
            groups = [decode(group_of(2 * k + i)) for i in range(3)]
            pl.when(has_mem)(lambda: cross_groups(*groups))
            return ja, jr

        lax.fori_loop(0, len(COUNTS), step, (jnp.int32(0), jnp.int32(0)))

        @pl.when(more)
        def _():
            nxt[CK].wait()
            nxt[CV].wait()

        def finish(i, b):
            v = last_of(i)
            n = jnp.where(jnp.logical_and(more, has_mem), v // 64, 0)
            lax.fori_loop(b, jnp.minimum(b + n, KBC), memory_block, 0)
            reduce_step(lax.rem(v, 64))

            @pl.when(lax.rem(v, 8) == 0)
            def _():
                p = lax.rem(v // 16, 4)
                pair_swap(p).start()
                pair_project(a_half[1, c, pair_rows(p)], my_cols, p)
            return b + n

        for n in CT:
            upd(0, n)[...] = hid[:, cols(n)].astype(F32)

        lax.fori_loop(0, len(LAST), finish, jnp.int32(0))

        @pl.when(l + 2 < n_layers)
        def _():
            after = wcopies(jnp.minimum(l + 2, n_layers - 1))
            after[CK].start()
            after[CV].start()

        for v in LAST[-NP:]:
            p = v % 64 // 16
            pair_swap(p).wait_recv()
            pair_project(att_c[pair_rows(p)], other_cols, p)
        for n in CT:
            hid[:, cols(n)] = upd(0, n)[...].astype(BF16)

        xm = rms_norm(hid[...], gain(g_mlp, l))

        acts = []
        for f in range(NF):
            gt = dot(xm, wg[:, cols(f)])
            up = dot(xm, wu[:, cols(f)])
            acts.append((gt * lax.logistic(gt) * up).astype(BF16))
        full = jnp.concatenate(acts, axis=1)

        for n in CT:
            hid[:, cols(n)] = (hid[:, cols(n)].astype(F32) + dot(full, wd[:, cols(n)])).astype(BF16)
        return carry

    lax.fori_loop(0, n_layers, layer_body, 0)
    drain_ring()
    out[...] = hid[...]


def solution(mesh):
    n_dev = mesh.shape["sp"]

    def local_step(hidden, memory, mem_len, norm_self, norm_cross, norm_mlp, self_q, self_k, self_v, self_o,
                   cross_q, cross_k, cross_v, cross_o, mlp_gate, mlp_up, mlp_down):
        rows, D = hidden.shape
        mem_rows = memory.shape[0]
        L, heads, head_dim = self_o.shape[:3]
        FF = mlp_gate.shape[2]
        Dc = D // 2
        NP = Dc // 128
        Z = n_dev // 2
        KBC = 2 * mem_rows // T
        any_ = pl.BlockSpec(memory_space=pl.ANY)
        vmem = pl.BlockSpec(memory_space=pltpu.VMEM)
        smem = pl.BlockSpec(memory_space=pltpu.SMEM)
        dma = pltpu.SemaphoreType.DMA
        V = pltpu.VMEM
        scratch = [
            V((rows, D), BF16),
            V((Z, 2 * rows, D), BF16),
            V((2, mem_rows, D), BF16),
            V((Z, NP, T, 128), BF16),
            V((Z, NP, 128, T), BF16),
            V((KBC, NP, T, 128), BF16),
            V((KBC, NP, 128, T), BF16),
            V((KBC, T, 128), BF16),
            V((2 * NP, 128, T), BF16),
            V((Z, NP, 128, T), BF16),
            V((2, max(2 * NP, KBC) * T, T), F32),
            V((8, T), F32),
            V((D, Dc), BF16), V((D, Dc), BF16), V((D, Dc), BF16), V((D, D), BF16),
            V((D, Dc), BF16), V((D, Dc), BF16), V((D, Dc), BF16), V((D, D), BF16),
            V((D, FF), BF16), V((D, FF), BF16), V((FF, D), BF16),
            V((8 * NP, 128, T), F32),
            V((8 * NP, 8, 128), F32),
            V((2, 4, NP, 136, T), BF16),
            V((2, 4, NP, 136, T), BF16),
            V((2 * NP, 64, T), F32),
            V((8, T), F32), V((8, T), F32),
            V((2, 2, Dc, 128), BF16),
            V((2, Dc, 128), BF16), V((Dc, 128), BF16),
            V((rows, D), BF16),
            dma((2, 5)), dma((2, 5, 4)), dma((Z,)), dma((Z,)),
            dma((2, 5)), dma((2, 5, NP)),
            dma((2, 4)), dma((2, 4, NP)),
            dma((NP,)), dma((NP,)),
            dma((4,)), dma((4,)), dma((11,)), dma((2,)),
        ]
        call = pl.pallas_call(
            functools.partial(kernel, n_dev, head_dim, L),
            out_shape=jax.ShapeDtypeStruct((rows, D), BF16),
            in_specs=[smem, any_, any_, vmem, vmem, vmem] + [any_] * 11,
            out_specs=vmem,
            scratch_shapes=scratch,
            compiler_params=pltpu.CompilerParams(
                collective_id=0, has_side_effects=True, vmem_limit_bytes=67043328),
            name="decoder",
        )
        return call(mem_len, hidden, memory, norm_self, norm_cross, norm_mlp,
                    self_q, self_k, self_v, self_o.reshape(L, D, D), cross_q, cross_k, cross_v,
                    cross_o.reshape(L, D, D), mlp_gate, mlp_up, mlp_down)

    row_spec = P(("dp", "sp"), None)
    return jax.shard_map(local_step, mesh=mesh, in_specs=(row_spec, row_spec, P("dp")) + (P(),) * 14,
                         out_specs=row_spec, check_vma=False)
```

```python
import functools
import math

import jax
import jax.numpy as jnp
from jax import lax
from jax.experimental import pallas as pl
from jax.experimental.pallas import tpu as pltpu
from jax.sharding import PartitionSpec as P

MESH = pl.DeviceIdType.MESH
EPS = 1e-6
NEG = -1e30
T = 256
F32 = jnp.float32
BF16 = jnp.bfloat16

def unpack(bits, count, *words):
    per = 84 // bits
    return [(words[i // per] >> (i % per * bits)) % 2 ** bits for i in range(count)]


GROUPS = unpack(6, 32, 0xca882c79859049430020, 0xcd2ad3f0b91c8fb11a6fa, 0xa51ab2)
ARRIVALS = unpack(6, 30, 0xa6268ac42e61441649c20, 0x93c4dcab213b6e348b0fa, 0xceb)
RETURNS = unpack(6, 21, 0x4c1f3a2e471aee30846c3, 0x1266a2a2ceb)
COUNTS = unpack(6, 16, 0x61a61b2ca3020c3083081, 0x618)
LAST = unpack(9, 11, 0x50401c5223914a244232, 0x6020)


def table(values, bits):
    per = 30 // bits
    words = [sum(v << (bits * j) for j, v in enumerate(values[i:i + per])) for i in range(0, len(values), per)]

    def get(i):
        w = jnp.int32(words[0])
        for k, v in enumerate(words[1:], 1):
            w = jnp.where(i >= k * per, jnp.int32(v), w)
        return lax.rem(lax.shift_right_logical(w, lax.rem(i, per) * bits), 1 << bits)

    return get


def decode(v):
    return lax.rem(v, 8), lax.rem(v // 8, 2), lax.rem(v // 16, 4)


def dot(a, b):
    return jnp.dot(a, b, preferred_element_type=F32)


def fold_max(x):
    return jnp.max(x.reshape(x.shape[0] // 8, 8, x.shape[1]), axis=0)


def fold_sum(x):
    return jnp.sum(x.reshape(x.shape[0] // 8, 8, x.shape[1]), axis=0)


def one_head(qt, e):
    rest = jnp.zeros((64, qt.shape[1]), BF16)
    return jnp.concatenate([qt[0:64], rest] if e == 0 else [rest, qt[64:128]], axis=0)


def ones_row(cols):
    row = lax.broadcasted_iota(jnp.int32, (128, cols), 0)
    return jnp.where(row == 0, 1.0, 0.0).astype(BF16)


def scores(S, slot, keys, rhs, b):
    s = dot(keys(b), rhs)
    S[slot, b * T:(b + 1) * T, :] = s
    return fold_max(s)


def score_all(S, slot, keys, rhs, blocks):
    return functools.reduce(jnp.maximum, [scores(S, slot, keys, rhs, b) for b in range(blocks)])


def score_and_sum(S, slot, keys, rhs, slot_v, values, top, blocks, c):
    ahead = min(3, blocks)
    hi, lo = two_terms(jnp.max(top, axis=0, keepdims=True))
    m = hi.astype(F32) + lo.astype(F32)
    tops = [scores(S, slot, keys, rhs, b) for b in range(ahead)]
    part = jnp.zeros((8, T), F32)
    num = jnp.zeros((64, T), F32)
    for b in range(blocks):
        p = jnp.exp2((S[slot_v, b * T:(b + 1) * T, :] - m) * c)
        part = part + fold_sum(p)
        num = num + dot(values(b), p.astype(BF16))
        if b + ahead < blocks:
            tops.append(scores(S, slot, keys, rhs, b + ahead))
    return functools.reduce(jnp.maximum, tops), num, jnp.sum(part, axis=0, keepdims=True), m


def two_terms(x):
    hi = x.astype(BF16)
    return hi, (x - hi.astype(F32)).astype(BF16)


def rms_norm(h, g):
    h = h.astype(F32)
    inv = lax.rsqrt(jnp.mean(h * h, axis=-1, keepdims=True) + EPS)
    return (h * inv * g).astype(BF16)


def kernel(n_dev, head_dim, n_layers,
           mem_len, hid_in, mem_in, g_self, g_cross, g_mlp,
           self_q, self_k, self_v, self_o, cross_q, cross_k, cross_v, cross_o, mlp_g, mlp_u, mlp_d,
           out,
           hid, x_all, mem, ks, vs, kc, vc, bias, qm, q_all, S, top_s,
           wq, wk, wv, wo, cq, ck, cv, co, wg, wu, wd,
           part, part_ml, o_send, o_recv,
           s_num, s_max, s_sum, a_half, att, att_c, hid_p,
           xtx, xrx, ptx, prx, qtx, qrx, otx, orx, ctx, crx, dtx, drx, wsem, isem):
    Z = n_dev // 2
    rows, D = hid.shape
    piece = rows // 4
    NP = q_all.shape[1]
    KBC = kc.shape[0]
    NF = wg.shape[1] // T
    Dc = D // 2
    mem_rows = mem_in.shape[0]
    c_exp = math.log2(math.e) * head_dim ** -0.5
    assert KBC <= Z

    me = lax.axis_index("sp")
    z = me // 2
    c = me % 2
    partner = z * 2 + (1 - c)

    def ring(k):
        return lax.rem(z + k * (1 - 2 * c) + 2 * Z, Z)

    def nbr(d):
        return ring(1 - 2 * d) * 2 + c

    def rcopy(src, dst, ssem, rsem, dev):
        return pltpu.make_async_remote_copy(src_ref=src, dst_ref=dst, send_sem=ssem, recv_sem=rsem,
                                            device_id={"sp": dev}, device_id_type=MESH)

    has_mem = z * (2 * mem_rows) < n_dev * mem_rows * 3 // 4
    my_rows = pl.multiple_of(c * rows, rows)
    my_cols = pl.multiple_of(c * Dc, Dc)
    other_cols = pl.multiple_of((1 - c) * Dc, Dc)

    barrier = pltpu.get_barrier_semaphore()
    for dev in (nbr(0), nbr(1), partner):
        pl.semaphore_signal(barrier, inc=1, device_id={"sp": dev}, device_id_type=MESH)

    def wcopies(l):
        mine = pl.ds(my_cols, Dc)
        w = [
            (self_k.at[l, :, mine], wk), (self_q.at[l, :, mine], wq), (self_v.at[l, :, mine], wv),
            (cross_k.at[l, :, mine], ck), (cross_v.at[l, :, mine], cv),
            (self_o.at[l], wo), (cross_q.at[l, :, mine], cq), (cross_o.at[l], co),
            (mlp_g.at[l], wg), (mlp_u.at[l], wu), (mlp_d.at[l], wd),
        ]
        return [pltpu.make_async_copy(s, d, wsem.at[i]) for i, (s, d) in enumerate(w)]

    WK, WQ, WV, CK, CV, WO, CQ, CO, WG, WU, WD = range(11)

    hid_copy = pltpu.make_async_copy(hid_in, hid, isem.at[0])
    mem_copy = pltpu.make_async_copy(mem_in, mem.at[c], isem.at[1])
    mem_swap = rcopy(mem_in, mem.at[c], dtx.at[3], drx.at[3], partner)
    hid_copy.start()
    first = wcopies(0)
    for i in (WQ, WK, WV):
        first[i].start()
    mem_copy.start()
    for i in (CK, CV):
        first[i].start()

    hid_copy.wait()

    def gain(ref, l):
        g = jnp.zeros((1, D), F32)
        for i in range(n_layers):
            g = jnp.where(l == i, ref[i:i + 1, :].astype(F32), g)
        return g

    def kv_blocks(x, wk_ref, wv_ref, kdst, vdst, *at):
        v = dot(x, wv_ref[...])
        k = dot(x, wk_ref[...]).astype(BF16)
        for i, b in enumerate(at):
            r = slice(i * T, (i + 1) * T)
            for p in range(NP):
                vdst[b, p] = jnp.transpose(v[r, p * 128:(p + 1) * 128]).astype(BF16)
            for p in range(NP):
                kdst[b, p] = k[r, p * 128:(p + 1) * 128]

    def memory_block(b, _):
        per = mem_rows // T
        at = pl.ds(pl.multiple_of(lax.rem(b, per) * T, T), T)
        kv_blocks(mem[b // per, at, :], ck, cv, kc, vc, b)
        return 0

    def memory_pair(i):
        per = mem_rows // (2 * T)
        at = pl.ds(pl.multiple_of(lax.rem(i, per) * 2 * T, 2 * T), 2 * T)
        kv_blocks(mem[i // per, at, :], ck, cv, kc, vc, 2 * i, 2 * i + 1)

    def key_mask():
        length = mem_len[0]
        for b in range(KBC):
            key = z * (2 * mem_rows) + b * T + lax.broadcasted_iota(jnp.int32, (T, 128), 0)
            lane = lax.broadcasted_iota(jnp.int32, (T, 128), 1)
            bias[b] = jnp.where(jnp.logical_and(lane == 0, key >= length), NEG, 0.0).astype(BF16)

    def empty_parts():
        for i in range(part.shape[0]):
            part[i] = jnp.zeros(part.shape[1:], F32)
            row = lax.broadcasted_iota(jnp.int32, part_ml.shape[1:], 0)
            part_ml[i] = jnp.where(row < 4, NEG, 0.0)

    def rows_of(a):
        return jnp.transpose(a.astype(F32)).astype(BF16)

    CT = range(D // T)

    def cols(n):
        return slice(n * T, (n + 1) * T)

    def upd(j, n):
        return S.at[0, pl.ds(pl.multiple_of((j * len(CT) + n) * rows, rows), rows), :]

    def swap_project(w_ref, ready):
        swap = rcopy(a_half.at[0], att, dtx.at[0], drx.at[0], partner)
        swap.start()
        ready.wait()
        for j in range(2):
            own = rows_of(a_half[0, j])
            for n in CT:
                upd(j, n)[...] = dot(own, w_ref[pl.ds(my_cols, Dc), cols(n)])
        hid_swap().wait()
        swap.wait()
        for j in range(2):
            others = rows_of(att[j])
            for n in CT:
                own, other = upd(j, n)[...], dot(others, w_ref[pl.ds(other_cols, Dc), cols(n)])
                before = jnp.where(c == j, hid[:, cols(n)], hid_p[:, cols(n)]).astype(F32)
                upd(j, n)[...] = before + jnp.where(c == 0, own, other) + jnp.where(c == 0, other, own)
        for n in CT:
            hid[:, cols(n)] = upd(c, n)[...].astype(BF16)

    def hid_swap():
        return rcopy(hid, hid_p, dtx.at[2], drx.at[2], partner)

    def pair_rows(p):
        return pl.ds(pl.multiple_of(p * 128, 128), 128)

    def pair_swap(p):
        return rcopy(a_half.at[1, 1 - c, pair_rows(p)], att_c.at[pair_rows(p)], ctx.at[p], crx.at[p], partner)

    def pair_project(a, base, p):
        a = rows_of(a)
        for n in CT:
            upd(0, n)[...] += dot(a, co[pl.ds(pl.multiple_of(base + p * 128, 128), 128), cols(n)])

    group_of = table(GROUPS + GROUPS[-1:], 6)
    count_of = table(COUNTS, 6)
    arrival_of = table(ARRIVALS, 6)
    return_of = table(RETURNS, 6)
    last_of = table(LAST, 9)

    def drain_ring():
        for p in range(NP):
            pair_swap(p).wait_send()
        for d in range(2):
            for s in range(4):
                pairs = pl.ds(0, NP if s < 3 else NP // 2)
                src, part_out = q_all.at[z, pairs], o_send.at[d, s, pairs]
                rcopy(src, src, qtx.at[d, s], qrx.at[d, s, 0], nbr(d)).wait_send()
                rcopy(part_out, o_recv.at[d, s, pairs], otx.at[d, s], orx.at[d, s, 0], nbr(d)).wait_send()

    def layer_body(l, carry):
        more = l + 1 < n_layers
        cur = wcopies(l)
        nxt = wcopies(jnp.minimum(l + 1, n_layers - 1))

        def prefetch(*ids):
            @pl.when(more)
            def _():
                for i in ids:
                    nxt[i].start()

        x_all[z, pl.ds(my_rows, rows), :] = rms_norm(hid[...], gain(g_self, l))

        @pl.when(l == 0)
        def _():
            pl.semaphore_wait(barrier, 3)

        def xslot(o, h):
            return x_all.at[o, pl.ds(pl.multiple_of(c * rows + h * piece, piece), piece), :]

        for h in range(4):
            src = xslot(z, h)
            for d in range(2):
                rcopy(src, src, xtx.at[d, 0], xrx.at[d, 1, h], nbr(d)).start()
            rcopy(src, src, ptx.at[z], prx.at[z], partner).start()

        hid_swap().start()
        @pl.when(l == 0)
        def _():
            mem_swap.start()
            key_mask()
            pl.when(jnp.logical_not(has_mem))(empty_parts)

        pl.when(l > 0)(drain_ring)
        for i in (WO, CQ, CO, WG, WU, WD):
            cur[i].start()


        def x_event(d, s, h):
            o = ring(-(1 - 2 * d) * s)
            src = xslot(o, h)

            @pl.when(jnp.logical_or(s <= 3, h % 2 == d))
            def _():
                rcopy(src, src, xtx.at[d, s], xrx.at[d, s, h], nbr(d)).wait_recv()

                @pl.when(jnp.logical_or(s < 3, jnp.logical_and(s == 3, h % 2 == d)))
                def _():
                    rcopy(src, src, xtx.at[d, s], xrx.at[d, s + 1, h], nbr(d)).start()
                rcopy(src, src, ptx.at[o], prx.at[o], partner).start()

        def partner_rows(o):
            dst = x_all.at[o, pl.ds(pl.multiple_of((1 - c) * rows, rows), rows), :]
            rcopy(dst, dst, ptx.at[o], prx.at[o], partner).wait_recv()

        delta = (lax.broadcasted_iota(jnp.int32, (T, T), 0) - lax.broadcasted_iota(jnp.int32, (T, T), 1))

        def attend(start, *blocks):
            tops = []
            for h in range(2 * NP):
                top = None
                for i, o in enumerate(blocks):
                    s = dot(ks[o, h // 2], qm[h])
                    if start:
                        s = jnp.where(delta <= 0, s, NEG)
                    S[i, h * T:(h + 1) * T, :] = s
                    top = fold_max(s) if top is None else jnp.maximum(top, fold_max(s))
                tops.append(top)
            for h in range(2 * NP):
                m = jnp.max(tops[h], axis=0, keepdims=True)
                e = h % 2
                if not start:
                    old = s_max[h:h + 1, :]
                    m = jnp.maximum(m, old)
                part_sum = jnp.zeros((8, T), F32)
                num = jnp.zeros((64, T), F32)
                for i, o in enumerate(blocks):
                    p = jnp.exp2((S[i, h * T:(h + 1) * T, :] - m) * c_exp)
                    part_sum = part_sum + fold_sum(p)
                    num = num + dot(vs[o, h // 2, e * 64:(e + 1) * 64, :], p.astype(BF16))
                tot = jnp.sum(part_sum, axis=0, keepdims=True)
                if not start:
                    keep = jnp.exp2((old - m) * c_exp)
                    tot = tot + s_sum[h:h + 1, :] * keep
                    num = num + s_num[h] * keep
                s_max[h:h + 1, :] = m
                s_sum[h:h + 1, :] = tot
                s_num[h] = num

        for i in (WQ, WK, WV):
            cur[i].wait()
        partner_rows(z)
        q = dot(x_all[z], wq[...])
        for p in range(NP):
            qt = jnp.transpose(q[:, p * 128:(p + 1) * 128]).astype(BF16)
            for e in range(2):
                qm[2 * p + e] = one_head(qt, e)
        kv_blocks(x_all[z], wk, wv, ks, vs, z)
        attend(True, z)

        def memory_part(i):
            @pl.when(l == 0)
            def _():
                @pl.when(i == 0)
                def _():
                    cur[CK].wait()
                    cur[CV].wait()
                    mem_copy.wait()
                    mem_swap.wait()
            pl.when(jnp.logical_and(has_mem, i < KBC // 2))(lambda: memory_pair(i))

        def earlier(s, one, two):
            o, q = ring(s), ring(-s)
            pl.when(jnp.logical_and(o < z, q < z))(lambda: two(o, q))
            pl.when(jnp.logical_xor(o < z, q < z))(lambda: one(jnp.minimum(o, q)))

        def attend_level(s):
            earlier(s, lambda o: attend(False, o), lambda o, q: attend(False, o, q))

        def project_level(s):
            earlier(s, lambda o: kv_blocks(x_all[o], wk, wv, ks, vs, o),
                    lambda o, q: kv_blocks(jnp.concatenate([x_all[o], x_all[q]], axis=0), wk, wv, ks, vs, o, q))

        def level(s, _):
            def arrivals(h):
                for d in range(2):
                    x_event(d, s, h)

            arrivals(0)
            arrivals(1)

            @pl.when(s == 1)
            def _():
                memory_part(0)

            @pl.when(s >= 2)
            def _():
                attend_level(s - 1)
            arrivals(2)
            arrivals(3)
            for o in (ring(s), ring(-s)):
                partner_rows(o)
            project_level(s)
            memory_part(s)
            return 0

        lax.fori_loop(1, Z // 2, level, 0)
        far = ring(Z // 2)
        for h in range(4):
            x_event(h % 2, Z // 2, h)
            if h == 1:
                attend_level(Z // 2 - 1)
        partner_rows(far)

        @pl.when(far < z)
        def _():
            kv_blocks(x_all[far], wk, wv, ks, vs, far)
            attend(False, far)
        for h in range(2 * NP):
            a = (s_num[h] / s_sum[h:h + 1, :]).astype(BF16)
            for j in range(2):
                a_half[0, j, h * 64:(h + 1) * 64, :] = a[:, j * 128:(j + 1) * 128]
        swap_project(wo, cur[WO])

        for j in range(2):
            mine = jnp.concatenate([upd(j, n)[...].astype(BF16) for n in CT], axis=1)
            x = rms_norm(mine, gain(g_cross, l))
            if j == 0:
                cur[CQ].wait()
            q = dot(x, cq[...])
            for p in range(NP):
                q_all[z, p, :, j * rows:(j + 1) * rows] = jnp.transpose(q[:, p * 128:(p + 1) * 128]).astype(BF16)

        def q_own(p):
            for d in range(2):
                src = q_all.at[z, p]
                rcopy(src, src, qtx.at[d, 0], qrx.at[d, 1, p], nbr(d)).start()

        def arrival(i, _):
            s, d, p = decode(arrival_of(i))

            @pl.when(s == 0)
            def _():
                q_own(p)

            @pl.when(s >= 1)
            def _():
                src = q_all.at[ring(-(1 - 2 * d) * s), p]
                rcopy(src, src, qtx.at[d, s], qrx.at[d, s, p], nbr(d)).wait_recv()

                @pl.when(jnp.logical_or(s < 3, jnp.logical_and(s == 3, lax.rem(p, 2) == d)))
                def _():
                    rcopy(src, src, qtx.at[d, s], qrx.at[d, s + 1, p], nbr(d)).start()
            return 0

        one = ones_row(T)

        def head_rhs(o, p, e):
            return jnp.concatenate([one_head(q_all[o, p], e), one], axis=0)

        def keys_of(p):
            return lambda b: jnp.concatenate([kc[b, p], bias[b]], axis=1)

        def place(s, d, p):
            return p * 8 + jnp.where(s == 0, 0, jnp.where(s == 4, 7, 2 * s - 1 + d))

        def origin(s, d):
            return ring(jnp.where(d == 0, -s, s))

        def cross_groups(*groups):
            where = [(origin(s, d), p, place(s, d, p)) for s, d, p in groups]
            heads = [(w, e) for w in where[:-1] for e in range(2)] + [(where[-1], 0)]
            top = top_s[...]
            stats = []
            for ((o, p, to), e), ((on, pn, _), en) in zip(heads, heads[1:]):
                top, num, l, m = score_and_sum(
                    S, en, keys_of(pn), head_rhs(on, pn, en),
                    e, lambda b: vc[b, p, e * 64:(e + 1) * 64, :], top, KBC, c_exp)
                part[to, e * 64:(e + 1) * 64, :] = num
                stats.append((m, l))
                if e == 1:
                    part_ml[to] = jnp.concatenate(
                        [x[k][:, j * 128:(j + 1) * 128] for k in range(2) for j in range(2) for x in stats[-2:]], axis=0)
            top_s[...] = top

        def incoming(d, s, p):
            rcopy(o_send.at[d, s, p], o_recv.at[d, s, p], otx.at[d, s], orx.at[d, s, p], nbr(d)).wait_recv()

        def stats_in(d, s, p):
            x = o_recv[d, s, p, 128:136, :].astype(F32)
            return x[:, 0:128] + x[:, 128:256]

        def stats_out(d, s, p, x):
            o_send[d, s, p, 128:136, :] = jnp.concatenate(two_terms(x), axis=1)

        def scales(mls):
            m = functools.reduce(jnp.maximum, [x[0:4] for x in mls])
            w = [jnp.exp2((x[0:4] - m) * c_exp) for x in mls]
            return w, m, sum(x[4:8] * y for x, y in zip(mls, w))

        def tile(ref, e, j):
            return ref[e * 64:(e + 1) * 64, j * 128:(j + 1) * 128].astype(F32)

        def reduce_step(v):
            s, d_arr, p = decode(v)
            at = place(s, d_arr, p)
            d = jnp.where(s == 4, lax.rem(p, 2), 1 - d_arr)
            has_in = jnp.logical_and(s >= 1, jnp.logical_or(s < 3, jnp.logical_and(s == 3, lax.rem(p, 2) == d)))
            to = jnp.maximum(s - 1, 0)

            def send():
                rcopy(o_send.at[d, to, p], o_recv.at[d, to, p], otx.at[d, to], orx.at[d, to, p], nbr(d)).start()

            @pl.when(has_in)
            def _():
                incoming(d, s, p)
                (wa, wb), m, l = scales([part_ml[at], stats_in(d, s, p)])
                stats_out(d, to, p, jnp.concatenate([m, l], axis=0))
                for e in range(2):
                    for j in range(2):
                        r = slice(2 * j + e, 2 * j + e + 1)
                        o_send[d, to, p, e * 64:(e + 1) * 64, j * 128:(j + 1) * 128] = (
                            tile(part.at[at], e, j) * wa[r] + tile(o_recv.at[d, s, p], e, j) * wb[r]).astype(BF16)
                send()

            @pl.when(jnp.logical_and(s >= 1, jnp.logical_not(has_in)))
            def _():
                o_send[d, to, p, 0:128, :] = part[at].astype(BF16)
                stats_out(d, to, p, part_ml[at])
                send()

            @pl.when(s == 0)
            def _():
                for dd in range(2):
                    incoming(dd, 0, p)
                w, m, l = scales([part_ml[at], stats_in(0, 0, p), stats_in(1, 0, p)])
                to_rows = pl.multiple_of(p * 128, 128)
                for e in range(2):
                    for j in range(2):
                        r = slice(2 * j + e, 2 * j + e + 1)
                        tot = (tile(part.at[at], e, j) * w[0][r] + tile(o_recv.at[0, 0, p], e, j) * w[1][r]
                               + tile(o_recv.at[1, 0, p], e, j) * w[2][r])
                        a_half[1, j, pl.ds(to_rows + e * 64, 64), :] = (tot / l[r]).astype(BF16)

        q_own(0)
        q_own(1)
        @pl.when(has_mem)
        def _():
            top_s[...] = score_all(S, 0, keys_of(GROUPS[0] // 16), head_rhs(z, GROUPS[0] // 16, 0), KBC)

        for d in range(2):
            for s in range(4):
                src = x_all.at[z, pl.ds(my_rows, rows if s < 3 else rows // 2), :]
                rcopy(src, src, xtx.at[d, s], xrx.at[d, s, 0], nbr(d)).wait_send()
        for o in range(Z):
            src = x_all.at[o, pl.ds(my_rows, rows), :]
            rcopy(src, src, ptx.at[o], prx.at[o], partner).wait_send()
        for i in (WG, WU, WD, CO):
            cur[i].wait()
        prefetch(WK, WQ, WV)

        @pl.when(l == 0)
        def _():
            prefetch(CK, CV)

        def step(k, at):
            ia, ir = at
            n = count_of(k)
            ja, jr = ia + lax.rem(n, 8), ir + n // 8
            lax.fori_loop(ia, ja, arrival, 0)

            def ret(i, _):
                reduce_step(return_of(i))
                return 0

            lax.fori_loop(ir, jr, ret, 0)
            groups = [decode(group_of(2 * k + i)) for i in range(3)]
            pl.when(has_mem)(lambda: cross_groups(*groups))
            return ja, jr

        lax.fori_loop(0, len(COUNTS), step, (jnp.int32(0), jnp.int32(0)))

        @pl.when(more)
        def _():
            nxt[CK].wait()
            nxt[CV].wait()

        def finish(i, b):
            v = last_of(i)
            n = jnp.where(jnp.logical_and(more, has_mem), v // 64, 0)
            lax.fori_loop(b, jnp.minimum(b + n, KBC), memory_block, 0)
            reduce_step(lax.rem(v, 64))

            @pl.when(lax.rem(v, 8) == 0)
            def _():
                p = lax.rem(v // 16, 4)
                pair_swap(p).start()
                pair_project(a_half[1, c, pair_rows(p)], my_cols, p)
            return b + n

        for n in CT:
            upd(0, n)[...] = hid[:, cols(n)].astype(F32)

        lax.fori_loop(0, len(LAST), finish, jnp.int32(0))

        @pl.when(l + 2 < n_layers)
        def _():
            after = wcopies(jnp.minimum(l + 2, n_layers - 1))
            after[CK].start()
            after[CV].start()

        for v in LAST[-NP:]:
            p = v % 64 // 16
            pair_swap(p).wait_recv()
            pair_project(att_c[pair_rows(p)], other_cols, p)
        for n in CT:
            hid[:, cols(n)] = upd(0, n)[...].astype(BF16)

        xm = rms_norm(hid[...], gain(g_mlp, l))

        acts = []
        for f in range(NF):
            gt = dot(xm, wg[:, cols(f)])
            up = dot(xm, wu[:, cols(f)])
            acts.append((gt * lax.logistic(gt) * up).astype(BF16))
        full = jnp.concatenate(acts, axis=1)

        for n in CT:
            hid[:, cols(n)] = (hid[:, cols(n)].astype(F32) + dot(full, wd[:, cols(n)])).astype(BF16)
        return carry

    lax.fori_loop(0, n_layers, layer_body, 0)
    drain_ring()
    out[...] = hid[...]


def solution(mesh):
    n_dev = mesh.shape["sp"]

    def local_step(hidden, memory, mem_len, norm_self, norm_cross, norm_mlp, self_q, self_k, self_v, self_o,
                   cross_q, cross_k, cross_v, cross_o, mlp_gate, mlp_up, mlp_down):
        rows, D = hidden.shape
        mem_rows = memory.shape[0]
        L, heads, head_dim = self_o.shape[:3]
        FF = mlp_gate.shape[2]
        Dc = D // 2
        NP = Dc // 128
        Z = n_dev // 2
        KBC = 2 * mem_rows // T
        any_ = pl.BlockSpec(memory_space=pl.ANY)
        vmem = pl.BlockSpec(memory_space=pltpu.VMEM)
        smem = pl.BlockSpec(memory_space=pltpu.SMEM)
        dma = pltpu.SemaphoreType.DMA
        V = pltpu.VMEM
        scratch = [
            V((rows, D), BF16),
            V((Z, 2 * rows, D), BF16),
            V((2, mem_rows, D), BF16),
            V((Z, NP, T, 128), BF16),
            V((Z, NP, 128, T), BF16),
            V((KBC, NP, T, 128), BF16),
            V((KBC, NP, 128, T), BF16),
            V((KBC, T, 128), BF16),
            V((2 * NP, 128, T), BF16),
            V((Z, NP, 128, T), BF16),
            V((2, max(2 * NP, KBC) * T, T), F32),
            V((8, T), F32),
            V((D, Dc), BF16), V((D, Dc), BF16), V((D, Dc), BF16), V((D, D), BF16),
            V((D, Dc), BF16), V((D, Dc), BF16), V((D, Dc), BF16), V((D, D), BF16),
            V((D, FF), BF16), V((D, FF), BF16), V((FF, D), BF16),
            V((8 * NP, 128, T), F32),
            V((8 * NP, 8, 128), F32),
            V((2, 4, NP, 136, T), BF16),
            V((2, 4, NP, 136, T), BF16),
            V((2 * NP, 64, T), F32),
            V((8, T), F32), V((8, T), F32),
            V((2, 2, Dc, 128), BF16),
            V((2, Dc, 128), BF16), V((Dc, 128), BF16),
            V((rows, D), BF16),
            dma((2, 5)), dma((2, 5, 4)), dma((Z,)), dma((Z,)),
            dma((2, 5)), dma((2, 5, NP)),
            dma((2, 4)), dma((2, 4, NP)),
            dma((NP,)), dma((NP,)),
            dma((4,)), dma((4,)), dma((11,)), dma((2,)),
        ]
        call = pl.pallas_call(
            functools.partial(kernel, n_dev, head_dim, L),
            out_shape=jax.ShapeDtypeStruct((rows, D), BF16),
            in_specs=[smem, any_, any_, vmem, vmem, vmem] + [any_] * 11,
            out_specs=vmem,
            scratch_shapes=scratch,
            compiler_params=pltpu.CompilerParams(
                collective_id=0, has_side_effects=True, vmem_limit_bytes=67043328),
            name="decoder",
        )
        return call(mem_len, hidden, memory, norm_self, norm_cross, norm_mlp,
                    self_q, self_k, self_v, self_o.reshape(L, D, D), cross_q, cross_k, cross_v,
                    cross_o.reshape(L, D, D), mlp_gate, mlp_up, mlp_down)

    row_spec = P(("dp", "sp"), None)
    return jax.shard_map(local_step, mesh=mesh, in_specs=(row_spec, row_spec, P("dp")) + (P(),) * 14,
                         out_specs=row_spec, check_vma=False)
```

```python
import functools
import math

import jax
import jax.numpy as jnp
from jax import lax
from jax.experimental import pallas as pl
from jax.experimental.pallas import tpu as pltpu
from jax.sharding import PartitionSpec as P

MESH = pl.DeviceIdType.MESH
EPS = 1e-6
NEG = -1e30
T = 256
F32 = jnp.float32
BF16 = jnp.bfloat16

def unpack(bits, count, *words):
    per = 84 // bits
    return [(words[i // per] >> (i % per * bits)) % 2 ** bits for i in range(count)]


GROUPS = unpack(6, 32, 0xca882c79859049430020, 0xcd2ad3f0b91c8fb11a6fa, 0xa51ab2)
ARRIVALS = unpack(6, 30, 0xa6268ac42e61441649c20, 0x93c4dcab213b6e348b0fa, 0xceb)
RETURNS = unpack(6, 21, 0x4c1f3a2e471aee30846c3, 0x1266a2a2ceb)
COUNTS = unpack(6, 16, 0x61a61b2ca3020c3083081, 0x618)
LAST = unpack(9, 11, 0x50401c5223914a244232, 0x6020)


def table(values, bits):
    per = 30 // bits
    words = [sum(v << (bits * j) for j, v in enumerate(values[i:i + per])) for i in range(0, len(values), per)]

    def get(i):
        w = jnp.int32(words[0])
        for k, v in enumerate(words[1:], 1):
            w = jnp.where(i >= k * per, jnp.int32(v), w)
        return lax.rem(lax.shift_right_logical(w, lax.rem(i, per) * bits), 1 << bits)

    return get


def decode(v):
    return lax.rem(v, 8), lax.rem(v // 8, 2), lax.rem(v // 16, 4)


def dot(a, b):
    return jnp.dot(a, b, preferred_element_type=F32)


def fold_max(x):
    return jnp.max(x.reshape(x.shape[0] // 8, 8, x.shape[1]), axis=0)


def fold_sum(x):
    return jnp.sum(x.reshape(x.shape[0] // 8, 8, x.shape[1]), axis=0)


def one_head(qt, e):
    rest = jnp.zeros((64, qt.shape[1]), BF16)
    return jnp.concatenate([qt[0:64], rest] if e == 0 else [rest, qt[64:128]], axis=0)


def ones_row(cols):
    row = lax.broadcasted_iota(jnp.int32, (128, cols), 0)
    return jnp.where(row == 0, 1.0, 0.0).astype(BF16)


def scores(S, slot, keys, rhs, b):
    s = dot(keys(b), rhs)
    S[slot, b * T:(b + 1) * T, :] = s
    return fold_max(s)


def score_all(S, slot, keys, rhs, blocks):
    return functools.reduce(jnp.maximum, [scores(S, slot, keys, rhs, b) for b in range(blocks)])


def score_and_sum(S, slot, keys, rhs, slot_v, values, top, blocks, c):
    ahead = min(3, blocks)
    hi, lo = two_terms(jnp.max(top, axis=0, keepdims=True))
    m = hi.astype(F32) + lo.astype(F32)
    tops = [scores(S, slot, keys, rhs, b) for b in range(ahead)]
    part = jnp.zeros((8, T), F32)
    num = jnp.zeros((64, T), F32)
    for b in range(blocks):
        p = jnp.exp2((S[slot_v, b * T:(b + 1) * T, :] - m) * c)
        part = part + fold_sum(p)
        num = num + dot(values(b), p.astype(BF16))
        if b + ahead < blocks:
            tops.append(scores(S, slot, keys, rhs, b + ahead))
    return functools.reduce(jnp.maximum, tops), num, jnp.sum(part, axis=0, keepdims=True), m


def two_terms(x):
    hi = x.astype(BF16)
    return hi, (x - hi.astype(F32)).astype(BF16)


def rms_norm(h, g):
    h = h.astype(F32)
    inv = lax.rsqrt(jnp.mean(h * h, axis=-1, keepdims=True) + EPS)
    return (h * inv * g).astype(BF16)


def kernel(n_dev, head_dim, n_layers,
           mem_len, hid_in, mem_in, g_self, g_cross, g_mlp,
           self_q, self_k, self_v, self_o, cross_q, cross_k, cross_v, cross_o, mlp_g, mlp_u, mlp_d,
           out,
           hid, x_all, mem, ks, vs, kc, vc, bias, qm, q_all, S, top_s,
           wq, wk, wv, wo, cq, ck, cv, co, wg, wu, wd,
           part, part_ml, o_send, o_recv,
           s_num, s_max, s_sum, a_half, att, att_c, hid_p,
           xtx, xrx, ptx, prx, qtx, qrx, otx, orx, ctx, crx, dtx, drx, wsem, isem):
    Z = n_dev // 2
    rows, D = hid.shape
    piece = rows // 4
    NP = q_all.shape[1]
    KBC = kc.shape[0]
    NF = wg.shape[1] // T
    Dc = D // 2
    mem_rows = mem_in.shape[0]
    c_exp = math.log2(math.e) * head_dim ** -0.5
    assert KBC <= Z

    me = lax.axis_index("sp")
    z = me // 2
    c = me % 2
    partner = z * 2 + (1 - c)

    def ring(k):
        return lax.rem(z + k * (1 - 2 * c) + 2 * Z, Z)

    def nbr(d):
        return ring(1 - 2 * d) * 2 + c

    def rcopy(src, dst, ssem, rsem, dev):
        return pltpu.make_async_remote_copy(src_ref=src, dst_ref=dst, send_sem=ssem, recv_sem=rsem,
                                            device_id={"sp": dev}, device_id_type=MESH)

    has_mem = z * (2 * mem_rows) < n_dev * mem_rows * 3 // 4
    my_rows = pl.multiple_of(c * rows, rows)
    my_cols = pl.multiple_of(c * Dc, Dc)
    other_cols = pl.multiple_of((1 - c) * Dc, Dc)

    barrier = pltpu.get_barrier_semaphore()
    for dev in (nbr(0), nbr(1), partner):
        pl.semaphore_signal(barrier, inc=1, device_id={"sp": dev}, device_id_type=MESH)

    def wcopies(l):
        mine = pl.ds(my_cols, Dc)
        w = [
            (self_k.at[l, :, mine], wk), (self_q.at[l, :, mine], wq), (self_v.at[l, :, mine], wv),
            (cross_k.at[l, :, mine], ck), (cross_v.at[l, :, mine], cv),
            (self_o.at[l], wo), (cross_q.at[l, :, mine], cq), (cross_o.at[l], co),
            (mlp_g.at[l], wg), (mlp_u.at[l], wu), (mlp_d.at[l], wd),
        ]
        return [pltpu.make_async_copy(s, d, wsem.at[i]) for i, (s, d) in enumerate(w)]

    WK, WQ, WV, CK, CV, WO, CQ, CO, WG, WU, WD = range(11)

    hid_copy = pltpu.make_async_copy(hid_in, hid, isem.at[0])
    mem_copy = pltpu.make_async_copy(mem_in, mem.at[c], isem.at[1])
    mem_swap = rcopy(mem_in, mem.at[c], dtx.at[3], drx.at[3], partner)
    hid_copy.start()
    first = wcopies(0)
    for i in (WQ, WK, WV):
        first[i].start()
    mem_copy.start()
    for i in (CK, CV):
        first[i].start()

    hid_copy.wait()

    def gain(ref, l):
        g = jnp.zeros((1, D), F32)
        for i in range(n_layers):
            g = jnp.where(l == i, ref[i:i + 1, :].astype(F32), g)
        return g

    def kv_blocks(x, wk_ref, wv_ref, kdst, vdst, *at):
        v = dot(x, wv_ref[...])
        k = dot(x, wk_ref[...]).astype(BF16)
        for i, b in enumerate(at):
            r = slice(i * T, (i + 1) * T)
            for p in range(NP):
                vdst[b, p] = jnp.transpose(v[r, p * 128:(p + 1) * 128]).astype(BF16)
            for p in range(NP):
                kdst[b, p] = k[r, p * 128:(p + 1) * 128]

    def memory_block(b, _):
        per = mem_rows // T
        at = pl.ds(pl.multiple_of(lax.rem(b, per) * T, T), T)
        kv_blocks(mem[b // per, at, :], ck, cv, kc, vc, b)
        return 0

    def memory_pair(i):
        per = mem_rows // (2 * T)
        at = pl.ds(pl.multiple_of(lax.rem(i, per) * 2 * T, 2 * T), 2 * T)
        kv_blocks(mem[i // per, at, :], ck, cv, kc, vc, 2 * i, 2 * i + 1)

    def key_mask():
        length = mem_len[0]
        for b in range(KBC):
            key = z * (2 * mem_rows) + b * T + lax.broadcasted_iota(jnp.int32, (T, 128), 0)
            lane = lax.broadcasted_iota(jnp.int32, (T, 128), 1)
            bias[b] = jnp.where(jnp.logical_and(lane == 0, key >= length), NEG, 0.0).astype(BF16)

    def empty_parts():
        for i in range(part.shape[0]):
            part[i] = jnp.zeros(part.shape[1:], F32)
            row = lax.broadcasted_iota(jnp.int32, part_ml.shape[1:], 0)
            part_ml[i] = jnp.where(row < 4, NEG, 0.0)

    def rows_of(a):
        return jnp.transpose(a.astype(F32)).astype(BF16)

    CT = range(D // T)

    def cols(n):
        return slice(n * T, (n + 1) * T)

    def upd(j, n):
        return S.at[0, pl.ds(pl.multiple_of((j * len(CT) + n) * rows, rows), rows), :]

    def swap_project(w_ref, ready):
        swap = rcopy(a_half.at[0], att, dtx.at[0], drx.at[0], partner)
        swap.start()
        ready.wait()
        for j in range(2):
            own = rows_of(a_half[0, j])
            for n in CT:
                upd(j, n)[...] = dot(own, w_ref[pl.ds(my_cols, Dc), cols(n)])
        hid_swap().wait()
        swap.wait()
        for j in range(2):
            others = rows_of(att[j])
            for n in CT:
                own, other = upd(j, n)[...], dot(others, w_ref[pl.ds(other_cols, Dc), cols(n)])
                before = jnp.where(c == j, hid[:, cols(n)], hid_p[:, cols(n)]).astype(F32)
                upd(j, n)[...] = before + jnp.where(c == 0, own, other) + jnp.where(c == 0, other, own)
        for n in CT:
            hid[:, cols(n)] = upd(c, n)[...].astype(BF16)

    def hid_swap():
        return rcopy(hid, hid_p, dtx.at[2], drx.at[2], partner)

    def pair_rows(p):
        return pl.ds(pl.multiple_of(p * 128, 128), 128)

    def pair_swap(p):
        return rcopy(a_half.at[1, 1 - c, pair_rows(p)], att_c.at[pair_rows(p)], ctx.at[p], crx.at[p], partner)

    def pair_project(a, base, p):
        a = rows_of(a)
        for n in CT:
            upd(0, n)[...] += dot(a, co[pl.ds(pl.multiple_of(base + p * 128, 128), 128), cols(n)])

    group_of = table(GROUPS + GROUPS[-1:], 6)
    count_of = table(COUNTS, 6)
    arrival_of = table(ARRIVALS, 6)
    return_of = table(RETURNS, 6)
    last_of = table(LAST, 9)

    def drain_ring():
        for p in range(NP):
            pair_swap(p).wait_send()
        for d in range(2):
            for s in range(4):
                pairs = pl.ds(0, NP if s < 3 else NP // 2)
                src, part_out = q_all.at[z, pairs], o_send.at[d, s, pairs]
                rcopy(src, src, qtx.at[d, s], qrx.at[d, s, 0], nbr(d)).wait_send()
                rcopy(part_out, o_recv.at[d, s, pairs], otx.at[d, s], orx.at[d, s, 0], nbr(d)).wait_send()

    def layer_body(l, carry):
        more = l + 1 < n_layers
        cur = wcopies(l)
        nxt = wcopies(jnp.minimum(l + 1, n_layers - 1))

        def prefetch(*ids):
            @pl.when(more)
            def _():
                for i in ids:
                    nxt[i].start()

        x_all[z, pl.ds(my_rows, rows), :] = rms_norm(hid[...], gain(g_self, l))

        @pl.when(l == 0)
        def _():
            pl.semaphore_wait(barrier, 3)

        def xslot(o, h):
            return x_all.at[o, pl.ds(pl.multiple_of(c * rows + h * piece, piece), piece), :]

        for h in range(4):
            src = xslot(z, h)
            for d in range(2):
                rcopy(src, src, xtx.at[d, 0], xrx.at[d, 1, h], nbr(d)).start()
            rcopy(src, src, ptx.at[z], prx.at[z], partner).start()

        hid_swap().start()
        @pl.when(l == 0)
        def _():
            mem_swap.start()
            key_mask()
            pl.when(jnp.logical_not(has_mem))(empty_parts)

        pl.when(l > 0)(drain_ring)
        for i in (WO, CQ, CO, WG, WU, WD):
            cur[i].start()


        def x_event(d, s, h):
            o = ring(-(1 - 2 * d) * s)
            src = xslot(o, h)

            @pl.when(jnp.logical_or(s <= 3, h % 2 == d))
            def _():
                rcopy(src, src, xtx.at[d, s], xrx.at[d, s, h], nbr(d)).wait_recv()

                @pl.when(jnp.logical_or(s < 3, jnp.logical_and(s == 3, h % 2 == d)))
                def _():
                    rcopy(src, src, xtx.at[d, s], xrx.at[d, s + 1, h], nbr(d)).start()

                @pl.when(jnp.logical_or(s == Z // 2, h % 2 == 1))
                def _():
                    first = jnp.where(s == Z // 2, h, h - 1) * piece
                    both = x_all.at[o, pl.ds(pl.multiple_of(c * rows + first, piece), 2 * piece), :]

                    @pl.when(s < Z // 2)
                    def _():
                        rcopy(both, both, ptx.at[o], prx.at[o], partner).start()

                    @pl.when(s == Z // 2)
                    def _():
                        rcopy(src, src, ptx.at[o], prx.at[o], partner).start()

        def partner_rows(o):
            dst = x_all.at[o, pl.ds(pl.multiple_of((1 - c) * rows, rows), rows), :]
            rcopy(dst, dst, ptx.at[o], prx.at[o], partner).wait_recv()

        delta = (lax.broadcasted_iota(jnp.int32, (T, T), 0) - lax.broadcasted_iota(jnp.int32, (T, T), 1))

        def attend(start, *blocks):
            tops = []
            for h in range(2 * NP):
                top = None
                for i, o in enumerate(blocks):
                    s = dot(ks[o, h // 2], qm[h])
                    if start:
                        s = jnp.where(delta <= 0, s, NEG)
                    S[i, h * T:(h + 1) * T, :] = s
                    top = fold_max(s) if top is None else jnp.maximum(top, fold_max(s))
                tops.append(top)
            for h in range(2 * NP):
                m = jnp.max(tops[h], axis=0, keepdims=True)
                e = h % 2
                if not start:
                    old = s_max[h:h + 1, :]
                    m = jnp.maximum(m, old)
                part_sum = jnp.zeros((8, T), F32)
                num = jnp.zeros((64, T), F32)
                for i, o in enumerate(blocks):
                    p = jnp.exp2((S[i, h * T:(h + 1) * T, :] - m) * c_exp)
                    part_sum = part_sum + fold_sum(p)
                    num = num + dot(vs[o, h // 2, e * 64:(e + 1) * 64, :], p.astype(BF16))
                tot = jnp.sum(part_sum, axis=0, keepdims=True)
                if not start:
                    keep = jnp.exp2((old - m) * c_exp)
                    tot = tot + s_sum[h:h + 1, :] * keep
                    num = num + s_num[h] * keep
                s_max[h:h + 1, :] = m
                s_sum[h:h + 1, :] = tot
                s_num[h] = num

        for i in (WQ, WK, WV):
            cur[i].wait()
        partner_rows(z)
        q = dot(x_all[z], wq[...])
        for p in range(NP):
            qt = jnp.transpose(q[:, p * 128:(p + 1) * 128]).astype(BF16)
            for e in range(2):
                qm[2 * p + e] = one_head(qt, e)
        kv_blocks(x_all[z], wk, wv, ks, vs, z)
        attend(True, z)

        def memory_part(i):
            @pl.when(l == 0)
            def _():
                @pl.when(i == 0)
                def _():
                    cur[CK].wait()
                    cur[CV].wait()
                    mem_copy.wait()
                    mem_swap.wait()
            pl.when(jnp.logical_and(has_mem, i < KBC // 2))(lambda: memory_pair(i))

        def earlier(s, one, two):
            o, q = ring(s), ring(-s)
            pl.when(jnp.logical_and(o < z, q < z))(lambda: two(o, q))
            pl.when(jnp.logical_xor(o < z, q < z))(lambda: one(jnp.minimum(o, q)))

        def attend_level(s):
            earlier(s, lambda o: attend(False, o), lambda o, q: attend(False, o, q))

        def project_level(s):
            earlier(s, lambda o: kv_blocks(x_all[o], wk, wv, ks, vs, o),
                    lambda o, q: kv_blocks(jnp.concatenate([x_all[o], x_all[q]], axis=0), wk, wv, ks, vs, o, q))

        def level(s, _):
            def arrivals(h):
                for d in range(2):
                    x_event(d, s, h)

            arrivals(0)
            arrivals(1)

            @pl.when(s == 1)
            def _():
                memory_part(0)

            @pl.when(s >= 2)
            def _():
                attend_level(s - 1)
            arrivals(2)
            arrivals(3)
            for o in (ring(s), ring(-s)):
                partner_rows(o)
            project_level(s)
            memory_part(s)
            return 0

        lax.fori_loop(1, Z // 2, level, 0)
        far = ring(Z // 2)
        for h in range(4):
            x_event(h % 2, Z // 2, h)
            if h == 1:
                attend_level(Z // 2 - 1)
        partner_rows(far)

        @pl.when(far < z)
        def _():
            kv_blocks(x_all[far], wk, wv, ks, vs, far)
            attend(False, far)
        for h in range(2 * NP):
            a = (s_num[h] / s_sum[h:h + 1, :]).astype(BF16)
            for j in range(2):
                a_half[0, j, h * 64:(h + 1) * 64, :] = a[:, j * 128:(j + 1) * 128]
        swap_project(wo, cur[WO])

        for j in range(2):
            mine = jnp.concatenate([upd(j, n)[...].astype(BF16) for n in CT], axis=1)
            x = rms_norm(mine, gain(g_cross, l))
            if j == 0:
                cur[CQ].wait()
            q = dot(x, cq[...])
            for p in range(NP):
                q_all[z, p, :, j * rows:(j + 1) * rows] = jnp.transpose(q[:, p * 128:(p + 1) * 128]).astype(BF16)

        def q_own(p):
            for d in range(2):
                src = q_all.at[z, p]
                rcopy(src, src, qtx.at[d, 0], qrx.at[d, 1, p], nbr(d)).start()

        def arrival(i, _):
            s, d, p = decode(arrival_of(i))

            @pl.when(s == 0)
            def _():
                q_own(p)

            @pl.when(s >= 1)
            def _():
                src = q_all.at[ring(-(1 - 2 * d) * s), p]
                rcopy(src, src, qtx.at[d, s], qrx.at[d, s, p], nbr(d)).wait_recv()

                @pl.when(jnp.logical_or(s < 3, jnp.logical_and(s == 3, lax.rem(p, 2) == d)))
                def _():
                    rcopy(src, src, qtx.at[d, s], qrx.at[d, s + 1, p], nbr(d)).start()
            return 0

        one = ones_row(T)

        def head_rhs(o, p, e):
            return jnp.concatenate([one_head(q_all[o, p], e), one], axis=0)

        def keys_of(p):
            return lambda b: jnp.concatenate([kc[b, p], bias[b]], axis=1)

        def place(s, d, p):
            return p * 8 + jnp.where(s == 0, 0, jnp.where(s == 4, 7, 2 * s - 1 + d))

        def origin(s, d):
            return ring(jnp.where(d == 0, -s, s))

        def cross_groups(*groups):
            where = [(origin(s, d), p, place(s, d, p)) for s, d, p in groups]
            heads = [(w, e) for w in where[:-1] for e in range(2)] + [(where[-1], 0)]
            top = top_s[...]
            stats = []
            for ((o, p, to), e), ((on, pn, _), en) in zip(heads, heads[1:]):
                top, num, l, m = score_and_sum(
                    S, en, keys_of(pn), head_rhs(on, pn, en),
                    e, lambda b: vc[b, p, e * 64:(e + 1) * 64, :], top, KBC, c_exp)
                part[to, e * 64:(e + 1) * 64, :] = num
                stats.append((m, l))
                if e == 1:
                    part_ml[to] = jnp.concatenate(
                        [x[k][:, j * 128:(j + 1) * 128] for k in range(2) for j in range(2) for x in stats[-2:]], axis=0)
            top_s[...] = top

        def incoming(d, s, p):
            rcopy(o_send.at[d, s, p], o_recv.at[d, s, p], otx.at[d, s], orx.at[d, s, p], nbr(d)).wait_recv()

        def stats_in(d, s, p):
            x = o_recv[d, s, p, 128:136, :].astype(F32)
            return x[:, 0:128] + x[:, 128:256]

        def stats_out(d, s, p, x):
            o_send[d, s, p, 128:136, :] = jnp.concatenate(two_terms(x), axis=1)

        def scales(mls):
            m = functools.reduce(jnp.maximum, [x[0:4] for x in mls])
            w = [jnp.exp2((x[0:4] - m) * c_exp) for x in mls]
            return w, m, sum(x[4:8] * y for x, y in zip(mls, w))

        def tile(ref, e, j):
            return ref[e * 64:(e + 1) * 64, j * 128:(j + 1) * 128].astype(F32)

        def reduce_step(v):
            s, d_arr, p = decode(v)
            at = place(s, d_arr, p)
            d = jnp.where(s == 4, lax.rem(p, 2), 1 - d_arr)
            has_in = jnp.logical_and(s >= 1, jnp.logical_or(s < 3, jnp.logical_and(s == 3, lax.rem(p, 2) == d)))
            to = jnp.maximum(s - 1, 0)

            def send():
                rcopy(o_send.at[d, to, p], o_recv.at[d, to, p], otx.at[d, to], orx.at[d, to, p], nbr(d)).start()

            @pl.when(has_in)
            def _():
                incoming(d, s, p)
                (wa, wb), m, l = scales([part_ml[at], stats_in(d, s, p)])
                stats_out(d, to, p, jnp.concatenate([m, l], axis=0))
                for e in range(2):
                    for j in range(2):
                        r = slice(2 * j + e, 2 * j + e + 1)
                        o_send[d, to, p, e * 64:(e + 1) * 64, j * 128:(j + 1) * 128] = (
                            tile(part.at[at], e, j) * wa[r] + tile(o_recv.at[d, s, p], e, j) * wb[r]).astype(BF16)
                send()

            @pl.when(jnp.logical_and(s >= 1, jnp.logical_not(has_in)))
            def _():
                o_send[d, to, p, 0:128, :] = part[at].astype(BF16)
                stats_out(d, to, p, part_ml[at])
                send()

            @pl.when(s == 0)
            def _():
                for dd in range(2):
                    incoming(dd, 0, p)
                w, m, l = scales([part_ml[at], stats_in(0, 0, p), stats_in(1, 0, p)])
                to_rows = pl.multiple_of(p * 128, 128)
                for e in range(2):
                    for j in range(2):
                        r = slice(2 * j + e, 2 * j + e + 1)
                        tot = (tile(part.at[at], e, j) * w[0][r] + tile(o_recv.at[0, 0, p], e, j) * w[1][r]
                               + tile(o_recv.at[1, 0, p], e, j) * w[2][r])
                        a_half[1, j, pl.ds(to_rows + e * 64, 64), :] = (tot / l[r]).astype(BF16)

        q_own(0)
        q_own(1)
        @pl.when(has_mem)
        def _():
            top_s[...] = score_all(S, 0, keys_of(GROUPS[0] // 16), head_rhs(z, GROUPS[0] // 16, 0), KBC)

        for d in range(2):
            for s in range(4):
                src = x_all.at[z, pl.ds(my_rows, rows if s < 3 else rows // 2), :]
                rcopy(src, src, xtx.at[d, s], xrx.at[d, s, 0], nbr(d)).wait_send()
        for o in range(Z):
            src = x_all.at[o, pl.ds(my_rows, rows), :]
            rcopy(src, src, ptx.at[o], prx.at[o], partner).wait_send()
        for i in (WG, WU, WD, CO):
            cur[i].wait()
        prefetch(WK, WQ, WV)

        @pl.when(l == 0)
        def _():
            prefetch(CK, CV)

        def step(k, at):
            ia, ir = at
            n = count_of(k)
            ja, jr = ia + lax.rem(n, 8), ir + n // 8
            lax.fori_loop(ia, ja, arrival, 0)

            def ret(i, _):
                reduce_step(return_of(i))
                return 0

            lax.fori_loop(ir, jr, ret, 0)
            groups = [decode(group_of(2 * k + i)) for i in range(3)]
            pl.when(has_mem)(lambda: cross_groups(*groups))
            return ja, jr

        lax.fori_loop(0, len(COUNTS), step, (jnp.int32(0), jnp.int32(0)))

        @pl.when(more)
        def _():
            nxt[CK].wait()
            nxt[CV].wait()

        def finish(i, b):
            v = last_of(i)
            n = jnp.where(jnp.logical_and(more, has_mem), v // 64, 0)
            lax.fori_loop(b, jnp.minimum(b + n, KBC), memory_block, 0)
            reduce_step(lax.rem(v, 64))

            @pl.when(lax.rem(v, 8) == 0)
            def _():
                p = lax.rem(v // 16, 4)
                pair_swap(p).start()
                pair_project(a_half[1, c, pair_rows(p)], my_cols, p)
            return b + n

        for n in CT:
            upd(0, n)[...] = hid[:, cols(n)].astype(F32)

        lax.fori_loop(0, len(LAST), finish, jnp.int32(0))

        @pl.when(l + 2 < n_layers)
        def _():
            after = wcopies(jnp.minimum(l + 2, n_layers - 1))
            after[CK].start()
            after[CV].start()

        for v in LAST[-NP:]:
            p = v % 64 // 16
            pair_swap(p).wait_recv()
            pair_project(att_c[pair_rows(p)], other_cols, p)
        for n in CT:
            hid[:, cols(n)] = upd(0, n)[...].astype(BF16)

        xm = rms_norm(hid[...], gain(g_mlp, l))

        acts = []
        for f in range(NF):
            gt = dot(xm, wg[:, cols(f)])
            up = dot(xm, wu[:, cols(f)])
            acts.append((gt * lax.logistic(gt) * up).astype(BF16))
        full = jnp.concatenate(acts, axis=1)

        for n in CT:
            hid[:, cols(n)] = (hid[:, cols(n)].astype(F32) + dot(full, wd[:, cols(n)])).astype(BF16)
        return carry

    lax.fori_loop(0, n_layers, layer_body, 0)
    drain_ring()
    out[...] = hid[...]


def solution(mesh):
    n_dev = mesh.shape["sp"]

    def local_step(hidden, memory, mem_len, norm_self, norm_cross, norm_mlp, self_q, self_k, self_v, self_o,
                   cross_q, cross_k, cross_v, cross_o, mlp_gate, mlp_up, mlp_down):
        rows, D = hidden.shape
        mem_rows = memory.shape[0]
        L, heads, head_dim = self_o.shape[:3]
        FF = mlp_gate.shape[2]
        Dc = D // 2
        NP = Dc // 128
        Z = n_dev // 2
        KBC = 2 * mem_rows // T
        any_ = pl.BlockSpec(memory_space=pl.ANY)
        vmem = pl.BlockSpec(memory_space=pltpu.VMEM)
        smem = pl.BlockSpec(memory_space=pltpu.SMEM)
        dma = pltpu.SemaphoreType.DMA
        V = pltpu.VMEM
        scratch = [
            V((rows, D), BF16),
            V((Z, 2 * rows, D), BF16),
            V((2, mem_rows, D), BF16),
            V((Z, NP, T, 128), BF16),
            V((Z, NP, 128, T), BF16),
            V((KBC, NP, T, 128), BF16),
            V((KBC, NP, 128, T), BF16),
            V((KBC, T, 128), BF16),
            V((2 * NP, 128, T), BF16),
            V((Z, NP, 128, T), BF16),
            V((2, max(2 * NP, KBC) * T, T), F32),
            V((8, T), F32),
            V((D, Dc), BF16), V((D, Dc), BF16), V((D, Dc), BF16), V((D, D), BF16),
            V((D, Dc), BF16), V((D, Dc), BF16), V((D, Dc), BF16), V((D, D), BF16),
            V((D, FF), BF16), V((D, FF), BF16), V((FF, D), BF16),
            V((8 * NP, 128, T), F32),
            V((8 * NP, 8, 128), F32),
            V((2, 4, NP, 136, T), BF16),
            V((2, 4, NP, 136, T), BF16),
            V((2 * NP, 64, T), F32),
            V((8, T), F32), V((8, T), F32),
            V((2, 2, Dc, 128), BF16),
            V((2, Dc, 128), BF16), V((Dc, 128), BF16),
            V((rows, D), BF16),
            dma((2, 5)), dma((2, 5, 4)), dma((Z,)), dma((Z,)),
            dma((2, 5)), dma((2, 5, NP)),
            dma((2, 4)), dma((2, 4, NP)),
            dma((NP,)), dma((NP,)),
            dma((4,)), dma((4,)), dma((11,)), dma((2,)),
        ]
        call = pl.pallas_call(
            functools.partial(kernel, n_dev, head_dim, L),
            out_shape=jax.ShapeDtypeStruct((rows, D), BF16),
            in_specs=[smem, any_, any_, vmem, vmem, vmem] + [any_] * 11,
            out_specs=vmem,
            scratch_shapes=scratch,
            compiler_params=pltpu.CompilerParams(
                collective_id=0, has_side_effects=True, vmem_limit_bytes=67043328),
            name="decoder",
        )
        return call(mem_len, hidden, memory, norm_self, norm_cross, norm_mlp,
                    self_q, self_k, self_v, self_o.reshape(L, D, D), cross_q, cross_k, cross_v,
                    cross_o.reshape(L, D, D), mlp_gate, mlp_up, mlp_down)

    row_spec = P(("dp", "sp"), None)
    return jax.shard_map(local_step, mesh=mesh, in_specs=(row_spec, row_spec, P("dp")) + (P(),) * 14,
                         out_specs=row_spec, check_vma=False)
```
